128 devices in a mesh: dp: 4 (over y), vocab: 32 (over z, x, core).
Axes of the slice: x: 4, y: 4, z: 4, core: 2. Of those that a mesh axis runs over, the one named last changes fastest.
Arguments:
- input_ids: int32 [1024], P('dp'), may hold values from 0 to 255999
- target_ids: int32 [1024], P('dp'), may hold values from 0 to 255999
- loss_mask: int32 [1024], P('dp'), may hold values 0 or 1
- final_hidden: bfloat16 [1024, 3584], P('dp'), may hold values from -5 to 5, as said below
- norm_gain: float32 [3584], replicated, may hold values from 0.25 to 1.75
- embed_cotangent: bfloat16 [1024, 3584], P('dp'), may hold values from -0.059814453 to 0.059814453
- table: bfloat16 [256000, 3584], P(('dp', 'vocab')), may hold values from -0.08351914 to 0.08351914, as said below
Outputs:
- embedded: bfloat16 [1024, 3584], P('dp')
- loss: float32 [], replicated
- grad_hidden: bfloat16 [1024, 3584], P('dp')
- gain_grad: float32 [3584], replicated
- table_grad: bfloat16 [256000, 3584], P(('dp', 'vocab'))
The draws below stay inside these ranges and needn't reach their ends.
Inputs may be any that keep to these rules, and one draw needn't show every extreme that they name: Every entry of table lies within -5 / sqrt(3584) and 5 / sqrt(3584). Every entry of final_hidden lies within -5 and 5.
All inputs are finite; a program needn't handle non-finite values.
Results may differ from the reference program's by a relative error of at most 0.003.
Values may be sent and summed in bfloat16 or wider, within the bound.
A program may use at most 256 MiB of HBM per device.

```python
import math
import jax
import jax.numpy as jnp
import numpy as np
from jax import lax

D = 3584
SOFTCAP = 30
ROWS = 2000
V = 256000
TOKENS = 1024
N_DP = 4
N_VOCAB = 32


def hub_layout(key):
    hub_stride = ROWS // 4
    hub_count = V // hub_stride
    unit_scale = 1.0 / math.sqrt(D)
    directions = jax.random.truncated_normal(jax.random.fold_in(key, 701), -4.0, 4.0, (hub_count, D), jnp.float32) * unit_scale
    return (hub_stride, hub_count, directions)


def draw_table(key, part):
    hub_stride, hub_count, directions = hub_layout(key)
    unit_scale = 1.0 / math.sqrt(D)
    noise_rows = jax.random.truncated_normal(jax.random.fold_in(key, 703), -4.0, 4.0, (V, D), jnp.float32)
    blocks = (noise_rows * unit_scale).reshape(hub_count, hub_stride, D)
    blocks = blocks.at[:, 0, :].add(directions)
    return jnp.clip(blocks.reshape(V, D), -5.0 * unit_scale, 5.0 * unit_scale).astype(jnp.bfloat16)


def draw_final_hidden(key, part):
    hub_stride, hub_count, directions = hub_layout(key)
    topics = jax.random.randint(jax.random.fold_in(key, 709), (TOKENS,), 0, hub_count)
    leaning = jax.random.uniform(jax.random.fold_in(key, 711), (TOKENS, 1), jnp.float32, 0.1, 0.45)
    base_rows = jax.random.truncated_normal(jax.random.fold_in(key, 713), -4.0, 4.0, (TOKENS, D), jnp.float32)
    pointed = jnp.take(directions, topics, axis=0) * math.sqrt(D)
    return jnp.clip(base_rows + leaning * pointed, -5.0, 5.0).astype(jnp.bfloat16)


def set_ends(entries, rng, low, high):
    shape = entries.shape
    index_at = [jax.random.randint(jax.random.fold_in(rng, axis), (), 0, shape[axis]) for axis in range(len(shape))]
    entries = entries.at[tuple(index_at)].set(low)
    longest = shape.index(max(shape))
    index_at[longest] = (index_at[longest] + 1) % shape[longest]
    return entries.at[tuple(index_at)].set(high)


def levels(rng, shape, pieces, smallest, largest):
    loudness, own = 1.0, jax.random.fold_in(rng, 6)
    for axis_at, blocks in pieces:
        steps = jnp.exp(jax.random.uniform(jax.random.fold_in(own, axis_at), (blocks,), jnp.float32, smallest / len(pieces), largest / len(pieces)))
        loudness = loudness * jnp.repeat(steps, shape[axis_at] // blocks).reshape([-1 if axis == axis_at else 1 for axis in range(len(shape))])
    return loudness


def ranked_wide(own_key, dims, count, skew):
    portions = [min(1 << octave, count + 1 - (1 << octave)) * (1 << 20) // math.isqrt((1 << octave) ** skew) + 1 for octave in range((count + 1).bit_length()) if 1 << octave <= count]
    spread = 1 + sum(portions) // (1 << 30)
    listing = np.cumsum(np.array([max(1, weight // spread) for weight in portions]))
    lot = jax.random.randint(jax.random.fold_in(own_key, 1), dims, 0, int(listing[len(portions) - 1]))
    start = jnp.left_shift(1, jnp.searchsorted(jnp.asarray(listing, jnp.int32), lot, side="right").astype(jnp.int32))
    rank = start - 1 + jax.random.randint(jax.random.fold_in(own_key, 4), dims, 0, 1 << 30) % jnp.minimum(start, count + 1 - start)
    return jax.random.permutation(jax.random.fold_in(own_key, 2), count)[rank].astype(jnp.int32)


def gaussian(stream_key, shape, deviation, limit, cuts=(), kind=jnp.bfloat16):
    gain = levels(stream_key, shape, cuts, -0.22, 0.18) if cuts else 1.0
    array = jax.random.normal(stream_key, shape, jnp.float32) * deviation * gain
    return jnp.minimum(jnp.maximum(array, -limit), limit).astype(kind)


def setup_inputs(seed: int = 0) -> dict:
    keys = jax.random.split(jax.random.key(seed), 8)
    input_ids = set_ends(ranked_wide(keys[0], (TOKENS,), V, 2), jax.random.fold_in(keys[0], 3), 0, V - 1).astype(jnp.int32)
    target_ids = set_ends(ranked_wide(keys[1], (TOKENS,), V, 2), jax.random.fold_in(keys[1], 3), 0, V - 1).astype(jnp.int32)
    loss_mask = set_ends((jax.random.randint(keys[2], (TOKENS,), 0, 8) < 7).astype(jnp.int32), jax.random.fold_in(keys[2], 1), 0, 1)
    final_hidden = draw_final_hidden(jax.random.fold_in(keys[7], 71), 0)
    norm_gain = jnp.clip(1.0 + 0.15 * jax.random.normal(keys[4], (D,), jnp.float32), 0.25, 1.75)
    embed_cotangent = gaussian(keys[5], (TOKENS, D), 0.01, 0.059814453, ((0, 4),))
    table = draw_table(jax.random.fold_in(keys[7], 71), 0)
    return dict(input_ids=input_ids, target_ids=target_ids, loss_mask=loss_mask, final_hidden=final_hidden, norm_gain=norm_gain, embed_cotangent=embed_cotangent, table=table)


EPSILON = 1e-06

def norm_backward(upstream, widened, inv_rms, norm_gain):
    scaled_up = upstream * norm_gain
    mean_dot = lax.optimization_barrier(jnp.mean(scaled_up * widened, axis=1, keepdims=True))
    gradient = inv_rms * scaled_up - widened * (inv_rms * inv_rms * inv_rms) * mean_dot
    gain_part = lax.optimization_barrier(jnp.sum(upstream * widened * inv_rms, axis=0))
    return (gradient.astype(jnp.bfloat16), gain_part)

def reference(input_ids, target_ids, loss_mask, final_hidden, norm_gain, embed_cotangent, table):
    block_count = N_DP * N_VOCAB
    block_rows = V // block_count
    embed_scale = math.sqrt(D)
    embedded = (jnp.take(table, input_ids, axis=0).astype(jnp.float32) * embed_scale).astype(jnp.bfloat16)
    widened = final_hidden.astype(jnp.float32)
    inv_rms = lax.rsqrt(lax.optimization_barrier(jnp.mean(widened * widened, axis=1, keepdims=True)) + EPSILON)
    normed = (widened * inv_rms * norm_gain).astype(jnp.bfloat16)
    blocks = table.reshape(block_count, block_rows, D)
    starts = (jnp.arange(block_count) * block_rows).astype(jnp.int32)

    def forward_block(rows_block):
        raw_logits = jnp.dot(normed, rows_block.T, preferred_element_type=jnp.float32)
        return SOFTCAP * jnp.tanh(raw_logits / SOFTCAP)
    capped = lax.map(forward_block, blocks)
    sum_exp = lax.optimization_barrier(jnp.sum(jnp.exp(capped), axis=(0, 2)))
    token_weight = loss_mask.astype(jnp.float32)
    cotangent_wide = embed_cotangent.astype(jnp.float32)

    def backward_block(carry, operands):
        upstream, picked = carry
        rows_block, start, capped_block = operands
        local_targets = (target_ids - start).astype(jnp.int32)
        target_hit = lax.broadcasted_iota(jnp.int32, capped_block.shape, 1) == local_targets[:, None]
        picked = picked + lax.optimization_barrier(jnp.sum(jnp.where(target_hit, capped_block, 0.0), axis=1))
        slope = token_weight[:, None] * (jnp.exp(capped_block) / sum_exp[:, None] - target_hit.astype(jnp.float32)) * (1.0 - (capped_block / SOFTCAP) ** 2)
        slope_low = slope.astype(jnp.bfloat16)
        upstream = upstream + jnp.dot(slope_low, rows_block, preferred_element_type=jnp.float32)
        head_part = lax.dot_general(slope_low, normed, (((0,), (0,)), ((), ())), preferred_element_type=jnp.float32)
        local_ids = (input_ids - start).astype(jnp.int32)
        inside = (local_ids >= 0) & (local_ids < block_rows)
        segment_ids = jnp.where(inside, local_ids, block_rows).astype(jnp.int32)
        embed_part = jax.ops.segment_sum(cotangent_wide, segment_ids, num_segments=block_rows + 1)[:block_rows] * embed_scale
        return ((upstream, picked), (head_part + embed_part).astype(jnp.bfloat16))
    initial = (jnp.zeros((TOKENS, D), jnp.float32), jnp.zeros((TOKENS,), jnp.float32))
    (upstream, picked), grad_blocks = lax.scan(backward_block, initial, (blocks, starts, capped))
    loss = jnp.sum(token_weight * (jnp.log(sum_exp) - picked)) / jnp.maximum(jnp.sum(token_weight), 1.0)
    grad_hidden, gain_grad = norm_backward(upstream, widened, inv_rms, norm_gain)
    table_grad = grad_blocks.reshape(V, D)
    return (embedded, loss, grad_hidden, gain_grad, table_grad)
```

```python
import math

import jax
import jax.numpy as jnp
from jax import lax
from jax.experimental import pallas as pl
from jax.experimental.pallas import tpu as pltpu
from jax.sharding import Mesh
from jax.sharding import PartitionSpec as P

SOFTCAP = 30.0
EPSILON = 1e-06
D = 3584
ROWS = 2000
DP_VOCAB = ("dp", "vocab_0", "vocab_1", "vocab_2")
MESH = pl.DeviceIdType.MESH
BF = jnp.bfloat16
F32 = jnp.float32
NT = (((1,), (1,)), ((), ()))
TN = (((0,), (0,)), ((), ()))
NN = (((1,), (0,)), ((), ()))
MT = 400
NV = ROWS // MT
CT = 512
NT_COLS = D // CT
HALF = D // 2
VMEM_LIMIT = 66_500_000
TABLE_BOUND = 5.0 / math.sqrt(D) * 1.01


class Place:
    def __init__(self):
        self.y = lax.axis_index("dp")
        self.z = lax.axis_index("vocab_0")
        self.x = lax.axis_index("vocab_1")
        self.c = lax.axis_index("vocab_2")
        self.o = 1 - self.c
        y, z, x, c = self.y, self.z, self.x, self.c
        self.g = y + (y // 2) * (1 - 2 * (y % 2))
        self.ga = self.g + 1 - 2 * (self.g % 2)
        self.gb = (self.g + 2) % 4
        self.gc = (self.ga + 2) % 4
        self.a = x + c * (z - x)
        self.b = z + c * (x - z)
        self.bits = [
            (self.a + self.a // 2) % 2,
            self.a // 2,
            (self.b + self.b // 2) % 2,
            self.b // 2,
        ]
        self.r = self.bits[0] + 2 * self.bits[1] + 4 * self.bits[2] + 8 * self.bits[3]
        self.y_a = {"dp": y + 1 - 2 * (y % 2)}
        self.y_b = {"dp": 3 - y}
        self.core = {"vocab_2": self.o}
        self.mirror = {"vocab_0": x, "vocab_1": z, "vocab_2": self.o}
        self.plane = [self._in_plane(e) for e in range(4)]
        self.ring = {
            name: [{name: (i + off) % 4} for off in (1, 2, 3)]
            for name, i in (("vocab_1", x), ("vocab_0", z), ("dp", y))
        }
        self.ring_at = {"vocab_1": x, "vocab_0": z, "dp": y}
        self.cols = pl.ds(pl.multiple_of(c * HALF, 128), HALF)

    def _in_plane(self, e):
        a, b = self.a, self.b
        if e == 0:
            a = a + 1 - 2 * (a % 2)
        elif e == 1:
            a = 3 - a
        elif e == 2:
            b = b + 1 - 2 * (b % 2)
        else:
            b = 3 - b
        return {"vocab_1": a + self.c * (b - a), "vocab_0": b + self.c * (a - b)}

    def meet(self, mirror=False):
        peers = [self.core] + [d for name in self.ring for d in self.ring[name]]
        if mirror:
            peers.append(self.mirror)
        barrier = pltpu.get_barrier_semaphore()
        for peer in peers:
            pl.semaphore_signal(barrier, inc=1, device_id=peer, device_id_type=MESH)
        return lambda: pl.semaphore_wait(barrier, len(peers))


class Post:
    def __init__(self, send_sems, recv_sems):
        self.sems = (send_sems, recv_sems)
        self.used = 0
        self.open = []

    def send(self, src, dst, peer):
        copy = pltpu.make_async_remote_copy(
            src_ref=src,
            dst_ref=dst,
            send_sem=self.sems[0].at[self.used],
            recv_sem=self.sems[1].at[self.used],
            device_id=peer,
            device_id_type=MESH,
        )
        self.used += 1
        copy.start()
        self.open.append(copy)
        return copy

    def sent(self, copy):
        copy.wait_send()
        self.open = [c for c in self.open if c is not copy]

    def close(self):
        for copy in self.open:
            copy.wait_send()
        self.open = []


class Agenda:
    def __init__(self):
        self.now = 0.0
        self.todo = []
        self.count = 0

    def add(self, after, step):
        self.todo.append((self.now + after, self.count, step))
        self.count += 1

    def run(self, until=None):
        while self.todo:
            self.todo.sort(key=lambda item: item[:2])
            if until is not None and self.todo[0][0] > until:
                return
            when, _, step = self.todo.pop(0)
            self.now = max(self.now, when)
            step()

    def compute(self, cost, work):
        self.run(self.now)
        work()
        self.now += cost
        self.run(self.now)


def pick(dims, fixed):
    return tuple(fixed.get(d, slice(None)) for d in dims)


class Scatter:
    def __init__(self, place, post, agenda, tile, bufs, last):
        self.place, self.post, self.agenda = place, post, agenda
        self.bufs, self.last = bufs, last
        self.order = [(tile + i) % 4 for i in range(4)]
        self.dims = [3, 2, 1, 0]

    def start(self, held):
        self._send(held, 0)

    def _send(self, held, step):
        e = self.order[step]
        bit = self.place.bits[e]
        out = (slice(None),) + pick(self.dims, {e: 1 - bit})
        keep = (slice(None),) + pick(self.dims, {e: bit})
        target = self.bufs[step]
        copy = self.post.send(held.at[out], target, self.place.plane[e])
        wait = (5.5, 4.0, 3.2, 3.0)[step]

        def arrived():
            copy.wait_recv()
            if step < 3:
                target[...] = held[keep] + target[...]
                self.dims.remove(e)
                self._send(target, step + 1)
            else:
                self.last(held[keep] + target[...])

        self.agenda.add(wait, arrived)


def columns(table, j):
    at = j * CT // 2
    return jnp.concatenate([table[:, at : at + 256], table[:, HALF + at : HALF + at + 256]], axis=1)


def y_scatter(place, post, full, mid, end):
    low = place.g % 2
    high = place.g // 2
    copy = post.send(full.at[:, 1 - low], mid, place.y_a)
    copy.wait_recv()
    mid[...] = full[:, low] + mid[...]
    copy = post.send(mid.at[1 - high], end, place.y_b)
    copy.wait_recv()
    return mid[high] + end[...]


def head_kernel(
    meta, hidden, gain, table_hbm,
    capped_hbm, normed_hbm, stats_out, metas_out, found_out,
    table, normed, metas, onehot, cap_tiles, stage, rc, r1, r2, r3, r4, found, y_mid, y_end, stats, ring_in,
    local_sems, send_sems, recv_sems,
):
    place = Place()
    post = Post(send_sems, recv_sems)
    agenda = Agenda()
    first_row = (((place.y * 4 + place.z) * 4 + place.x) * 2 + place.c) * ROWS
    entered = place.meet()
    loads = []
    for i in range(NV):
        rows = pl.ds(i * MT, MT)
        load = pltpu.make_async_copy(table_hbm.at[rows], table.at[rows], local_sems.at[i])
        load.start()
        loads.append(load)

    g = place.g
    own = normed.at[g]

    def normalise(i, carry):
        rows = pl.ds(pl.multiple_of(i * 16, 16), 16)
        wide = hidden[rows, :].astype(F32)
        inv = lax.rsqrt(jnp.mean(wide * wide, axis=1, keepdims=True) + EPSILON)
        own[rows, :] = (wide * inv * gain[...]).astype(BF)
        return carry

    metas[g] = meta[...]
    lax.fori_loop(0, 16, normalise, 0)
    entered()

    low, high = pl.ds(0, 128), pl.ds(128, 128)
    meta_in = [
        post.send(metas.at[g], metas.at[g], peer) for peer in (place.y_a, place.y_b)
    ]

    def ship(block, rows, peer):
        part = normed.at[block, rows, place.cols]
        return post.send(part, part, peer)

    a_low = ship(g, low, place.y_a)
    b_high = ship(g, high, place.y_b)
    a_high = ship(g, high, place.y_a)
    b_low = ship(g, low, place.y_b)
    for copy in meta_in:
        copy.wait_recv()
    copy = post.send(metas.at[place.ga], metas.at[place.ga], place.y_b)
    copy.wait_recv()

    swaps = {}
    relays = {}

    def relay_low():
        a_low.wait_recv()
        relays["low"] = ship(place.ga, low, place.y_b)
        agenda.add(11, lambda: arrive("c_low", relays["low"], place.gc, low))

    def relay_high():
        b_high.wait_recv()
        relays["high"] = ship(place.gb, high, place.y_a)
        agenda.add(11, lambda: arrive("c_high", relays["high"], place.gc, high))

    def arrive(name, copy, block, rows):
        copy.wait_recv()
        swaps[name] = ship(block, rows, place.core)

    def arrive_a():
        a_high.wait_recv()
        swaps["a"] = ship(place.ga, pl.ds(0, 256), place.core)

    def arrive_b():
        b_low.wait_recv()
        swaps["b"] = ship(place.gb, pl.ds(0, 256), place.core)

    agenda.add(11.5, relay_low)
    agenda.add(11.5, relay_high)
    agenda.add(21.5, arrive_a)
    agenda.add(21.5, arrive_b)

    stats[...] = jnp.zeros_like(stats)
    stores = {}

    def forward(block, side, wait_loads=False):
        def tile(i, carry):
            rows = pl.ds(pl.multiple_of(i * MT, 16), MT)
            logits = lax.dot_general(
                table[rows, :], normed[block], NT, preferred_element_type=F32
            )
            capped = SOFTCAP * jnp.tanh(logits / SOFTCAP)
            ids = lax.broadcasted_iota(jnp.int32, capped.shape, 0) + (first_row + i * MT)
            hit = ids == metas[block, 1:2, :]
            total = jnp.sum(jnp.exp(capped), axis=0, keepdims=True)
            picked = jnp.sum(jnp.where(hit, capped, 0.0), axis=0, keepdims=True)
            stats[block, 0:1, :] += total
            stats[block, 1:2, :] += picked
            cap_tiles[side, rows, :] = capped
            return carry

        if wait_loads:
            for i in range(NV):
                loads[i].wait()
        if side in stores:
            stores.pop(side).wait()
        lax.fori_loop(0, NV, tile, 0)
        copy = pltpu.make_async_copy(cap_tiles.at[side], capped_hbm.at[block], local_sems.at[NV + side])
        copy.start()
        stores[side] = copy

    agenda.compute(5.2, lambda: forward(g, 0, True))

    def mark(i, carry):
        rows = pl.ds(pl.multiple_of(i * 16, 16), 16)
        ids = lax.broadcasted_iota(jnp.int32, (16, 256), 0) + (first_row + i * 16)
        for k in range(4):
            same = ids == metas[k, 0:1, :]
            onehot[rows, k * 256 : (k + 1) * 256] = jnp.where(same, 1.0, 0.0).astype(BF)
        return carry

    agenda.compute(1.5, lambda: lax.fori_loop(0, ROWS // 16, mark, 0))

    crossing = {}

    def look_up(j):
        slot = j % 2
        if j >= 2:
            post.sent(crossing[j - 2])
        product = lax.dot_general(
            onehot[...], columns(table, j), TN, preferred_element_type=F32
        ).astype(BF)
        shape = (4, 2, 2, 2, 2, 16, CT // 2)
        stage[slot, 0] = product[:, : CT // 2].reshape(shape)
        stage[slot, 1] = product[:, CT // 2 :].reshape(shape)
        crossing[j] = post.send(stage.at[slot, place.o], rc.at[j], place.core)

    def merge_up(j):
        crossing[j].wait_recv()
        rc[j] = stage[j % 2, place.c] + rc[j]

        def last(value):
            found[:, :, :, j * 256 : (j + 1) * 256] = value.reshape(2, 2, 16, 256)

        Scatter(
            place, post, agenda, j, [r1.at[j], r2.at[j], r3.at[j], r4.at[j]], last
        ).start(rc.at[j])

    def look(j):
        agenda.compute(2.5, lambda: look_up(j))
        agenda.add(0.0 if j == NT_COLS - 1 else 1.5, lambda: merge_up(j))
        if j >= 1:
            agenda.run(agenda.now + 0.0)

    looked = [0]

    def look_while(limit):
        while looked[0] < limit:
            j = looked[0]
            looked[0] += 1
            look(j)

    look_while(5)

    def need(name, work):
        while name not in swaps:
            agenda.run(agenda.todo[0][0] if agenda.todo else None)
        swaps[name].wait_recv()
        work()

    agenda.compute(5.2, lambda: need("a", lambda: forward(place.ga, 1)))
    agenda.compute(5.2, lambda: need("b", lambda: forward(place.gb, 0)))

    def both():
        need("c_low", lambda: None)
        need("c_high", lambda: forward(place.gc, 1))

    agenda.compute(5.2, both)


    def ring_start(name, base, peers, at):
        ring_in[base + at] = stats[...]
        return [
            post.send(ring_in.at[base + at], ring_in.at[base + at], peer) for peer in peers
        ]

    def ring_end(copies, base, count):
        for copy in copies:
            copy.wait_recv()
        total = ring_in[base]
        for i in range(1, count):
            total = total + ring_in[base + i]
        stats[...] = total

    core_copies = ring_start("core", 0, [place.core], place.c)
    base, copies, count = 0, core_copies, 2
    plan = [("vocab_1", 2), ("vocab_0", 6), ("dp", 10)]
    for name, nxt in plan:
        look_one = looked[0] < NT_COLS
        if look_one and base != 0:
            look_while(looked[0] + 1)
        ring_end(copies, base, count)
        copies = ring_start(name, nxt, place.ring[name], place.ring_at[name])
        base, count = nxt, 4
    look_while(NT_COLS)
    agenda.run()
    value = y_scatter(place, post, found, y_mid, y_end)
    found_out[...] = (value.astype(F32) * math.sqrt(D)).astype(BF)
    ring_end(copies, base, count)
    stats_out[...] = stats[...]
    metas_out[...] = metas[...]
    out = pltpu.make_async_copy(normed, normed_hbm, local_sems.at[0])
    out.start()
    for copy in stores.values():
        copy.wait()
    post.close()
    out.wait()


def back_kernel(
    capped_hbm, stats, metas, hidden, gain, cotangent, found, table_hbm,
    slope_hbm, cot_hbm, embed_hbm, grad_hbm, gain_out, loss_out,
    table, slope, cap_tiles, scale_rows, stage, rc, q0, r1, r2, r3, r4, up, y_mid, y_end,
    sums, grad, embed, ring_in, local_sems, send_sems, recv_sems,
):
    place = Place()
    post = Post(send_sems, recv_sems)
    agenda = Agenda()
    first_row = (((place.y * 4 + place.z) * 4 + place.x) * 2 + place.c) * ROWS
    g = place.g
    entered = place.meet(mirror=True)

    def cap_load(i):
        return pltpu.make_async_copy(
            capped_hbm.at[:, pl.ds(i * MT, MT)], cap_tiles.at[i % 2], local_sems.at[i % 2]
        )

    cap_load(0).start()
    cap_load(1).start()

    def table_load(j, h):
        cols = pl.ds(h * HALF + j * 256, 256)
        return pltpu.make_async_copy(
            table_hbm.at[:, cols], table.at[:, cols], local_sems.at[2 + 2 * j + h]
        )

    for j in range(NT_COLS):
        table_load(j, 0).start()
        table_load(j, 1).start()
    own_cot = pltpu.make_async_copy(cotangent, cot_hbm.at[g], local_sems.at[2 + 2 * NT_COLS])
    own_cot.start()

    def line(k, row):
        return metas[k, row : row + 1, :]

    weights = [line(k, 2).astype(F32) for k in range(4)]
    totals = [stats[k, 0:1, :] for k in range(4)]
    targets = [stats[k, 1:2, :] for k in range(4)]
    entered()

    low, high, whole = pl.ds(0, 128), pl.ds(128, 128), pl.ds(0, 256)

    def ship(src, block, rows, peer):
        return post.send(src, cot_hbm.at[block, rows, place.cols], peer)

    a_low = ship(cotangent.at[low, place.cols], g, low, place.y_a)
    b_high = ship(cotangent.at[high, place.cols], g, high, place.y_b)
    a_high = ship(cotangent.at[high, place.cols], g, high, place.y_a)
    b_low = ship(cotangent.at[low, place.cols], g, low, place.y_b)
    swaps = []

    def relay(copy, block, rows, peer, at):
        copy.wait_recv()
        part = cot_hbm.at[block, rows, place.cols]
        onward = post.send(part, part, peer)
        agenda.add(at, lambda: swap(onward, place.gc, rows))

    def swap(copy, block, rows):
        copy.wait_recv()
        part = cot_hbm.at[block, rows, place.cols]
        swaps.append(post.send(part, part, place.core))

    def swap_a():
        a_high.wait_recv()
        part = cot_hbm.at[place.ga, whole, place.cols]
        swaps.append(post.send(part, part, place.core))

    def swap_b():
        b_low.wait_recv()
        part = cot_hbm.at[place.gb, whole, place.cols]
        swaps.append(post.send(part, part, place.core))

    agenda.add(13.0, lambda: relay(a_low, place.ga, low, place.y_b, 12.0))
    agenda.add(13.0, lambda: relay(b_high, place.gb, high, place.y_a, 12.0))
    agenda.add(23.0, swap_a)
    agenda.add(23.0, swap_b)

    def doubling(buf, order, cols, base_wait, then):
        free = []

        def step(n):
            e = order[n]
            at = pick([3, 2, 1, 0], {d: place.bits[d] for d in range(4) if d not in free})
            part = buf.at[at + (slice(None), cols)]
            copy = post.send(part, part, place.plane[e])
            free.append(e)

            def arrived():
                copy.wait_recv()
                if n < 3:
                    step(n + 1)
                else:
                    then()

            agenda.add(base_wait + 0.4 * (1 << n), arrived)

        step(0)

    colour = [
        ((0, 1, 2, 3), pl.ds(pl.multiple_of(place.c * HALF, 128), HALF // 2)),
        ((1, 0, 3, 2), pl.ds(pl.multiple_of(place.c * HALF + HALF // 2, 128), HALF // 2)),
    ]
    mine = tuple(place.bits[d] for d in (3, 2, 1, 0))
    gathered = {"embed": 0, "grad": 0}
    final = []

    def gather_all(buf, name, wait):
        def one_done():
            gathered[name] += 1
            if gathered[name] == 2:
                part = buf.at[:, :, :, :, :, place.cols]
                final.append(post.send(part, part, place.core))

        for order, cols in colour:
            doubling(buf, order, cols, wait, one_done)

    embed[mine + (slice(None), place.cols)] = found[...]
    gather_all(embed, "embed", 3.0)

    factors = [w / s for w, s in zip(weights, totals)]

    def slopes(i):
        cap_load(i).wait()

        def slab(n, carry):
            rows = pl.ds(pl.multiple_of(n * 16, 16), 16)
            ids = lax.broadcasted_iota(jnp.int32, (16, 256), 0) + (first_row + i * MT + n * 16)
            for k in range(4):
                capped = cap_tiles[i % 2, k, rows, :]
                hit = jnp.where(ids == line(k, 1), weights[k], 0.0)
                ratio = capped * (1.0 / SOFTCAP)
                value = (jnp.exp(capped) * factors[k] - hit) * (1.0 - ratio * ratio)
                slope[pl.ds(pl.multiple_of(i * MT + n * 16, 16), 16), k * 256 : (k + 1) * 256] = (
                    value.astype(BF)
                )
            return carry

        lax.fori_loop(0, MT // 16, slab, 0)
        if i + 2 < NV:
            cap_load(i + 2).start()

    for i in range(NV):
        agenda.compute(1.2, lambda: slopes(i))
    slope_store = pltpu.make_async_copy(slope, slope_hbm, local_sems.at[0])
    slope_store.start()

    bound = []
    for k in range(4):
        rest = jnp.maximum(1.0 - jnp.exp(targets[k]) / totals[k], 0.0)
        bound.append(TABLE_BOUND * (2.0 * rest + 1e-4))
    for k in range(4):
        up_scale = jnp.broadcast_to(32600.0 / bound[k], (128, 256))
        scale_rows[0, k * 16 : (k + 1) * 16] = up_scale.T.reshape(16, 16, 128)
        down = jnp.broadcast_to(bound[k] * (1.0 / 32600.0), (128, 256))
        scale_rows[1, k * 16 : (k + 1) * 16] = down.T.reshape(16, 16, 128)

    weight_sum = sum(jnp.sum(w) for w in weights)
    loss_sum = sum(
        jnp.sum(w * (jnp.log(s) - t)) for w, s, t in zip(weights, totals, targets)
    )
    loss_out[...] = jnp.full((8, 128), loss_sum / jnp.maximum(weight_sum, 1.0), F32)

    crossing = {}

    def pull(j):
        slot = j % 2
        if j >= 2:
            post.sent(crossing[j - 2])
        table_load(j, 0).wait()
        table_load(j, 1).wait()
        product = lax.dot_general(
            slope[...], columns(table, j), TN, preferred_element_type=F32
        )
        stage[slot, 0] = product[:, : CT // 2].reshape(64, 16, CT // 2)
        stage[slot, 1] = product[:, CT // 2 :].reshape(64, 16, CT // 2)
        crossing[j] = post.send(stage.at[slot, place.o], rc.at[j], place.core)

    def merge(j):
        crossing[j].wait_recv()

        def slab(n, carry):
            for side in range(2):
                cols = slice(side * 128, side * 128 + 128)
                rows = pl.ds(n * 4, 4)
                total = stage[j % 2, place.c, rows, :, cols] + rc[j, rows, :, cols]
                fixed = jnp.round(total * scale_rows[0, rows])
                q0[j, rows, :, cols] = fixed.astype(jnp.int32).astype(jnp.int16)
            return carry

        lax.fori_loop(0, 16, slab, 0)

        def last(value):
            up[:, :, :, j * 256 : (j + 1) * 256] = value.reshape(2, 2, 16, 256)

        held = q0.at[j].reshape(4, 2, 2, 2, 2, 16, 256)
        Scatter(
            place, post, agenda, j, [r1.at[j], r2.at[j], r3.at[j], r4.at[j]], last
        ).start(held)

    def turn(j):
        agenda.compute(2.5, lambda: pull(j))
        agenda.add(1.8, lambda: merge(j))

    for j in range(NT_COLS):
        turn(j)
    agenda.run()

    fixed = y_scatter(place, post, up, y_mid, y_end)
    back = scale_rows[1, g * 16 + place.r]
    upstream = fixed.astype(jnp.int32).astype(F32) * jnp.concatenate([back] * (HALF // 128), axis=1)
    own_rows = pl.ds(pl.multiple_of(place.r * 16, 16), 16)
    wide_all = hidden[own_rows, :].astype(F32)
    inv = lax.rsqrt(jnp.mean(wide_all * wide_all, axis=1, keepdims=True) + EPSILON)
    wide = hidden[own_rows, place.cols].astype(F32)
    scaled_up = upstream * gain[:, place.cols]
    dot = jnp.sum(scaled_up * wide, axis=1, keepdims=True)
    sums[0] = jnp.broadcast_to(dot, (16, 128))
    other = post.send(sums.at[0], sums.at[1], place.mirror)

    part = jnp.sum(upstream * wide * inv, axis=0, keepdims=True)
    lane = jnp.concatenate([part[:, i * 128 : (i + 1) * 128] for i in range(HALF // 128)], axis=0)

    def ring_start(base, name):
        at = base + place.ring_at[name]
        return [post.send(ring_in.at[at], ring_in.at[at], peer) for peer in place.ring[name]]

    ring_in[place.x, 0 : HALF // 128] = lane
    copies = ring_start(0, "vocab_1")

    other.wait_recv()
    mean_dot = (sums[0, :, 0:1] + sums[1, :, 0:1]) * (1.0 / D)
    value = inv * scaled_up - wide * (inv * inv * inv) * mean_dot
    grad[mine + (slice(None), place.cols)] = value.astype(BF)
    gather_all(grad, "grad", 2.4)

    def ring_turn(copies, base, nxt, name):
        for copy in copies:
            copy.wait_recv()
        total = ring_in[base, 0:14]
        for i in range(1, 4):
            total = total + ring_in[base + i, 0:14]
        if name is None:
            ring_in[nxt + place.c, 0:14] = total
            at = ring_in.at[nxt + place.c]
            copy = post.send(at, at, place.core)
            agenda.add(1.5, copy.wait_recv)
            return
        ring_in[nxt + place.ring_at[name], 0:14] = total
        onward = ring_start(nxt, name)
        then = {"vocab_0": (8, "dp"), "dp": (12, None)}[name]
        agenda.add(3.2, lambda: ring_turn(onward, nxt, *then))

    agenda.add(2.5, lambda: ring_turn(copies, 0, 4, "vocab_0"))
    agenda.run()
    for copy in final:
        copy.wait_recv()
    outs = [
        pltpu.make_async_copy(embed, embed_hbm, local_sems.at[1]),
        pltpu.make_async_copy(grad, grad_hbm, local_sems.at[2]),
    ]
    for copy in outs:
        copy.start()
    gain_out[0] = ring_in[12]
    gain_out[1] = ring_in[13]
    for copy in swaps:
        copy.wait_recv()
    own_cot.wait()
    slope_store.wait()
    post.close()
    for copy in outs:
        copy.wait()


def table_kernel(slope, normed, cot, ids, out):
    first = (
        lax.axis_index(DP_VOCAB) * ROWS + pl.program_id(0) * MT
    )
    rows = lax.broadcasted_iota(jnp.int32, (MT, 256), 0) + first
    mark = jnp.concatenate(
        [jnp.where(rows == ids[k, 0:1, :], 1.0, 0.0).astype(BF) for k in range(4)], axis=1
    )
    for h in range(2):
        cols = slice(h * HALF, (h + 1) * HALF)
        head = lax.dot_general(slope[...], normed[:, cols], NN, preferred_element_type=F32)
        part = lax.dot_general(mark, cot[:, cols], NN, preferred_element_type=F32)
        out[:, cols] = (head + part * math.sqrt(D)).astype(BF)


def body(input_ids, target_ids, loss_mask, final_hidden, norm_gain, embed_cotangent, table):
    any_ = pl.BlockSpec(memory_space=pl.ANY)
    vmem = pl.BlockSpec(memory_space=pltpu.VMEM)
    dma = pltpu.SemaphoreType.DMA
    meta = jnp.pad(jnp.stack([input_ids, target_ids, loss_mask]), ((0, 5), (0, 0)))
    gain = norm_gain.reshape(1, D)
    S = jax.ShapeDtypeStruct

    def params(cid):
        return pltpu.CompilerParams(
            collective_id=cid, has_side_effects=True, vmem_limit_bytes=VMEM_LIMIT
        )

    def halving(n, dt):
        shapes = [(n, 4, 2, 2, 2, 16, 256), (n, 4, 2, 2, 16, 256), (n, 4, 2, 16, 256), (n, 4, 16, 256)]
        return [pltpu.VMEM(s, dt) for s in shapes]

    capped, normed, stats, metas, found = pl.pallas_call(
        head_kernel,
        out_shape=(
            S((4, ROWS, 256), F32),
            S((4, 256, D), BF),
            S((4, 2, 256), F32),
            S((4, 8, 256), jnp.int32),
            S((16, HALF), BF),
        ),
        in_specs=[vmem, vmem, vmem, any_],
        out_specs=(any_, any_, vmem, vmem, vmem),
        scratch_shapes=[
            pltpu.VMEM((ROWS, D), BF),
            pltpu.VMEM((4, 256, D), BF),
            pltpu.VMEM((4, 8, 256), jnp.int32),
            pltpu.VMEM((ROWS, 1024), BF),
            pltpu.VMEM((2, ROWS, 256), F32),
            pltpu.VMEM((2, 2, 4, 2, 2, 2, 2, 16, 256), BF),
            pltpu.VMEM((NT_COLS, 4, 2, 2, 2, 2, 16, 256), BF),
            *halving(NT_COLS, BF),
            pltpu.VMEM((2, 2, 16, HALF), BF),
            pltpu.VMEM((2, 16, HALF), BF),
            pltpu.VMEM((16, HALF), BF),
            pltpu.VMEM((4, 2, 256), F32),
            pltpu.VMEM((14, 4, 2, 256), F32),
            dma((NV + 2,)),
            dma((64,)),
            dma((64,)),
        ],
        compiler_params=params(0),
        name="head",
    )(meta, final_hidden, gain, table)

    slope, cot, embed, grad, gain_parts, loss = pl.pallas_call(
        back_kernel,
        out_shape=(
            S((ROWS, 1024), BF),
            S((4, 256, D), BF),
            S((2, 2, 2, 2, 16, D), BF),
            S((2, 2, 2, 2, 16, D), BF),
            S((2, 16, 128), F32),
            S((8, 128), F32),
        ),
        in_specs=[any_, vmem, vmem, vmem, vmem, vmem, vmem, any_],
        out_specs=(any_, any_, any_, any_, vmem, vmem),
        scratch_shapes=[
            pltpu.VMEM((ROWS, D), BF),
            pltpu.VMEM((ROWS, 1024), BF),
            pltpu.VMEM((2, 4, MT, 256), F32),
            pltpu.VMEM((2, 64, 16, 128), F32),
            pltpu.VMEM((2, 2, 64, 16, 256), F32),
            pltpu.VMEM((NT_COLS, 64, 16, 256), F32),
            pltpu.VMEM((NT_COLS, 64, 16, 256), jnp.int16),
            *halving(NT_COLS, jnp.int16),
            pltpu.VMEM((2, 2, 16, HALF), jnp.int16),
            pltpu.VMEM((2, 16, HALF), jnp.int16),
            pltpu.VMEM((16, HALF), jnp.int16),
            pltpu.VMEM((2, 16, 128), F32),
            pltpu.VMEM((2, 2, 2, 2, 16, D), BF),
            pltpu.VMEM((2, 2, 2, 2, 16, D), BF),
            pltpu.VMEM((14, 16, 128), F32),
            dma((3 + 2 * NT_COLS,)),
            dma((96,)),
            dma((96,)),
        ],
        compiler_params=params(1),
        name="back",
    )(capped, stats, metas, final_hidden, gain, embed_cotangent, found, table)

    table_grad = pl.pallas_call(
        table_kernel,
        grid=(NV,),
        out_shape=S((ROWS, D), BF),
        in_specs=[
            pl.BlockSpec((MT, 1024), lambda i: (i, 0)),
            pl.BlockSpec((1024, D), lambda i: (0, 0)),
            pl.BlockSpec((1024, D), lambda i: (0, 0)),
            pl.BlockSpec((4, 8, 256), lambda i: (0, 0, 0)),
        ],
        out_specs=pl.BlockSpec((MT, D), lambda i: (i, 0)),
        compiler_params=pltpu.CompilerParams(vmem_limit_bytes=VMEM_LIMIT),
        name="table_grad",
    )(slope, normed.reshape(1024, D), cot.reshape(1024, D), metas)
    return (
        embed.reshape(256, D),
        loss[0, 0],
        grad.reshape(256, D),
        gain_parts[:, : HALF // 128].reshape(D),
        table_grad,
    )


def solution(mesh):
    finer = Mesh(
        mesh.devices.reshape(mesh.shape["dp"], 4, 4, 2), ("dp", "vocab_0", "vocab_1", "vocab_2")
    )
    placed = (P("dp"), P("dp"), P("dp"), P("dp", None), P(), P("dp", None), P(DP_VOCAB, None))
    return jax.shard_map(
        body,
        mesh=finer,
        in_specs=placed,
        out_specs=(P("dp", None), P(), P("dp", None), P(), P(DP_VOCAB, None)),
        check_vma=False,
    )
```

```python
import math

import jax
import jax.numpy as jnp
from jax import lax
from jax.experimental import pallas as pl
from jax.experimental.pallas import tpu as pltpu
from jax.sharding import Mesh
from jax.sharding import PartitionSpec as P

SOFTCAP = 30.0
EPSILON = 1e-06
D = 3584
ROWS = 2000
EMBED_SCALE = math.sqrt(D)
DP_VOCAB = ("dp", "vocab_0", "vocab_1", "vocab_2")
MESH = pl.DeviceIdType.MESH
BF = jnp.bfloat16
F32 = jnp.float32
I16 = jnp.int16
NT = (((1,), (1,)), ((), ()))
TN = (((0,), (0,)), ((), ()))
NN = (((1,), (0,)), ((), ()))
MT = 400
MF = 256
NV = ROWS // MT
HALF = D // 2
W = 256
NT_COLS = HALF // W
CHUNK = 32
D_START = 24.0
VMEM_LIMIT = 66_900_000
TABLE_BOUND = 5.0 / math.sqrt(D) * 1.01
UNITS = 24000.0
KNEE = 256.0
FINE = 32.0


def encode(value):
    bent = jnp.clip(value, -KNEE, KNEE)
    return jnp.round(value + bent * (FINE - 1.0)).astype(jnp.int32).astype(I16)


def decode(code):
    wide = code.astype(jnp.int32).astype(F32)
    return wide - jnp.clip(wide, -KNEE * FINE, KNEE * FINE) * (1.0 - 1.0 / FINE)


def gray(i):
    return i + (i // 2) * (1 - 2 * (i % 2))


class Place:
    def __init__(self):
        self.y = y = lax.axis_index("dp")
        self.z = z = lax.axis_index("vocab_0")
        self.x = x = lax.axis_index("vocab_1")
        self.c = c = lax.axis_index("vocab_2")
        self.o = 1 - c
        self.first_row = (((y * 4 + z) * 4 + x) * 2 + c) * ROWS
        self.g = gray(y)
        self.ga = self.g + 1 - 2 * (self.g % 2)
        self.gb = (self.g + 2) % 4
        self.gc = (self.ga + 2) % 4
        self.y_a = {"dp": y + 1 - 2 * (y % 2)}
        self.y_b = {"dp": 3 - y}
        self.core = {"vocab_2": self.o}
        self.a = x + c * (z - x)
        self.b = z + c * (x - z)
        self.a_peers = [self._at((self.a + off) % 4, self.b) for off in (1, 2, 3)]
        self.b_peers = [self._at(self.a, (self.b + off) % 4) for off in (1, 2, 3)]
        self.x_peers = [{"vocab_1": (x + off) % 4} for off in (1, 2, 3)]
        self.z_peers = [{"vocab_0": (z + off) % 4} for off in (1, 2, 3)]
        self.y_peers = [{"dp": (y + off) % 4} for off in (1, 2, 3)]
        self.cols = pl.ds(pl.multiple_of(c * HALF, 128), HALF)
        self.tiles = [self.tile_cols(j) for j in range(NT_COLS)]
        self.a_at = [(self.a + off) % 4 for off in (1, 2, 3)]
        self.b_at = [(self.b + off) % 4 for off in (1, 2, 3)]
        self.y_at = [gray((y + off) % 4) for off in (1, 2, 3)]
        a, b = self.a, self.b
        a0, a1, b0 = (a + a // 2) % 2, a // 2, (b + b // 2) % 2
        self.colour = (a0 + b0) % 2 + 2 * ((a1 + b0) % 2)
        flip_a, flip_b = a + 1 - 2 * (a % 2), b + 1 - 2 * (b % 2)
        self.near = [self._at(flip_a, b), self._at(3 - a, b), self._at(a, flip_b)]

    def _at(self, a, b):
        return {"vocab_1": a + self.c * (b - a), "vocab_0": b + self.c * (a - b)}

    def tile_cols(self, j, core=None):
        core = self.c if core is None else core
        return pl.ds(pl.multiple_of(core * HALF + j * W, 128), W)

    def meet(self):
        peers = [self.core] + self.x_peers + self.z_peers + self.y_peers
        barrier = pltpu.get_barrier_semaphore()
        for peer in peers:
            pl.semaphore_signal(barrier, inc=1, device_id=peer, device_id_type=MESH)
        return lambda: pl.semaphore_wait(barrier, len(peers))


class Sent:
    def __init__(self, sems, at, out_like, in_like, times):
        self.sems, self.at = sems, at
        self.out_like, self.in_like, self.times = out_like, in_like, times

    def wait_send(self):
        for _ in range(self.times):
            like = self.out_like()
            pltpu.make_async_copy(like, like, self.sems[0].at[self.at]).wait()

    def wait_recv(self):
        like = self.in_like()
        pltpu.make_async_copy(like, like, self.sems[1].at[self.at]).wait()


class Post:
    def __init__(self, send_sems, recv_sems):
        self.sems = (send_sems, recv_sems)
        self.used = 0
        self.open = []

    def send(self, src, dst, peer):
        return self.group([(src, dst, peer)], src, dst)

    def group(self, parts, out_like, in_like, times=1):
        for src, dst, peer in parts:
            pltpu.make_async_remote_copy(
                src_ref=src(),
                dst_ref=dst(),
                send_sem=self.sems[0].at[self.used],
                recv_sem=self.sems[1].at[self.used],
                device_id=peer,
                device_id_type=MESH,
            ).start()
        sent = Sent(self.sems, self.used, out_like, in_like, times)
        self.used += 1
        self.open.append(sent)
        return sent

    def sent(self, item):
        item.wait_send()
        self.open = [c for c in self.open if c is not item]

    def close(self):
        for item in self.open:
            item.wait_send()
        self.open = []


class Agenda:
    def __init__(self):
        self.now = 0.0
        self.todo = []
        self.count = 0

    def add(self, after, step):
        self.todo.append((self.now + after, self.count, step))
        self.count += 1

    def run(self, until=None):
        while self.todo:
            self.todo.sort(key=lambda item: item[:2])
            if until is not None and self.todo[0][0] > until:
                return
            when, _, step = self.todo.pop(0)
            self.now = max(self.now, when)
            step()

    def due(self, until):
        return any(item[0] <= until for item in self.todo)

    def compute(self, cost, work):
        self.run(self.now)
        work()
        self.now += cost
        self.run(self.now)


def columns(table, j):
    left = pl.ds(pl.multiple_of(j * W, 128), W)
    right = pl.ds(pl.multiple_of(HALF + j * W, 128), W)
    return jnp.concatenate([table[:, left], table[:, right]], axis=1)


def gather_tile(place, post, agenda, buf, j, sends):
    a, b = place.a, place.b
    cols = place.tiles[j]

    def mine():
        return buf.at[b, a, :, cols]

    first = post.group(
        [(mine, mine, peer) for peer in place.b_peers], mine, lambda: buf.at[0:3, 0, :, cols], 3
    )

    def along_a():
        first.wait_recv()

        def part():
            return buf.at[:, a, :, cols]

        def like():
            return buf.at[:, 0:3, :, cols]

        second = post.group([(part, part, peer) for peer in place.a_peers], like, like)
        sends.append(second)
        agenda.add(4.5, lambda: across(second))

    def across(second):
        second.wait_recv()

        def part():
            return buf.at[:, :, :, cols]

        third = post.send(part, part, place.core)
        sends.append(third)
        agenda.add(2.5, third.wait_recv)

    sends.append(first)
    agenda.add(3.6, along_a)


STEPS = 7
LAG = (1, 4, 6, 8, 10, 12, 13)
TG_TURNS = NT_COLS
TURNS = NT_COLS + LAG[-1]


def main_kernel(
    meta, hidden, gain, table_hbm, cotangent,
    head_hbm, cot_hbm, metas_out, embed_hbm, grad_hbm, gain_out, loss_out, cap_hbm,
    table, normed, metas, marks, stats, stat_in, scale_rows, back_rows, inverses,
    d_stage, d_rc, d_rx, d_rz, d_ry, found,
    stage, snd, rc, sx, rx, acc, sz, rz, acc_z, sy, ry, up,
    gain_in, local_sems, send_sems, recv_sems, flow_send, flow_recv,
):
    place = Place()
    post = Post(send_sems, recv_sems)
    agenda = Agenda()
    first_row = place.first_row
    a, b, c, o, g, y = place.a, place.b, place.c, place.o, place.g, place.y
    blocks = [g, place.ga, place.gb, place.gc]
    entered = place.meet()
    table_load = pltpu.make_async_copy(table_hbm, table, local_sems.at[0])
    table_load.start()
    metas[g] = meta[...]

    def inverse(wide):
        return lax.rsqrt(jnp.mean(wide * wide, axis=1, keepdims=True) + EPSILON)

    def rows_of(block, first, count):
        return pl.ds(pl.multiple_of(block * 256 + first, 16), count)

    quarter = place.colour

    def normalise(i, carry):
        at = ((quarter + i) % 4) * 64
        rows = pl.ds(pl.multiple_of(at, 16), 64)
        wide = hidden[rows, :].astype(F32)
        inv = inverse(wide)
        inverses[rows, :] = jnp.broadcast_to(inv, (64, 128))
        normed[rows_of(g, at, 64), :] = (wide * inv * gain[...]).astype(BF)
        return carry

    normalise(0, 0)
    stats[...] = jnp.zeros_like(stats)
    entered()

    def ship(block, first, count, peer):
        def part():
            return normed.at[rows_of(block, first, count), place.cols]

        return post.send(part, part, peer)

    at_q = quarter * 64
    meta_in = [
        post.send(lambda: metas.at[g], lambda: metas.at[g], peer) for peer in (place.y_a, place.y_b)
    ]
    a_low = ship(g, at_q, 32, place.y_a)
    b_high = ship(g, at_q + 32, 32, place.y_b)
    a_high = ship(g, at_q + 32, 32, place.y_a)
    b_low = ship(g, at_q, 32, place.y_b)
    lax.fori_loop(1, 4, normalise, 0)
    for item in meta_in:
        item.wait_recv()
    meta_c = post.send(lambda: metas.at[place.ga], lambda: metas.at[place.ga], place.y_b)
    spread = {}
    swaps = {}
    relays = []

    def relay():
        a_low.wait_recv()
        relays.append(ship(place.ga, at_q, 32, place.y_b))
        b_high.wait_recv()
        relays.append(ship(place.gb, at_q + 32, 32, place.y_a))

    def spread_block(name, block, items):
        for item in items:
            item.wait_recv()
        spread[name] = [ship(block, at_q, 64, peer) for peer in place.near]

    def swap_block(name, block):
        for item in spread[name]:
            item.wait_recv()
        swaps[name] = ship(block, 0, 256, place.core)

    cot_in = {}
    pieces = 256 // CHUNK

    def piece(n):
        rows_a = pl.ds((n % pieces) * CHUNK, CHUNK)
        rows_b = pl.ds((pieces - 1 - n % pieces) * CHUNK, CHUNK)

        def part(ref, rows, block=None):
            if block is None:
                return lambda: ref.at[rows, place.cols]
            return lambda: ref.at[block, rows, place.cols]

        if n < pieces:
            cot_in["a", n] = post.send(part(cotangent, rows_a), part(cot_hbm, rows_a, g), place.y_a)
            cot_in["b", n] = post.send(part(cotangent, rows_b), part(cot_hbm, rows_b, g), place.y_b)
        else:
            cot_in["b", n - pieces].wait_recv()
            cot_in["a", n - pieces].wait_recv()
            at_a, at_b = part(cot_hbm, rows_b, place.gb), part(cot_hbm, rows_a, place.ga)
            cot_in["a", n] = post.send(at_a, at_a, place.y_a)
            cot_in["b", n] = post.send(at_b, at_b, place.y_b)

    def cot_swap():
        for n in range(pieces // 2, pieces + pieces // 2):
            cot_in["a", n].wait_recv()
            cot_in["b", n].wait_recv()

        def part(block):
            return lambda: cot_hbm.at[block, :, place.cols]

        for n, block in enumerate((place.ga, place.gb, place.gc)):
            cot_in["swap", n] = post.send(part(block), part(block), place.core)

    def cap_store(n):
        return pltpu.make_async_copy(
            stage.at[n, pl.ds(0, ROWS)], cap_hbm.at[n], local_sems.at[1 + n]
        )

    def forward(n):
        block, side = blocks[n], n % 2
        if n >= 2:
            cap_store(side).wait()
        rows = normed[rows_of(block, 0, 256), :]
        total = jnp.zeros((1, 256), F32)
        picked = total
        for at in range(0, ROWS, MF):
            size = min(MF, ROWS - at)
            logits = lax.dot_general(table[at : at + size, :], rows, NT, preferred_element_type=F32)
            capped = SOFTCAP * jnp.tanh(logits * (1.0 / SOFTCAP))
            stage[side, at : at + size] = capped
            ids = lax.broadcasted_iota(jnp.int32, capped.shape, 0) + (first_row + at)
            hit = ids == metas[block, 1:2, :]
            total += jnp.sum(jnp.exp(capped), axis=0, keepdims=True)
            picked += jnp.sum(jnp.where(hit, capped, 0.0), axis=0, keepdims=True)
        stats[block, 0:1, :] = total
        stats[block, 1:2, :] = picked
        if n < 2:
            cap_store(side).start()

    table_load.wait()
    agenda.now = 4.5
    agenda.compute(4.0, lambda: forward(0))

    def mark(i, carry):
        rows = pl.ds(pl.multiple_of(i * MT, 16), MT)
        ids = lax.broadcasted_iota(jnp.int32, (MT, 256), 0) + (first_row + i * MT)
        for k in range(4):
            same = ids == metas[k, 0:1, :]
            marks[rows, k * 256 : (k + 1) * 256] = jnp.where(same, 1.0, 0.0).astype(BF)
        return carry

    meta_c.wait_recv()
    relay()
    agenda.compute(1.2, lambda: lax.fori_loop(0, NV, mark, 0))
    crossing = {}
    shape = (4, 4, 4, 16, W)

    def look_up(j):
        slot = j % 2
        if j >= 2:
            post.sent(crossing[j - 2])
        product = lax.dot_general(
            marks[...], columns(table, j), TN, preferred_element_type=F32
        ).astype(BF)
        d_stage[slot, 0:1024] = product[:, :W]
        d_stage[slot, 1024:2048] = product[:, W:]

        def there():
            return d_stage.at[slot, pl.ds(pl.multiple_of(o * 1024, 16), 1024)].reshape(*shape)

        crossing[j] = post.send(there, lambda: d_rc.at[j], place.core)

    def d_merge(j):
        crossing[j].wait_recv()
        here = d_stage[j % 2, pl.ds(pl.multiple_of(c * 1024, 16), 1024), :]
        d_rc[j] = here.reshape(*shape) + d_rc[j]
        agenda.add(max(0.0, D_START - agenda.now), lambda: d_along_a(j))

    def d_along_a(j):
        parts = [
            (lambda n=n: d_rc.at[j, :, :, place.a_at[n]], lambda n=n: d_rx.at[j, n], peer)
            for n, peer in enumerate(place.a_peers)
        ]
        item = post.group(parts, lambda: d_rx.at[j], lambda: d_rx.at[j])
        agenda.add(7.0, lambda: d_along_b(j, item))

    def d_along_b(j, item):
        item.wait_recv()
        d_rc[j, :, :, a] = (d_rc[j, :, :, a] + d_rx[j, 0]) + (d_rx[j, 1] + d_rx[j, 2])
        parts = [
            (lambda n=n: d_rc.at[j, :, place.b_at[n], a], lambda n=n: d_rz.at[j, n], peer)
            for n, peer in enumerate(place.b_peers)
        ]
        item = post.group(parts, lambda: d_rz.at[j], lambda: d_rz.at[j])
        agenda.add(5.0, lambda: d_along_y(j, item))

    def d_along_y(j, item):
        item.wait_recv()
        d_rc[j, :, b, a] = (d_rc[j, :, b, a] + d_rz[j, 0]) + (d_rz[j, 1] + d_rz[j, 2])
        parts = [
            (lambda n=n: d_rc.at[j, place.y_at[n], b, a], lambda n=n: d_ry.at[j, n], peer)
            for n, peer in enumerate(place.y_peers)
        ]
        item = post.group(parts, lambda: d_ry.at[j], lambda: d_ry.at[j])
        agenda.add(6.0, lambda: d_end(j, item))

    def d_end(j, item):
        item.wait_recv()
        row = (d_rc[j, g, b, a] + d_ry[j, 0]) + (d_ry[j, 1] + d_ry[j, 2])
        found[b, a, :, place.tiles[j]] = (row.astype(F32) * EMBED_SCALE).astype(BF)
        gather_tile(place, post, agenda, found, j, found_sends)

    looked = [0]
    found_sends = []

    def look():
        j = looked[0]
        looked[0] += 1
        agenda.compute(2.4, lambda: look_up(j))
        agenda.add(2.2, lambda: d_merge(j))

    look()
    spread_block("a", place.ga, [a_low_rest for a_low_rest in (a_high,)])
    spread_block("b", place.gb, [b_low])
    look()
    spread_block("c", place.gc, relays)
    for _ in range(2):
        look()
    swap_block("a", place.ga)
    swap_block("b", place.gb)
    agenda.now = max(agenda.now, 23.0)
    swaps["a"].wait_recv()
    agenda.compute(4.0, lambda: forward(1))
    swap_block("c", place.gc)
    piece(0)
    swaps["b"].wait_recv()
    agenda.compute(4.0, lambda: forward(2))
    piece(1)
    swaps["c"].wait_recv()
    agenda.compute(4.0, lambda: forward(3))

    def ring_start(base, peers, at):
        stat_in[base + at] = stats[...]

        def part():
            return stat_in.at[base + at]

        def like():
            return stat_in.at[pl.ds(0, len(peers))]

        return post.group([(part, part, peer) for peer in peers], like, like)

    def ring_end(item, base, count):
        item.wait_recv()
        total = stat_in[base]
        for i in range(1, count):
            total = total + stat_in[base + i]
        stats[...] = total

    item, base, count = ring_start(0, [place.core], c), 0, 2
    for peers, at in ((place.x_peers, place.x), (place.z_peers, place.z), (place.y_peers, y)):
        if base:
            look()
        ring_end(item, base, count)
        base = base + 4
        item, count = ring_start(base, peers, at), 4
    while looked[0] < NT_COLS:
        look()
    agenda.run(agenda.now + 1.5)
    ring_end(item, base, count)
    piece(2)

    def cap_load(n):
        return pltpu.make_async_copy(
            cap_hbm.at[n], stage.at[n, pl.ds(0, ROWS)], local_sems.at[1 + n]
        )

    def slopes(n):
        block, side = blocks[n], n % 2
        if n < 2:
            cap_load(n).wait()
        weight = metas[block, 2:3, :].astype(F32)
        factor = weight / stats[block, 0:1, :]
        target = metas[block, 1:2, :]
        lanes = pl.ds(pl.multiple_of(block * 256, 128), 256)

        def slab(i, carry):
            rows = pl.ds(pl.multiple_of(i * MT, 16), MT)
            ids = lax.broadcasted_iota(jnp.int32, (MT, 256), 0) + (first_row + i * MT)
            capped = stage[side, rows, :]
            hit = jnp.where(ids == target, weight, 0.0)
            ratio = capped * (1.0 / SOFTCAP)
            value = (jnp.exp(capped) * factor - hit) * (1.0 - ratio * ratio)
            marks[rows, lanes] = value.astype(BF)
            return carry

        lax.fori_loop(0, NV, slab, 0)
        if n >= 2:
            cap_load(n - 2).start()

    for n in (2, 3, 0, 1):
        agenda.compute(0.9, lambda: slopes(n))

    def bound(k):
        rest = jnp.maximum(1.0 - jnp.exp(stats[k, 1:2, :]) / stats[k, 0:1, :], 0.0)
        return TABLE_BOUND * (2.0 * rest + 1e-4)

    for k in range(4):
        turned = jnp.broadcast_to(UNITS / bound(k), (128, 256)).T
        scale_rows[k * 256 : (k + 1) * 256, :] = turned
    back_rows[...] = jnp.broadcast_to(bound(g) * (1.0 / UNITS), (128, 256)).T

    weights = [metas[k, 2:3, :].astype(F32) for k in range(4)]
    weight_sum = sum(jnp.sum(w) for w in weights)
    loss_sum = sum(
        jnp.sum(w * (jnp.log(stats[k, 0:1, :]) - stats[k, 1:2, :])) for k, w in enumerate(weights)
    )
    loss_out[...] = jnp.full((8, 128), loss_sum / jnp.maximum(weight_sum, 1.0), F32)
    for j in (NT_COLS - 2, NT_COLS - 1):
        post.sent(crossing[j])

    class Flow:
        def __init__(self, step, j):
            self.send_sem, self.recv_sem = flow_send.at[step, j], flow_recv.at[step, j]

        def start(self, parts):
            for src, dst, peer in parts:
                pltpu.make_async_remote_copy(
                    src_ref=src,
                    dst_ref=dst,
                    send_sem=self.send_sem,
                    recv_sem=self.recv_sem,
                    device_id=peer,
                    device_id_type=MESH,
                ).start()

        def sent(self, like):
            pltpu.make_async_copy(like, like, self.send_sem).wait()

        def here(self, like):
            pltpu.make_async_copy(like, like, self.recv_sem).wait()

    def pull(t):
        slot = t % 2

        @pl.when(t >= 2)
        def _():
            Flow(0, t - 2).sent(snd.at[slot])

        product = lax.dot_general(marks[...], columns(table, t), TN, preferred_element_type=F32)
        for side in range(2):
            for half in range(2):
                at = side * W + half * 128
                stage[slot, side * 1024 : side * 1024 + 1024, half * 128 : half * 128 + 128] = (
                    product[:, at : at + 128] * scale_rows[...]
                )
        there = pl.ds(pl.multiple_of(o * 1024, 16), 1024)
        snd[slot] = encode(stage[slot, there, :]).reshape(*shape)
        Flow(0, t).start([(snd.at[slot], rc.at[t % 4], place.core)])

    def held(slot, at):
        whole = stage.at[slot, pl.ds(pl.multiple_of(c * 1024, 16), 1024)].reshape(*shape)
        return whole[:, :, at]

    def merge(j):
        slot = j % 2
        Flow(0, j).here(rc.at[j % 4])

        @pl.when(j >= 2)
        def _():
            Flow(1, j - 2).sent(sx.at[slot])

        acc[j] = held(slot, a) + decode(rc[j % 4, :, :, a])
        parts = []
        for n, peer in enumerate(place.a_peers):
            at = place.a_at[n]
            sx[slot, n] = encode(held(slot, at) + decode(rc[j % 4, :, :, at]))
            parts.append((sx.at[slot, n], rx.at[j, n], peer))
        Flow(1, j).start(parts)

    def along_b(j):
        Flow(1, j).here(rx.at[j])
        parts = []
        for n in range(4):
            at = (b + n) % 4
            value = acc[j, :, at] + decode(rx[j, 0, :, at])
            value = value + decode(rx[j, 1, :, at]) + decode(rx[j, 2, :, at])
            if n == 0:
                acc_z[j] = value
            else:
                sz[j, n - 1] = encode(value)
                parts.append((sz.at[j, n - 1], rz.at[j, n - 1], place.b_peers[n - 1]))
        Flow(2, j).start(parts)

    def along_y(j):
        Flow(2, j).here(rz.at[j])
        acc_z[j] = acc_z[j] + decode(rz[j, 0]) + decode(rz[j, 1]) + decode(rz[j, 2])
        parts = []
        for n, peer in enumerate(place.y_peers):
            sy[j, n] = encode(acc_z[j, place.y_at[n]])
            parts.append((sy.at[j, n], ry.at[j, n], peer))
        Flow(3, j).start(parts)

    def give_b(j):
        Flow(3, j).here(ry.at[j])
        value = acc_z[j, g] + decode(ry[j, 0]) + decode(ry[j, 1]) + decode(ry[j, 2])
        cols = place.tile_cols(j)
        up[b, a, :, cols] = encode(value)
        part = up.at[b, a, :, cols]
        Flow(4, j).start([(part, part, peer) for peer in place.b_peers])

    def give_a(j):
        cols = place.tile_cols(j)
        Flow(4, j).here(up.at[0:3, 0, :, cols])
        part = up.at[:, a, :, cols]
        Flow(5, j).start([(part, part, peer) for peer in place.a_peers])

    def give_core(j):
        cols = place.tile_cols(j)
        Flow(5, j).here(up.at[:, 0:3, :, cols])
        part = up.at[:, :, :, cols]
        Flow(6, j).start([(part, part, place.core)])

    def last(j):
        Flow(6, j).here(up.at[:, :, :, place.tile_cols(j)])

    steps = (merge, along_b, along_y, give_b, give_a, give_core, last)

    def head_store(n, h):
        cols = pl.ds(pl.multiple_of((2 * n + h) * W, 128), W)
        return pltpu.make_async_copy(
            d_stage.at[h, pl.ds(0, ROWS)], head_hbm.at[:, cols], local_sems.at[3 + h]
        )

    def head_tiles(n):
        def one(h, carry):
            @pl.when(n > 0)
            def _():
                head_store(n - 1, h).wait()

            cols = pl.ds(pl.multiple_of((2 * n + h) * W, 128), W)
            product = lax.dot_general(marks[...], normed[:, cols], NN, preferred_element_type=F32)
            d_stage[h, 0:ROWS] = product.astype(BF)
            head_store(n, h).start()
            return carry

        lax.fori_loop(0, 2, one, 0)

    for n in range(3, pieces + pieces // 2):
        agenda.add(2.8 * (n - 3) + 0.1, lambda n=n: piece(n))
    agenda.add(2.8 * (pieces + pieces // 2 - 3) + 4.0, cot_swap)
    began = agenda.now

    def turn(t, carry):
        @pl.when(t < NT_COLS)
        def _():
            pull(t)

        @pl.when((t >= NT_COLS) & (t < NT_COLS + TG_TURNS))
        def _():
            head_tiles(t - NT_COLS)

        for lag, step in zip(LAG, steps):
            @pl.when((t >= lag) & (t < lag + NT_COLS))
            def _():
                step(t - lag)

        for k in range(TURNS):
            due = began + 2.8 * (k + 1)
            if agenda.due(due):
                @pl.when(t == k)
                def _():
                    agenda.run(due)
                    agenda.now = max(agenda.now, due)
            agenda.now = max(agenda.now, due)
        return carry

    lax.fori_loop(0, TURNS, turn, 0)
    agenda.run()

    embed_store = pltpu.make_async_copy(found, embed_hbm, local_sems.at[0])
    embed_store.start()

    GR = 16

    def upstream(i):
        rows = pl.ds(pl.multiple_of(i * GR, 16), GR)
        down = back_rows[rows, :]
        value = decode(up[i // 4, i % 4]) * jnp.concatenate([down] * (D // 128), axis=1)
        return value, hidden[rows, :].astype(F32), inverses[rows, :]

    def gain_rows(i, total):
        value, wide, inv = upstream(i)
        product = value * wide * jnp.concatenate([inv] * (D // 128), axis=1)
        return total + (product[0:8] + product[8:16])

    part = jnp.sum(lax.fori_loop(0, 16, gain_rows, jnp.zeros((8, D), F32)), axis=0, keepdims=True)
    gain_in[y] = jnp.concatenate([part[:, i * 128 : (i + 1) * 128] for i in range(D // 128)], axis=0)

    def gain_part():
        return gain_in.at[y]

    gain_item = post.group(
        [(gain_part, gain_part, peer) for peer in place.y_peers],
        lambda: gain_in.at[0:3],
        lambda: gain_in.at[0:3],
    )
    embed_store.wait()
    for item in found_sends:
        post.sent(item)

    def grad_rows(i, carry):
        value, wide, inv = upstream(i)
        scaled_up = value * gain[...]
        mean_dot = jnp.sum(scaled_up * wide, axis=1, keepdims=True) * (1.0 / D)
        pull_back = inv * inv * inv * mean_dot
        out = jnp.concatenate([inv] * (D // 128), axis=1) * scaled_up
        out = out - wide * jnp.concatenate([pull_back] * (D // 128), axis=1)
        found[i // 4, i % 4] = out.astype(BF)
        return carry

    lax.fori_loop(0, 16, grad_rows, 0)
    grad_store = pltpu.make_async_copy(found, grad_hbm, local_sems.at[0])
    grad_store.start()
    for n in range(3):
        cot_in["swap", n].wait_recv()
    metas_out[...] = metas[...]
    for h in range(2):
        head_store(TG_TURNS - 1, h).wait()

    def drain(j, carry):
        cols = place.tile_cols(j)
        Flow(2, j).sent(sz.at[j])
        Flow(3, j).sent(sy.at[j])
        for _ in range(3):
            Flow(4, j).sent(up.at[0, 0, :, cols])
        Flow(5, j).sent(up.at[:, 0:3, :, cols])
        Flow(6, j).sent(up.at[:, :, :, cols])
        return carry

    lax.fori_loop(0, NT_COLS, drain, 0)
    for j in (NT_COLS - 2, NT_COLS - 1):
        Flow(0, j).sent(snd.at[j % 2])
        Flow(1, j).sent(sx.at[j % 2])
    post.close()
    gain_item.wait_recv()
    gain_out[...] = gain_in[0] + gain_in[1] + gain_in[2] + gain_in[3]
    grad_store.wait()


FAR = 1 << 30
SLOTS = 128


def patch_kernel(
    metas, own_cot, cot_hbm, head_hbm, out_hbm, grad, cot, left, picks, sums, rows_of, sems
):
    g = gray(lax.axis_index("dp"))
    first = lax.axis_index(DP_VOCAB) * ROWS
    for k in range(4):
        @pl.when(g == k)
        def _():
            pltpu.make_async_copy(own_cot, cot.at[k], sems.at[k]).start()

        @pl.when(g != k)
        def _():
            pltpu.make_async_copy(cot_hbm.at[k], cot.at[k], sems.at[k]).start()

    def tile(ref, i):
        return ref.at[pl.ds(i * MT, MT)]

    for i in range(NV):
        pltpu.make_async_copy(tile(head_hbm, i), tile(grad, i), sems.at[4 + i]).start()
    for k in range(4):
        local = metas[k, 0:1, :] - first
        left[k : k + 1, :] = jnp.where((local >= 0) & (local < ROWS), local, FAR)
    for k in range(4):
        pltpu.make_async_copy(own_cot, cot.at[k], sems.at[k]).wait()
    for i in range(NV):
        pltpu.make_async_copy(tile(head_hbm, i), tile(grad, i), sems.at[4 + i]).wait()

    def one_pass(lowest):
        picks[...] = jnp.zeros_like(picks)

        def more(state):
            return (state[0] < SLOTS) & (state[1] < FAR)

        def take(state):
            n, row = state
            rows_of[n] = row
            rest = left[...]
            same = rest == row
            for k in range(4):
                picks[pl.ds(n, 1), k * 256 : (k + 1) * 256] = jnp.where(same[k : k + 1], 1.0, 0.0)
            rest = jnp.where(same, FAR, rest)
            left[...] = rest
            return n + 1, jnp.min(rest)

        count, lowest = lax.while_loop(more, take, (0, lowest))
        sums[...] = lax.dot_general(
            picks[...].astype(BF), cot[...].reshape(1024, D), NN, preferred_element_type=F32
        )

        def patch(n, carry):
            row = rows_of[n]
            base = pl.multiple_of((row // 16) * 16, 16)
            old = grad[pl.ds(base, 16), :]
            new = (old.astype(F32) + sums[pl.ds(n, 1), :] * EMBED_SCALE).astype(BF)
            here = lax.broadcasted_iota(jnp.int32, (16, D), 0) == row - base
            grad[pl.ds(base, 16), :] = jnp.where(here, new, old)
            return carry

        lax.fori_loop(0, count, patch, 0)
        return lowest

    lax.while_loop(lambda lowest: lowest < FAR, one_pass, jnp.min(left[...]))
    for i in range(NV):
        pltpu.make_async_copy(tile(grad, i), tile(out_hbm, i), sems.at[4 + i]).start()
    for i in range(NV):
        pltpu.make_async_copy(tile(grad, i), tile(out_hbm, i), sems.at[4 + i]).wait()


def body(input_ids, target_ids, loss_mask, final_hidden, norm_gain, embed_cotangent, table):
    any_ = pl.BlockSpec(memory_space=pl.ANY)
    vmem = pl.BlockSpec(memory_space=pltpu.VMEM)
    dma = pltpu.SemaphoreType.DMA
    V = pltpu.VMEM
    S = jax.ShapeDtypeStruct
    meta = jnp.pad(jnp.stack([input_ids, target_ids, loss_mask]), ((0, 5), (0, 0)))
    gain = norm_gain.reshape(1, D)
    n = NT_COLS
    head, cot, metas, embed, grad, gain_grad, loss, _ = pl.pallas_call(
        main_kernel,
        out_shape=(
            S((ROWS, D), BF),
            S((4, 256, D), BF),
            S((4, 8, 256), jnp.int32),
            S((4, 4, 16, D), BF),
            S((4, 4, 16, D), BF),
            S((D // 128, 128), F32),
            S((8, 128), F32),
            S((2, ROWS, 256), F32),
        ),
        in_specs=[vmem, vmem, vmem, any_, any_],
        out_specs=(any_, any_, vmem, any_, any_, vmem, vmem, any_),
        scratch_shapes=[
            V((ROWS, D), BF),
            V((1024, D), BF),
            V((4, 8, 256), jnp.int32),
            V((ROWS, 1024), BF),
            V((4, 2, 256), F32),
            V((16, 4, 2, 256), F32),
            V((1024, 128), F32),
            V((256, 128), F32),
            V((256, 128), F32),
            V((2, 2048, W), BF),
            V((n, 4, 4, 4, 16, W), BF),
            V((n, 3, 4, 4, 16, W), BF),
            V((n, 3, 4, 16, W), BF),
            V((n, 3, 16, W), BF),
            V((4, 4, 16, D), BF),
            V((2, 2048, W), F32),
            V((2, 4, 4, 4, 16, W), I16),
            V((4, 4, 4, 4, 16, W), I16),
            V((2, 3, 4, 4, 16, W), I16),
            V((n, 3, 4, 4, 16, W), I16),
            V((n, 4, 4, 16, W), F32),
            V((n, 3, 4, 16, W), I16),
            V((n, 3, 4, 16, W), I16),
            V((n, 4, 16, W), F32),
            V((n, 3, 16, W), I16),
            V((n, 3, 16, W), I16),
            V((4, 4, 16, D), I16),
            V((4, D // 128, 128), F32),
            dma((5,)),
            dma((120,)),
            dma((120,)),
            dma((STEPS, n)),
            dma((STEPS, n)),
        ],
        compiler_params=pltpu.CompilerParams(
            collective_id=0, has_side_effects=True, vmem_limit_bytes=VMEM_LIMIT
        ),
        name="main",
    )(meta, final_hidden, gain, table, embed_cotangent)

    table_grad = pl.pallas_call(
        patch_kernel,
        out_shape=S((ROWS, D), BF),
        in_specs=[vmem, any_, any_, any_],
        out_specs=any_,
        scratch_shapes=[
            V((ROWS, D), BF),
            V((4, 256, D), BF),
            V((4, 256), jnp.int32),
            V((SLOTS, 1024), F32),
            V((SLOTS, D), F32),
            pltpu.SMEM((SLOTS,), jnp.int32),
            dma((4 + NV,)),
        ],
        compiler_params=pltpu.CompilerParams(vmem_limit_bytes=VMEM_LIMIT),
        name="patch",
    )(metas, embed_cotangent, cot, head)
    return (
        embed.reshape(256, D),
        loss[0, 0],
        grad.reshape(256, D),
        gain_grad.reshape(D),
        table_grad,
    )


def solution(mesh):
    finer = Mesh(
        mesh.devices.reshape(mesh.shape["dp"], 4, 4, 2), ("dp", "vocab_0", "vocab_1", "vocab_2")
    )
    placed = (P("dp"), P("dp"), P("dp"), P("dp", None), P(), P("dp", None), P(DP_VOCAB, None))
    return jax.shard_map(
        body,
        mesh=finer,
        in_specs=placed,
        out_specs=(P("dp", None), P(), P("dp", None), P(), P(DP_VOCAB, None)),
        check_vma=False,
    )
```

```python
import math

import jax
import jax.numpy as jnp
from jax import lax
from jax.experimental import pallas as pl
from jax.experimental.pallas import tpu as pltpu
from jax.sharding import Mesh
from jax.sharding import PartitionSpec as P

SOFTCAP = 30.0
EPSILON = 1e-06
D = 3584
ROWS = 2000
EMBED_SCALE = math.sqrt(D)
DP_VOCAB = ("dp", "vocab_0", "vocab_1", "vocab_2")
MESH = pl.DeviceIdType.MESH
BF = jnp.bfloat16
F32 = jnp.float32
I16 = jnp.int16
NT = (((1,), (1,)), ((), ()))
TN = (((0,), (0,)), ((), ()))
NN = (((1,), (0,)), ((), ()))
MT = 400
MF = 256
NV = ROWS // MT
HALF = D // 2
W = 256
NT_COLS = HALF // W
SLOTS = 32
ALL_SLOTS = 4 * SLOTS
VMEM_LIMIT = 66_900_000
TABLE_BOUND = 5.0 / math.sqrt(D) * 1.01
UNITS = 24000.0
KNEE = 256.0
FINE = 32.0


def encode(value):
    bent = jnp.clip(value, -KNEE, KNEE)
    return jnp.round(value + bent * (FINE - 1.0)).astype(jnp.int32).astype(I16)


def decode(code):
    wide = code.astype(jnp.int32).astype(F32)
    return wide - jnp.clip(wide, -KNEE * FINE, KNEE * FINE) * (1.0 - 1.0 / FINE)


def gray(i):
    return i + (i // 2) * (1 - 2 * (i % 2))


class Place:
    def __init__(self):
        self.y = y = lax.axis_index("dp")
        self.z = z = lax.axis_index("vocab_0")
        self.x = x = lax.axis_index("vocab_1")
        self.c = c = lax.axis_index("vocab_2")
        self.o = 1 - c
        self.first_row = (((y * 4 + z) * 4 + x) * 2 + c) * ROWS
        self.g = gray(y)
        self.ga = self.g + 1 - 2 * (self.g % 2)
        self.gb = (self.g + 2) % 4
        self.gc = (self.ga + 2) % 4
        self.y_a = {"dp": y + 1 - 2 * (y % 2)}
        self.y_b = {"dp": 3 - y}
        self.core = {"vocab_2": self.o}
        self.a = x + c * (z - x)
        self.b = z + c * (x - z)
        self.a_peers = [self._at((self.a + off) % 4, self.b) for off in (1, 2, 3)]
        self.b_peers = [self._at(self.a, (self.b + off) % 4) for off in (1, 2, 3)]
        self.x_peers = [{"vocab_1": (x + off) % 4} for off in (1, 2, 3)]
        self.z_peers = [{"vocab_0": (z + off) % 4} for off in (1, 2, 3)]
        self.y_peers = [{"dp": (y + off) % 4} for off in (1, 2, 3)]
        self.cols = pl.ds(pl.multiple_of(c * HALF, 128), HALF)
        self.a_at = [(self.a + off) % 4 for off in (1, 2, 3)]
        self.b_at = [(self.b + off) % 4 for off in (1, 2, 3)]
        self.y_at = [gray((y + off) % 4) for off in (1, 2, 3)]
        a, b = self.a, self.b
        a0, a1, b0 = (a + a // 2) % 2, a // 2, (b + b // 2) % 2
        self.colour = (a0 + b0) % 2 + 2 * ((a1 + b0) % 2)
        flip_a, flip_b = a + 1 - 2 * (a % 2), b + 1 - 2 * (b % 2)
        self.near = [self._at(flip_a, b), self._at(3 - a, b), self._at(a, flip_b)]

    def _at(self, a, b):
        return {"vocab_1": a + self.c * (b - a), "vocab_0": b + self.c * (a - b)}

    def tile_cols(self, j):
        return pl.ds(pl.multiple_of(self.c * HALF + j * W, 128), W)

    def first_row_of(self, k):
        return (((gray(k) * 4 + self.z) * 4 + self.x) * 2 + self.c) * ROWS

    def meet(self):
        peers = [self.core] + self.x_peers + self.z_peers + self.y_peers
        barrier = pltpu.get_barrier_semaphore()
        for peer in peers:
            pl.semaphore_signal(barrier, inc=1, device_id=peer, device_id_type=MESH)
        return lambda: pl.semaphore_wait(barrier, len(peers))


class Sent:
    def __init__(self, sems, at, out_like, in_like, times):
        self.sems, self.at = sems, at
        self.out_like, self.in_like, self.times = out_like, in_like, times

    def wait_send(self):
        for _ in range(self.times):
            like = self.out_like()
            pltpu.make_async_copy(like, like, self.sems[0].at[self.at]).wait()

    def wait_recv(self):
        like = self.in_like()
        pltpu.make_async_copy(like, like, self.sems[1].at[self.at]).wait()


class Post:
    def __init__(self, send_sems, recv_sems):
        self.sems = (send_sems, recv_sems)
        self.used = 0
        self.open = []

    def send(self, src, dst, peer):
        return self.group([(src, dst, peer)], src, dst)

    def group(self, parts, out_like, in_like, times=1):
        for src, dst, peer in parts:
            pltpu.make_async_remote_copy(
                src_ref=src(),
                dst_ref=dst(),
                send_sem=self.sems[0].at[self.used],
                recv_sem=self.sems[1].at[self.used],
                device_id=peer,
                device_id_type=MESH,
            ).start()
        sent = Sent(self.sems, self.used, out_like, in_like, times)
        self.used += 1
        self.open.append(sent)
        return sent

    def sent(self, item):
        item.wait_send()
        self.open = [c for c in self.open if c is not item]

    def close(self):
        for item in self.open:
            item.wait_send()
        self.open = []


class Agenda:
    def __init__(self):
        self.now = 0.0
        self.todo = []
        self.count = 0

    def add(self, after, step):
        self.todo.append((self.now + after, self.count, step))
        self.count += 1

    def run(self, until=None):
        while self.todo:
            self.todo.sort(key=lambda item: item[:2])
            if until is not None and self.todo[0][0] > until:
                return
            when, _, step = self.todo.pop(0)
            self.now = max(self.now, when)
            step()

    def due(self, until):
        return any(item[0] <= until for item in self.todo)

    def compute(self, cost, work):
        self.run(self.now)
        work()
        self.now += cost
        self.run(self.now)


def columns(table, j):
    left = pl.ds(pl.multiple_of(j * W, 128), W)
    right = pl.ds(pl.multiple_of(HALF + j * W, 128), W)
    return jnp.concatenate([table[:, left], table[:, right]], axis=1)


def gather_rows(place, post, agenda, buf, sends):
    a, b, cols = place.a, place.b, place.cols

    def mine():
        return buf.at[b, a, :, cols]

    def row():
        return buf.at[:, a, :, cols]

    def rows():
        return buf.at[:, 0:3, :, cols]

    def half():
        return buf.at[:, :, :, cols]

    first = post.group(
        [(mine, mine, peer) for peer in place.b_peers], mine, lambda: buf.at[0:3, 0, :, cols], 3
    )
    sends.append(first)

    def along_a():
        first.wait_recv()
        second = post.group([(row, row, peer) for peer in place.a_peers], rows, rows)
        sends.append(second)
        agenda.add(10.0, lambda: across(second))

    def across(second):
        second.wait_recv()
        third = post.send(half, half, place.core)
        sends.append(third)
        agenda.add(4.0, third.wait_recv)

    agenda.add(6.0, along_a)


STEPS = 7
LAG = (1, 4, 6, 8, 10, 12, 13)
TG_TURNS = NT_COLS
TURNS = NT_COLS + LAG[-1]


def main_kernel(
    own_ids, own_targets, own_mask, hidden, gain_in_rows, table_hbm, cot_hbm,
    head_hbm, metas_out, embed_hbm, grad_hbm, gain_out, loss_out, cap_hbm,
    table, normed, metas, gain, marks, stats, stat_in, scale_rows, back_rows, inverses,
    d_stage, d_part, d_rc, d_rx, d_rz, found, owner_of, slot_of, packed, lines, cot_packed, cot_lines,
    stage, snd, rc, sx, rx, acc, sz, rz, acc_z, sy, ry, up,
    gain_in, local_sems, send_sems, recv_sems, flow_send, flow_recv,
):
    place = Place()
    post = Post(send_sems, recv_sems)
    agenda = Agenda()
    first_row = place.first_row
    a, b, c, o, g, y = place.a, place.b, place.c, place.o, place.g, place.y
    blocks = [g, place.ga, place.gb, place.gc]
    entered = place.meet()
    table_load = pltpu.make_async_copy(table_hbm, table, local_sems.at[0])
    table_load.start()
    metas[g, 0:1, :] = own_ids[...]
    metas[g, 1:2, :] = own_targets[...]
    metas[g, 2:3, :] = own_mask[...]
    gain[...] = jnp.concatenate([gain_in_rows[i : i + 1, :] for i in range(D // 128)], axis=1)
    cot_load = pltpu.make_async_copy(cot_hbm, found, local_sems.at[3])
    cot_load.start()

    def inverse(wide):
        return lax.rsqrt(jnp.mean(wide * wide, axis=1, keepdims=True) + EPSILON)

    def rows_of(block, first, count):
        return pl.ds(pl.multiple_of(block * 256 + first, 16), count)

    quarter = place.colour

    def normalise(i, carry):
        at = ((quarter + i) % 4) * 64
        rows = pl.ds(pl.multiple_of(at, 16), 64)
        wide = hidden[rows, :].astype(F32)
        inv = inverse(wide)
        inverses[rows, :] = jnp.broadcast_to(inv, (64, 128))
        normed[rows_of(g, at, 64), :] = (wide * inv * gain[...]).astype(BF)
        return carry

    normalise(0, 0)
    stats[...] = jnp.zeros_like(stats)
    entered()

    def ship(block, first, count, peer):
        def part():
            return normed.at[rows_of(block, first, count), place.cols]

        return post.send(part, part, peer)

    at_q = quarter * 64
    meta_in = [
        post.send(lambda: metas.at[g], lambda: metas.at[g], peer) for peer in (place.y_a, place.y_b)
    ]
    a_low = ship(g, at_q, 32, place.y_a)
    b_high = ship(g, at_q + 32, 32, place.y_b)
    a_high = ship(g, at_q + 32, 32, place.y_a)
    b_low = ship(g, at_q, 32, place.y_b)
    lax.fori_loop(1, 4, normalise, 0)
    for item in meta_in:
        item.wait_recv()
    meta_c = post.send(lambda: metas.at[place.ga], lambda: metas.at[place.ga], place.y_b)
    spread = {}
    swaps = {}
    relays = []

    def relay():
        a_low.wait_recv()
        relays.append(ship(place.ga, at_q, 32, place.y_b))
        b_high.wait_recv()
        relays.append(ship(place.gb, at_q + 32, 32, place.y_a))

    def spread_block(name, block, items):
        for item in items:
            item.wait_recv()
        spread[name] = [ship(block, at_q, 64, peer) for peer in place.near]

    def swap_block(name, block):
        for item in spread[name]:
            item.wait_recv()
        swaps[name] = ship(block, 0, 256, place.core)

    def cap_store(n):
        return pltpu.make_async_copy(
            stage.at[n, pl.ds(0, ROWS)], cap_hbm.at[n], local_sems.at[1 + n]
        )

    def forward(n):
        block, side = blocks[n], n % 2
        if n >= 2:
            cap_store(side).wait()
        rows = normed[rows_of(block, 0, 256), :]
        total = jnp.zeros((1, 256), F32)
        picked = total
        for at in range(0, ROWS, MF):
            size = min(MF, ROWS - at)
            logits = lax.dot_general(table[at : at + size, :], rows, NT, preferred_element_type=F32)
            capped = SOFTCAP * jnp.tanh(logits * (1.0 / SOFTCAP))
            stage[side, at : at + size] = capped
            ids = lax.broadcasted_iota(jnp.int32, capped.shape, 0) + (first_row + at)
            hit = ids == metas[block, 1:2, :]
            total += jnp.sum(jnp.exp(capped), axis=0, keepdims=True)
            picked += jnp.sum(jnp.where(hit, capped, 0.0), axis=0, keepdims=True)
        stats[block, 0:1, :] = total
        stats[block, 1:2, :] = picked
        if n < 2:
            cap_store(side).start()

    table_load.wait()
    agenda.now = 4.5
    agenda.compute(4.0, lambda: forward(0))


    meta_c.wait_recv()
    relay()
    ids = [metas[k, 0:1, :] for k in range(4)]
    locals_ = [row - first_row for row in ids]
    for k in range(4):
        locals_.append(own_ids[...] - place.first_row_of(k))
    owned = [jnp.where((row >= 0) & (row < ROWS), 1.0, 0.0) for row in locals_]
    later = lax.broadcasted_iota(jnp.int32, (256, 256), 0) < lax.broadcasted_iota(
        jnp.int32, (256, 256), 1
    )
    ranks = lax.dot_general(
        jnp.concatenate(owned + [jnp.zeros((8, 256), F32)], axis=0).astype(BF),
        jnp.where(later, 1.0, 0.0).astype(BF),
        NN,
        preferred_element_type=F32,
    )
    numbers = lax.broadcasted_iota(jnp.int32, (SLOTS, 256), 0).astype(F32)

    def chosen(k):
        same = (numbers == ranks[k : k + 1, :]) & (owned[k] > 0.5)
        return jnp.where(same, 1.0, 0.0)

    mine = jnp.concatenate([chosen(k) for k in range(4)], axis=0).astype(BF)
    slot_of[...] = jnp.concatenate([chosen(4 + k) for k in range(4)], axis=0).astype(BF)
    digits = [jnp.right_shift(row, 6) for row in locals_[:4]]
    digits += [jnp.bitwise_and(row, 63) for row in locals_[:4]]
    digits = [jnp.where(owned[n % 4] > 0.5, row.astype(F32), 0.0) for n, row in enumerate(digits)]
    read = lax.dot_general(
        jnp.concatenate(digits + [jnp.ones((8, 256), F32)], axis=0).astype(BF),
        mine,
        NT,
        preferred_element_type=F32,
    )
    lane = lax.broadcasted_iota(jnp.int32, (1, ALL_SLOTS), 1)
    wanted = jnp.zeros((1, ALL_SLOTS), F32)
    for k in range(4):
        here = (lane >= k * SLOTS) & (lane < (k + 1) * SLOTS)
        wanted = jnp.where(here, read[k : k + 1] * 64.0 + read[4 + k : 5 + k], wanted)
    wanted = jnp.where(read[8:9] > 0.5, wanted, -1.0)

    def mark(i, carry):
        rows = pl.ds(pl.multiple_of(i * MT, 16), MT)
        at = lax.broadcasted_iota(jnp.int32, (MT, ALL_SLOTS), 0) + i * MT
        owner_of[rows, :] = jnp.where(at.astype(F32) == wanted, 1.0, 0.0).astype(BF)
        return carry

    lax.fori_loop(0, NV, mark, 0)
    starts = lax.broadcasted_iota(jnp.int32, (128, 256), 0) * ROWS
    most = jnp.float32(0.0)
    for row in ids:
        held = jnp.where((row >= starts) & (row < starts + ROWS), 1.0, 0.0)
        most = jnp.maximum(most, jnp.max(jnp.sum(held, axis=1, keepdims=True)))
    embed_scale = jnp.where(most <= SLOTS, EMBED_SCALE, 0.0)

    spread_block("a", place.ga, [a_high])
    spread_block("b", place.gb, [b_low])

    def look_up(j, carry):
        cols = pl.ds(pl.multiple_of(j * 2 * W, 128), 2 * W)
        rows = lax.dot_general(owner_of[...], table[:, cols], TN, preferred_element_type=F32)
        packed[:, :, cols] = rows.astype(BF).reshape(4, SLOTS, 2 * W)
        return carry

    lax.fori_loop(0, 3, look_up, 0)
    spread_block("c", place.gc, relays)
    cot_load.wait()

    def cot_pack(j, carry):
        cols = pl.ds(pl.multiple_of(j * 2 * W, 128), 2 * W)
        rows = lax.dot_general(
            slot_of[...], found[:, :, :, cols].reshape(256, 2 * W), NN, preferred_element_type=F32
        )
        cot_packed[:, :, cols] = rows.astype(BF).reshape(4, SLOTS, 2 * W)
        return carry

    lax.fori_loop(0, NT_COLS, cot_pack, 0)

    def exchange(src, dst):
        dst[g] = src[g]
        parts = [
            (lambda n=n: src.at[place.y_at[n]], lambda: dst.at[g], peer)
            for n, peer in enumerate(place.y_peers)
        ]
        return post.group(parts, lambda: src.at[0:3], lambda: dst.at[0:3])

    lax.fori_loop(3, NT_COLS, look_up, 0)
    line_item = exchange(packed, lines)
    cot_item = exchange(cot_packed, cot_lines)

    swap_block("a", place.ga)
    swap_block("b", place.gb)
    agenda.now = max(agenda.now, 23.0)
    swaps["a"].wait_recv()
    agenda.compute(4.3, lambda: forward(1))
    swap_block("c", place.gc)
    swaps["b"].wait_recv()
    agenda.compute(4.3, lambda: forward(2))
    swaps["c"].wait_recv()
    agenda.compute(4.3, lambda: forward(3))

    found_sends = []

    def unpack():
        line_item.wait_recv()
        cot_item.wait_recv()
        for h in range(2):
            rows = lax.dot_general(
                slot_of[...],
                lines[:, :, h * HALF : (h + 1) * HALF].reshape(ALL_SLOTS, HALF),
                TN,
                preferred_element_type=F32,
            )
            d_part[h] = rows.astype(BF).reshape(4, 4, 16, HALF)
        item = post.send(lambda: d_part.at[o], lambda: d_rc, place.core)
        agenda.add(3.5, lambda: d_merge(item))

    def d_merge(item):
        item.wait_recv()
        d_rc[...] = d_part[c] + d_rc[...]
        parts = [
            (lambda n=n: d_rc.at[:, place.a_at[n]], lambda n=n: d_rx.at[n], peer)
            for n, peer in enumerate(place.a_peers)
        ]
        item = post.group(parts, lambda: d_rx, lambda: d_rx)
        agenda.add(11.0, lambda: d_along_b(item))

    def d_along_b(item):
        item.wait_recv()
        d_rc[:, a] = (d_rc[:, a] + d_rx[0]) + (d_rx[1] + d_rx[2])
        parts = [
            (lambda n=n: d_rc.at[place.b_at[n], a], lambda n=n: d_rz.at[n], peer)
            for n, peer in enumerate(place.b_peers)
        ]
        item = post.group(parts, lambda: d_rz, lambda: d_rz)
        agenda.add(6.0, lambda: d_end(item))

    def d_end(item):
        item.wait_recv()
        row = (d_rc[b, a] + d_rz[0]) + (d_rz[1] + d_rz[2])
        found[b, a, :, place.cols] = (row.astype(F32) * EMBED_SCALE).astype(BF)
        gather_rows(place, post, agenda, found, found_sends)

    def ring_start(base, peers, at):
        stat_in[base + at] = stats[...]

        def part():
            return stat_in.at[base + at]

        def like():
            return stat_in.at[pl.ds(0, len(peers))]

        return post.group([(part, part, peer) for peer in peers], like, like)

    def ring_end(item, base, count):
        item.wait_recv()
        total = stat_in[base]
        for i in range(1, count):
            total = total + stat_in[base + i]
        stats[...] = total

    item, base, count = ring_start(0, [place.core], c), 0, 2
    for peers, at in ((place.x_peers, place.x), (place.z_peers, place.z), (place.y_peers, y)):
        ring_end(item, base, count)
        base = base + 4
        item, count = ring_start(base, peers, at), 4
    ring_end(item, base, count)
    unpack()

    def cap_load(n):
        return pltpu.make_async_copy(
            cap_hbm.at[n], stage.at[n, pl.ds(0, ROWS)], local_sems.at[1 + n]
        )

    def slopes(n):
        block, side = blocks[n], n % 2
        if n < 2:
            cap_load(n).wait()
        weight = metas[block, 2:3, :].astype(F32)
        factor = weight / stats[block, 0:1, :]
        target = metas[block, 1:2, :]
        lanes = pl.ds(pl.multiple_of(block * 256, 128), 256)

        def slab(i, carry):
            rows = pl.ds(pl.multiple_of(i * MT, 16), MT)
            ids = lax.broadcasted_iota(jnp.int32, (MT, 256), 0) + (first_row + i * MT)
            capped = stage[side, rows, :]
            hit = jnp.where(ids == target, weight, 0.0)
            ratio = capped * (1.0 / SOFTCAP)
            value = (jnp.exp(capped) * factor - hit) * (1.0 - ratio * ratio)
            marks[rows, lanes] = value.astype(BF)
            return carry

        lax.fori_loop(0, NV, slab, 0)
        if n >= 2:
            cap_load(n - 2).start()

    for n in (2, 3, 0, 1):
        agenda.compute(0.9, lambda: slopes(n))

    def bound(k):
        rest = jnp.maximum(1.0 - jnp.exp(stats[k, 1:2, :]) / stats[k, 0:1, :], 0.0)
        return TABLE_BOUND * (2.0 * rest + 1e-4)

    for k in range(4):
        turned = jnp.broadcast_to(UNITS / bound(k), (128, 256)).T
        scale_rows[k * 256 : (k + 1) * 256, :] = turned
    back_rows[...] = jnp.broadcast_to(bound(g) * (1.0 / UNITS), (128, 256)).T

    weights = [metas[k, 2:3, :].astype(F32) for k in range(4)]
    weight_sum = sum(jnp.sum(w) for w in weights)
    loss_sum = sum(
        jnp.sum(w * (jnp.log(stats[k, 0:1, :]) - stats[k, 1:2, :])) for k, w in enumerate(weights)
    )
    loss_out[0:8] = jnp.full((8, 128), loss_sum / jnp.maximum(weight_sum, 1.0), F32)
    loss_out[8:16] = jnp.full((8, 128), most, F32)
    shape = (4, 4, 4, 16, W)

    class Flow:
        def __init__(self, step, j):
            self.send_sem, self.recv_sem = flow_send.at[step, j], flow_recv.at[step, j]

        def start(self, parts):
            for src, dst, peer in parts:
                pltpu.make_async_remote_copy(
                    src_ref=src,
                    dst_ref=dst,
                    send_sem=self.send_sem,
                    recv_sem=self.recv_sem,
                    device_id=peer,
                    device_id_type=MESH,
                ).start()

        def sent(self, like):
            pltpu.make_async_copy(like, like, self.send_sem).wait()

        def here(self, like):
            pltpu.make_async_copy(like, like, self.recv_sem).wait()

    def pull(t):
        slot = t % 2

        @pl.when(t >= 2)
        def _():
            Flow(0, t - 2).sent(snd.at[slot])

        product = lax.dot_general(marks[...], columns(table, t), TN, preferred_element_type=F32)
        for side in range(2):
            for half in range(2):
                at = side * W + half * 128
                stage[slot, side * 1024 : side * 1024 + 1024, half * 128 : half * 128 + 128] = (
                    product[:, at : at + 128] * scale_rows[...]
                )
        there = pl.ds(pl.multiple_of(o * 1024, 16), 1024)
        snd[slot] = encode(stage[slot, there, :]).reshape(*shape)
        Flow(0, t).start([(snd.at[slot], rc.at[t % 4], place.core)])

    def held(slot, at):
        whole = stage.at[slot, pl.ds(pl.multiple_of(c * 1024, 16), 1024)].reshape(*shape)
        return whole[:, :, at]

    def merge(j):
        slot = j % 2
        Flow(0, j).here(rc.at[j % 4])

        @pl.when(j >= 2)
        def _():
            Flow(1, j - 2).sent(sx.at[slot])

        acc[j] = held(slot, a) + decode(rc[j % 4, :, :, a])
        parts = []
        for n, peer in enumerate(place.a_peers):
            at = place.a_at[n]
            sx[slot, n] = encode(held(slot, at) + decode(rc[j % 4, :, :, at]))
            parts.append((sx.at[slot, n], rx.at[j, n], peer))
        Flow(1, j).start(parts)

    def along_b(j):
        Flow(1, j).here(rx.at[j])
        parts = []
        for n in range(4):
            at = (b + n) % 4
            value = acc[j, :, at] + decode(rx[j, 0, :, at])
            value = value + decode(rx[j, 1, :, at]) + decode(rx[j, 2, :, at])
            if n == 0:
                acc_z[j] = value
            else:
                sz[j, n - 1] = encode(value)
                parts.append((sz.at[j, n - 1], rz.at[j, n - 1], place.b_peers[n - 1]))
        Flow(2, j).start(parts)

    def along_y(j):
        Flow(2, j).here(rz.at[j])
        acc_z[j] = acc_z[j] + decode(rz[j, 0]) + decode(rz[j, 1]) + decode(rz[j, 2])
        parts = []
        for n, peer in enumerate(place.y_peers):
            sy[j, n] = encode(acc_z[j, place.y_at[n]])
            parts.append((sy.at[j, n], ry.at[j, n], peer))
        Flow(3, j).start(parts)

    def give_b(j):
        Flow(3, j).here(ry.at[j])
        value = acc_z[j, g] + decode(ry[j, 0]) + decode(ry[j, 1]) + decode(ry[j, 2])
        cols = place.tile_cols(j)
        up[b, a, :, cols] = encode(value)
        part = up.at[b, a, :, cols]
        Flow(4, j).start([(part, part, peer) for peer in place.b_peers])

    def give_a(j):
        cols = place.tile_cols(j)
        Flow(4, j).here(up.at[0:3, 0, :, cols])
        part = up.at[:, a, :, cols]
        Flow(5, j).start([(part, part, peer) for peer in place.a_peers])

    def give_core(j):
        cols = place.tile_cols(j)
        Flow(5, j).here(up.at[:, 0:3, :, cols])
        part = up.at[:, :, :, cols]
        Flow(6, j).start([(part, part, place.core)])

    def last(j):
        Flow(6, j).here(up.at[:, :, :, place.tile_cols(j)])

    steps = (merge, along_b, along_y, give_b, give_a, give_core, last)

    def head_store(n, h):
        cols = pl.ds(pl.multiple_of((2 * n + h) * W, 128), W)
        return pltpu.make_async_copy(
            d_stage.at[h, pl.ds(0, ROWS)], head_hbm.at[:, cols], local_sems.at[3 + h]
        )

    def head_tiles(n):
        def one(h, carry):
            @pl.when(n > 0)
            def _():
                head_store(n - 1, h).wait()

            cols = pl.ds(pl.multiple_of((2 * n + h) * W, 128), W)
            product = lax.dot_general(marks[...], normed[:, cols], NN, preferred_element_type=F32)
            rows = cot_lines[:, :, cols].reshape(ALL_SLOTS, W)
            embed = lax.dot_general(owner_of[...], rows, NN, preferred_element_type=F32)
            d_stage[h, 0:ROWS] = (product + embed * embed_scale).astype(BF)
            head_store(n, h).start()
            return carry

        lax.fori_loop(0, 2, one, 0)

    began = agenda.now

    def turn(t, carry):
        @pl.when(t < NT_COLS)
        def _():
            pull(t)

        @pl.when((t >= NT_COLS) & (t < NT_COLS + TG_TURNS))
        def _():
            head_tiles(t - NT_COLS)

        for lag, step in zip(LAG, steps):
            @pl.when((t >= lag) & (t < lag + NT_COLS))
            def _():
                step(t - lag)

        for k in range(TURNS):
            due = began + 2.8 * (k + 1)
            if agenda.due(due):
                @pl.when(t == k)
                def _():
                    agenda.run(due)
                    agenda.now = max(agenda.now, due)
            agenda.now = max(agenda.now, due)
        return carry

    lax.fori_loop(0, TURNS, turn, 0)
    agenda.run()

    embed_store = pltpu.make_async_copy(found, embed_hbm, local_sems.at[0])
    embed_store.start()

    GR = 16

    def upstream(i):
        rows = pl.ds(pl.multiple_of(i * GR, 16), GR)
        down = back_rows[rows, :]
        value = decode(up[i // 4, i % 4]) * jnp.concatenate([down] * (D // 128), axis=1)
        return value, hidden[rows, :].astype(F32), inverses[rows, :]

    def gain_rows(i, total):
        value, wide, inv = upstream(i)
        product = value * wide * jnp.concatenate([inv] * (D // 128), axis=1)
        return total + (product[0:8] + product[8:16])

    part = jnp.sum(lax.fori_loop(0, 16, gain_rows, jnp.zeros((8, D), F32)), axis=0, keepdims=True)
    gain_in[y] = jnp.concatenate([part[:, i * 128 : (i + 1) * 128] for i in range(D // 128)], axis=0)

    def gain_part():
        return gain_in.at[y]

    gain_item = post.group(
        [(gain_part, gain_part, peer) for peer in place.y_peers],
        lambda: gain_in.at[0:3],
        lambda: gain_in.at[0:3],
    )
    embed_store.wait()
    for item in found_sends:
        post.sent(item)

    def grad_rows(i, carry):
        value, wide, inv = upstream(i)
        scaled_up = value * gain[...]
        mean_dot = jnp.sum(scaled_up * wide, axis=1, keepdims=True) * (1.0 / D)
        pull_back = inv * inv * inv * mean_dot
        out = jnp.concatenate([inv] * (D // 128), axis=1) * scaled_up
        out = out - wide * jnp.concatenate([pull_back] * (D // 128), axis=1)
        found[i // 4, i % 4] = out.astype(BF)
        return carry

    lax.fori_loop(0, 16, grad_rows, 0)
    grad_store = pltpu.make_async_copy(found, grad_hbm, local_sems.at[0])
    grad_store.start()
    metas_out[...] = metas[...]
    for h in range(2):
        head_store(TG_TURNS - 1, h).wait()

    def drain(j, carry):
        cols = place.tile_cols(j)
        Flow(2, j).sent(sz.at[j])
        Flow(3, j).sent(sy.at[j])
        for _ in range(3):
            Flow(4, j).sent(up.at[0, 0, :, cols])
        Flow(5, j).sent(up.at[:, 0:3, :, cols])
        Flow(6, j).sent(up.at[:, :, :, cols])
        return carry

    lax.fori_loop(0, NT_COLS, drain, 0)
    for j in (NT_COLS - 2, NT_COLS - 1):
        Flow(0, j).sent(snd.at[j % 2])
        Flow(1, j).sent(sx.at[j % 2])
    post.close()
    gain_item.wait_recv()
    gain_out[...] = gain_in[0] + gain_in[1] + gain_in[2] + gain_in[3]
    grad_store.wait()


def deliver_kernel(*refs):
    ins, outs, (small, large, sems) = refs[:3], refs[3:6], refs[6:]
    moves = [(ins[n], outs[n], small.at[n], n) for n in range(2)]
    for i in range(NV):
        rows = pl.ds(i * MT, MT)
        moves.append((ins[2].at[rows], outs[2].at[rows], large.at[rows], 2 + i))
    for src, _, buf, n in moves:
        pltpu.make_async_copy(src, buf, sems.at[n]).start()
    for src, dst, buf, n in moves:
        pltpu.make_async_copy(src, buf, sems.at[n]).wait()
        pltpu.make_async_copy(buf, dst, sems.at[n]).start()
    for _, dst, buf, n in moves:
        pltpu.make_async_copy(buf, dst, sems.at[n]).wait()


def around(array, axis):
    count = lax.axis_size(axis)
    for _ in range(count - 1):
        array = lax.ppermute(array, axis, [(i, (i + 1) % count) for i in range(count)])
        yield array


def dense_embedding(ids, embed_cotangent, table, head):
    local = ids - lax.axis_index(DP_VOCAB) * ROWS
    inside = (local >= 0) & (local < ROWS)
    rows = jnp.take(table, jnp.clip(local, 0, ROWS - 1), axis=0)
    total = jnp.where(inside[:, None], rows, 0)
    for axis in DP_VOCAB:
        total = sum(around(total, axis), total)
    g = gray(lax.axis_index("dp"))
    own = lax.dynamic_slice_in_dim(total, g * 256, 256, axis=0)
    embedded = (own.astype(F32) * EMBED_SCALE).astype(BF)
    y = lax.axis_index("dp")
    cot = lax.dynamic_update_slice_in_dim(jnp.zeros((1024, D), BF), embed_cotangent, g * 256, axis=0)
    for off, block in enumerate(around(embed_cotangent, "dp")):
        cot = lax.dynamic_update_slice_in_dim(cot, block, gray((y - off - 1) % 4) * 256, axis=0)
    where = jnp.where(inside, local, ROWS)
    part = jax.ops.segment_sum(cot.astype(F32), where, num_segments=ROWS + 1)[:ROWS]
    return embedded, (head.astype(F32) + part * EMBED_SCALE).astype(BF)


def body(input_ids, target_ids, loss_mask, final_hidden, norm_gain, embed_cotangent, table):
    any_ = pl.BlockSpec(memory_space=pl.ANY)
    vmem = pl.BlockSpec(memory_space=pltpu.VMEM)
    dma = pltpu.SemaphoreType.DMA
    V = pltpu.VMEM
    S = jax.ShapeDtypeStruct
    gain = norm_gain.reshape(D // 128, 128)
    n = NT_COLS
    head, metas, embed, grad, gain_grad, loss, _ = pl.pallas_call(
        main_kernel,
        out_shape=(
            S((ROWS, D), BF),
            S((4, 8, 256), jnp.int32),
            S((4, 4, 16, D), BF),
            S((4, 4, 16, D), BF),
            S((D // 128, 128), F32),
            S((16, 128), F32),
            S((2, ROWS, 256), F32),
        ),
        in_specs=[vmem, vmem, vmem, vmem, vmem, any_, any_],
        out_specs=(any_, vmem, any_, any_, vmem, vmem, any_),
        scratch_shapes=[
            V((ROWS, D), BF),
            V((1024, D), BF),
            V((4, 8, 256), jnp.int32),
            V((1, D), F32),
            V((ROWS, 1024), BF),
            V((4, 2, 256), F32),
            V((16, 4, 2, 256), F32),
            V((1024, 128), F32),
            V((256, 128), F32),
            V((256, 128), F32),
            V((2, 2048, W), BF),
            V((2, 4, 4, 16, HALF), BF),
            V((4, 4, 16, HALF), BF),
            V((3, 4, 16, HALF), BF),
            V((3, 16, HALF), BF),
            V((4, 4, 16, D), BF),
            V((ROWS, ALL_SLOTS), BF),
            V((ALL_SLOTS, 256), BF),
            V((4, SLOTS, D), BF),
            V((4, SLOTS, D), BF),
            V((4, SLOTS, D), BF),
            V((4, SLOTS, D), BF),
            V((2, 2048, W), F32),
            V((2, 4, 4, 4, 16, W), I16),
            V((4, 4, 4, 4, 16, W), I16),
            V((2, 3, 4, 4, 16, W), I16),
            V((n, 3, 4, 4, 16, W), I16),
            V((n, 4, 4, 16, W), F32),
            V((n, 3, 4, 16, W), I16),
            V((n, 3, 4, 16, W), I16),
            V((n, 4, 16, W), F32),
            V((n, 3, 16, W), I16),
            V((n, 3, 16, W), I16),
            V((4, 4, 16, D), I16),
            V((4, D // 128, 128), F32),
            dma((5,)),
            dma((48,)),
            dma((48,)),
            dma((STEPS, n)),
            dma((STEPS, n)),
        ],
        compiler_params=pltpu.CompilerParams(
            collective_id=0, has_side_effects=True, vmem_limit_bytes=VMEM_LIMIT
        ),
        name="main",
    )(
        input_ids.reshape(1, 256),
        target_ids.reshape(1, 256),
        loss_mask.reshape(1, 256),
        final_hidden,
        gain,
        table,
        embed_cotangent.reshape(4, 4, 16, D),
    )

    embedded, table_grad = lax.cond(
        loss[8, 0] > SLOTS,
        lambda: dense_embedding(metas[:, 0, :].reshape(1024), embed_cotangent, table, head),
        lambda: (embed.reshape(256, D), head),
    )
    embedded, grad_hidden, table_grad = pl.pallas_call(
        deliver_kernel,
        out_shape=(S((256, D), BF), S((256, D), BF), S((ROWS, D), BF)),
        in_specs=[any_] * 3,
        out_specs=(any_,) * 3,
        scratch_shapes=[V((2, 256, D), BF), V((ROWS, D), BF), dma((2 + NV,))],
        compiler_params=pltpu.CompilerParams(vmem_limit_bytes=VMEM_LIMIT),
        name="deliver",
    )(embedded, grad.reshape(256, D), table_grad)
    return (embedded, loss[0, 0], grad_hidden, gain_grad.reshape(D), table_grad)


def solution(mesh):
    finer = Mesh(
        mesh.devices.reshape(mesh.shape["dp"], 4, 4, 2), ("dp", "vocab_0", "vocab_1", "vocab_2")
    )
    placed = (P("dp"), P("dp"), P("dp"), P("dp", None), P(), P("dp", None), P(DP_VOCAB, None))
    return jax.shard_map(
        body,
        mesh=finer,
        in_specs=placed,
        out_specs=(P("dp", None), P(), P("dp", None), P(), P(DP_VOCAB, None)),
        check_vma=False,
    )
```

```python
import math

import jax
import jax.numpy as jnp
from jax import lax
from jax.experimental import pallas as pl
from jax.experimental.pallas import tpu as pltpu
from jax.sharding import Mesh
from jax.sharding import PartitionSpec as P

SOFTCAP = 30.0
EPSILON = 1e-06
D = 3584
ROWS = 2000
EMBED_SCALE = math.sqrt(D)
SCALE_HIGH = 59.75
SCALE_LOW = EMBED_SCALE - SCALE_HIGH
DP_VOCAB = ("dp", "vocab_0", "vocab_1", "vocab_2")
MESH = pl.DeviceIdType.MESH
BF = jnp.bfloat16
F32 = jnp.float32
I16 = jnp.int16
NT = (((1,), (1,)), ((), ()))
TN = (((0,), (0,)), ((), ()))
NN = (((1,), (0,)), ((), ()))
MT = 400
MF = 256
NV = ROWS // MT
HALF = D // 2
W = 256
NT_COLS = HALF // W
EARLY = 4
SLOTS = 32
ALL_SLOTS = 4 * SLOTS
VMEM_LIMIT = 66_900_000
TABLE_BOUND = 5.0 / math.sqrt(D) * 1.01
UNITS = 24000.0
KNEE = 256.0
FINE = 32.0


def encode(value):
    bent = jnp.clip(value, -KNEE, KNEE)
    return jnp.round(value + bent * (FINE - 1.0)).astype(jnp.int32).astype(I16)


def decode(code):
    wide = code.astype(jnp.int32).astype(F32)
    return wide - jnp.clip(wide, -KNEE * FINE, KNEE * FINE) * (1.0 - 1.0 / FINE)


def gray(i):
    return i + (i // 2) * (1 - 2 * (i % 2))


class Place:
    def __init__(self):
        self.y = y = lax.axis_index("dp")
        self.z = z = lax.axis_index("vocab_0")
        self.x = x = lax.axis_index("vocab_1")
        self.c = c = lax.axis_index("vocab_2")
        self.o = 1 - c
        self.first_row = (((y * 4 + z) * 4 + x) * 2 + c) * ROWS
        self.g = gray(y)
        self.ga = self.g + 1 - 2 * (self.g % 2)
        self.gb = (self.g + 2) % 4
        self.gc = (self.ga + 2) % 4
        self.y_a = {"dp": y + 1 - 2 * (y % 2)}
        self.y_b = {"dp": 3 - y}
        self.core = {"vocab_2": self.o}
        self.a = x + c * (z - x)
        self.b = z + c * (x - z)
        self.a_peers = [self._at((self.a + off) % 4, self.b) for off in (1, 2, 3)]
        self.b_peers = [self._at(self.a, (self.b + off) % 4) for off in (1, 2, 3)]
        cores = [(off, core) for off in range(4) for core in (self.c, self.o)][1:]
        self.line = [{"vocab_1": (x + off) % 4, "vocab_2": core} for off, core in cores]
        planes = [(up, over) for up in range(4) for over in range(4)][1:]
        self.sheet = [{"vocab_0": (z + up) % 4, "dp": (y + over) % 4} for up, over in planes]
        self.y_peers = [{"dp": (y + off) % 4} for off in (1, 2, 3)]
        self.cols = pl.ds(pl.multiple_of(c * HALF, 128), HALF)
        self.a_at = [(self.a + off) % 4 for off in (1, 2, 3)]
        self.b_at = [(self.b + off) % 4 for off in (1, 2, 3)]
        self.y_at = [gray((y + off) % 4) for off in (1, 2, 3)]
        a, b = self.a, self.b
        a0, a1, b0, b1 = (a + a // 2) % 2, a // 2, (b + b // 2) % 2, b // 2
        self.colours = [(a0 + third) % 2 + 2 * ((a1 + third) % 2) for third in (b0, b1)]
        flip_a, flip_b = a + 1 - 2 * (a % 2), b + 1 - 2 * (b % 2)
        first, second = self._at(flip_a, b), self._at(3 - a, b)
        self.near = [
            [first, second, self._at(a, flip_b)],
            [second, first, self._at(a, 3 - b)],
        ]
        self.parts = [
            pl.ds(pl.multiple_of(c * HALF + part * (HALF // 2), 128), HALF // 2) for part in range(2)
        ]

    def _at(self, a, b):
        return {"vocab_1": a + self.c * (b - a), "vocab_0": b + self.c * (a - b)}

    def tile_cols(self, j):
        return pl.ds(pl.multiple_of(self.c * HALF + j * W, 128), W)

    def first_row_of(self, k):
        return (((gray(k) * 4 + self.z) * 4 + self.x) * 2 + self.c) * ROWS

    def meet(self):
        peers = self.line + self.sheet
        barrier = pltpu.get_barrier_semaphore()
        for peer in peers:
            pl.semaphore_signal(barrier, inc=1, device_id=peer, device_id_type=MESH)
        return lambda: pl.semaphore_wait(barrier, len(peers))


class Sent:
    def __init__(self, sems, at, parts, out_like, in_like, times):
        self.sems, self.at, self.parts = sems, at, parts
        self.out_like, self.in_like, self.times = out_like, in_like, times

    def start(self):
        for src, dst, peer in self.parts:
            pltpu.make_async_remote_copy(
                src_ref=src(),
                dst_ref=dst(),
                send_sem=self.sems[0].at[self.at],
                recv_sem=self.sems[1].at[self.at],
                device_id=peer,
                device_id_type=MESH,
            ).start()

    def wait_send(self):
        for _ in range(self.times):
            like = self.out_like()
            pltpu.make_async_copy(like, like, self.sems[0].at[self.at]).wait()

    def wait_recv(self):
        like = self.in_like()
        pltpu.make_async_copy(like, like, self.sems[1].at[self.at]).wait()


class Post:
    def __init__(self, send_sems, recv_sems):
        self.sems = (send_sems, recv_sems)
        self.used = 0
        self.open = []

    def send(self, src, dst, peer):
        return self.group([(src, dst, peer)], src, dst)

    def group(self, parts, out_like, in_like, times=1):
        sent = self.plan(parts, out_like, in_like, times)
        sent.start()
        return sent

    def plan(self, parts, out_like, in_like, times=1):
        sent = Sent(self.sems, self.used, parts, out_like, in_like, times)
        self.used += 1
        self.open.append(sent)
        return sent

    def sent(self, item):
        item.wait_send()
        self.open = [c for c in self.open if c is not item]

    def close(self):
        for item in self.open:
            item.wait_send()
        self.open = []


class Seen:
    def wait_recv(self):
        pass


class Agenda:
    def __init__(self):
        self.now = 0.0
        self.todo = []
        self.count = 0

    def add(self, after, step):
        self.todo.append((self.now + after, self.count, step))
        self.count += 1

    def run(self, until=None):
        while self.todo:
            self.todo.sort(key=lambda item: item[:2])
            if until is not None and self.todo[0][0] > until:
                return
            when, _, step = self.todo.pop(0)
            self.now = max(self.now, when)
            step()

    def due(self, until):
        return any(item[0] <= until for item in self.todo)

    def compute(self, cost, work):
        self.run(self.now)
        work()
        self.now += cost
        self.run(self.now)


def columns(table, j, core):
    own = pl.ds(pl.multiple_of(core * HALF + j * W, 128), W)
    other = pl.ds(pl.multiple_of((1 - core) * HALF + j * W, 128), W)
    return jnp.concatenate([table[:, own], table[:, other]], axis=1)


def gather_rows(place, post, agenda, buf, sends, done):
    a, b, cols = place.a, place.b, place.cols

    def mine():
        return buf.at[b, a, :, cols]

    def row():
        return buf.at[:, a, :, cols]

    def rows():
        return buf.at[:, 0:3, :, cols]

    def half():
        return buf.at[:, :, :, cols]

    first = post.group(
        [(mine, mine, peer) for peer in place.b_peers], mine, lambda: buf.at[0:3, 0, :, cols], 3
    )
    sends.append(first)

    def along_a():
        first.wait_recv()
        second = post.group([(row, row, peer) for peer in place.a_peers], rows, rows)
        sends.append(second)
        agenda.add(14.0, lambda: across(second))

    def across(second):
        second.wait_recv()
        third = post.send(half, half, place.core)
        sends.append(third)
        agenda.add(5.0, lambda: finish(third))

    def finish(third):
        third.wait_recv()
        done()

    agenda.add(8.0, along_a)


STEPS = 8
LAG = (1, 3, 5)
TAIL_AT = ((1, 2), (4, 2), (6, 1), (8, 1), (10, 1), (12, 1), (14, 1), (15, 1))
HEAD_TILES = 2 * NT_COLS
TAIL = TAIL_AT[-1][0] + 1


def main_kernel(
    own_ids, own_targets, own_mask, hidden, gain_in_rows, table_hbm, cot_hbm,
    head_hbm, metas_out, embed_hbm, grad_hbm, gain_out, loss_out, cap_hbm,
    table, normed, metas, gain, marks, stats, stat_in, scale_rows, back_rows, inverses, dots,
    d_stage, d_part, d_rc, d_rx, d_rz, found, owner_of, slot_of, packed, lines, cot_packed,
    stage, snd, rc, sx, rx, s_two, r_two, acc, acc_two, sz, rz, acc_z, sy, ry, up,
    gain_in, local_sems, send_sems, recv_sems, flow_send, flow_recv,
):
    place = Place()
    post = Post(send_sems, recv_sems)
    agenda = Agenda()
    first_row = place.first_row
    a, b, c, o, g, y = place.a, place.b, place.c, place.o, place.g, place.y
    blocks = [g, place.ga, place.gb, place.gc]
    entered = place.meet()
    def table_load(i):
        rows = pl.ds(i * 1024, 1024 - 48 * i)
        return pltpu.make_async_copy(table_hbm.at[rows], table.at[rows], local_sems.at[5 * i])

    table_load(0).start()
    table_load(1).start()
    metas[g, 0:1, :] = own_ids[...]
    metas[g, 1:2, :] = own_targets[...]
    metas[g, 2:3, :] = own_mask[...]
    gain[...] = jnp.concatenate([gain_in_rows[i : i + 1, :] for i in range(D // 128)], axis=1)
    cot_load = pltpu.make_async_copy(cot_hbm, found, local_sems.at[3])
    cot_load.start()

    def inverse(wide):
        return lax.rsqrt(jnp.mean(wide * wide, axis=1, keepdims=True) + EPSILON)

    def rows_of(block, first, count):
        return pl.ds(pl.multiple_of(block * 256 + first, 16), count)

    def normalise(i, carry):
        at = i * 64
        rows = pl.ds(pl.multiple_of(at, 16), 64)
        wide = hidden[rows, :].astype(F32)
        inv = inverse(wide)
        inverses[rows, :] = jnp.broadcast_to(inv, (64, 128))
        normed[rows_of(g, at, 64), :] = (wide * inv * gain[...]).astype(BF)
        return carry

    lax.fori_loop(0, 4, normalise, 0)
    stats[...] = jnp.zeros_like(stats)
    entered()

    def ship(block, part, half, peer):
        def rows():
            at = place.colours[part] * 64 + half * 32
            return normed.at[rows_of(block, at, 32), place.parts[part]]

        return post.send(rows, rows, peer)

    meta_in = [
        post.send(lambda: metas.at[g], lambda: metas.at[g], peer) for peer in (place.y_a, place.y_b)
    ]
    both = (0, 1)
    a_low = [ship(g, part, 0, place.y_a) for part in both]
    b_high = [ship(g, part, 1, place.y_b) for part in both]
    a_high = [ship(g, part, 1, place.y_a) for part in both]
    b_low = [ship(g, part, 0, place.y_b) for part in both]
    meta_c = post.plan(
        [(lambda: metas.at[place.ga], lambda: metas.at[place.ga], place.y_b)],
        lambda: metas.at[place.ga],
        lambda: metas.at[place.gc],
    )
    spread = {"a": [], "b": [], "c": []}
    relays = []

    def swap(block):
        def part():
            return normed.at[rows_of(block, 0, 256), place.cols]

        return post.plan([(part, part, place.core)], part, part)

    swaps = {"a": swap(place.ga), "b": swap(place.gb), "c": swap(place.gc)}

    def spread_piece(name, block, half, items):
        for part, item in enumerate(items):
            item.wait_recv()
            spread[name] += [ship(block, part, half, peer) for peer in place.near[part]]

    def swap_block(name):
        for item in spread[name]:
            item.wait_recv()
        swaps[name].start()

    def cap_store(n):
        return pltpu.make_async_copy(
            stage.at[n, pl.ds(0, ROWS)], cap_hbm.at[n], local_sems.at[1 + n]
        )

    def forward(n, block, between):
        side = n % 2
        rows = normed[rows_of(block, 0, 256), :]
        total = jnp.zeros((1, 256), F32)
        picked = total
        for at in range(0, ROWS, MF):
            if at == 4 * MF:
                between()
            size = min(MF, ROWS - at)
            logits = lax.dot_general(table[at : at + size, :], rows, NT, preferred_element_type=F32)
            capped = SOFTCAP * jnp.tanh(logits * (1.0 / SOFTCAP))
            stage[side, at : at + size] = capped
            ids = lax.broadcasted_iota(jnp.int32, capped.shape, 0) + (first_row + at)
            hit = ids == metas[block, 1:2, :]
            total += jnp.sum(jnp.exp(capped), axis=0, keepdims=True)
            picked += jnp.sum(jnp.where(hit, capped, 0.0), axis=0, keepdims=True)
        stats[block, 0:1, :] = total
        stats[block, 1:2, :] = picked

    seen = [Seen(), Seen()]

    def pass_on():
        table_load(1).wait()
        for item in meta_in:
            item.wait_recv()
        meta_c.start()
        for part in both:
            a_low[part].wait_recv()
            b_high[part].wait_recv()
            relays.append(
                (ship(place.ga, part, 0, place.y_b), ship(place.gb, part, 1, place.y_a))
            )
        spread_piece("a", place.ga, 0, seen)

    table_load(0).wait()
    forward(0, g, pass_on)
    cap_store(0).start()
    spread_piece("a", place.ga, 1, a_high)

    meta_c.wait_recv()
    ids = [metas[k, 0:1, :] for k in range(4)]
    locals_ = [row - first_row for row in ids]
    for k in range(4):
        locals_.append(own_ids[...] - place.first_row_of(k))
    owned = [jnp.where((row >= 0) & (row < ROWS), 1.0, 0.0) for row in locals_]
    later = lax.broadcasted_iota(jnp.int32, (256, 256), 0) < lax.broadcasted_iota(
        jnp.int32, (256, 256), 1
    )
    ranks = lax.dot_general(
        jnp.concatenate(owned + [jnp.zeros((8, 256), F32)], axis=0).astype(BF),
        jnp.where(later, 1.0, 0.0).astype(BF),
        NN,
        preferred_element_type=F32,
    )
    numbers = lax.broadcasted_iota(jnp.int32, (SLOTS, 256), 0).astype(F32)

    def chosen(k):
        same = (numbers == ranks[k : k + 1, :]) & (owned[k] > 0.5)
        return jnp.where(same, 1.0, 0.0)

    mine = jnp.concatenate([chosen(k) for k in range(4)], axis=0).astype(BF)
    slot_of[...] = jnp.concatenate([chosen(4 + k) for k in range(4)], axis=0).astype(BF)
    digits = [jnp.right_shift(row, 6) for row in locals_[:4]]
    digits += [jnp.bitwise_and(row, 63) for row in locals_[:4]]
    digits = [jnp.where(owned[n % 4] > 0.5, row.astype(F32), 0.0) for n, row in enumerate(digits)]
    read = lax.dot_general(
        jnp.concatenate(digits + [jnp.ones((8, 256), F32)], axis=0).astype(BF),
        mine,
        NT,
        preferred_element_type=F32,
    )
    lane = lax.broadcasted_iota(jnp.int32, (1, ALL_SLOTS), 1)
    wanted = jnp.zeros((1, ALL_SLOTS), F32)
    for k in range(4):
        here = (lane >= k * SLOTS) & (lane < (k + 1) * SLOTS)
        wanted = jnp.where(here, read[k : k + 1] * 64.0 + read[4 + k : 5 + k], wanted)
    wanted = jnp.where(read[8:9] > 0.5, wanted, -1.0)

    starts = lax.broadcasted_iota(jnp.int32, (128, 256), 0) * ROWS
    most = jnp.float32(0.0)
    for row in ids:
        held = jnp.where((row >= starts) & (row < starts + ROWS), 1.0, 0.0)
        most = jnp.maximum(most, jnp.max(jnp.sum(held, axis=1, keepdims=True)))
    keep = jnp.where(most <= SLOTS, 1.0, 0.0)

    def mark(i, carry):
        rows = pl.ds(pl.multiple_of(i * MT, 16), MT)
        at = lax.broadcasted_iota(jnp.int32, (MT, ALL_SLOTS), 0) + i * MT
        same = at.astype(F32) == wanted
        owner_of[rows, :] = jnp.where(same, 1.0, 0.0).astype(BF)
        marks[rows, 1024:1152] = jnp.where(same, keep * SCALE_HIGH, 0.0).astype(BF)
        marks[rows, 1152:1280] = jnp.where(same, keep * SCALE_LOW, 0.0).astype(BF)
        return carry


    lax.fori_loop(0, NV, mark, 0)

    spread_piece("b", place.gb, 1, seen)
    spread_piece("b", place.gb, 0, b_low)

    def look_up(j, carry):
        cols = pl.ds(pl.multiple_of(j * 2 * W, 128), 2 * W)
        rows = lax.dot_general(owner_of[...], table[:, cols], TN, preferred_element_type=F32)
        packed[:, :, cols] = rows.astype(BF).reshape(4, SLOTS, 2 * W)
        return carry

    def exchange(src, dst):
        dst[g] = src[g]
        parts = [
            (lambda n=n: src.at[place.y_at[n]], lambda: dst.at[g], peer)
            for n, peer in enumerate(place.y_peers)
        ]
        return post.group(parts, lambda: src.at[0:3], lambda: dst.at[0:3])

    lax.fori_loop(0, EARLY, look_up, 0)
    spread_piece("c", place.gc, 0, [pair[0] for pair in relays])
    spread_piece("c", place.gc, 1, [pair[1] for pair in relays])
    swap_block("a")
    lax.fori_loop(EARLY, NT_COLS, look_up, 0)
    line_item = exchange(packed, lines)

    def cot_pack(j, carry):
        cols = pl.ds(pl.multiple_of(j * 2 * W, 128), 2 * W)
        rows = lax.dot_general(
            slot_of[...], found[:, :, :, cols].reshape(256, 2 * W), NN, preferred_element_type=F32
        )
        cot_packed[:, :, cols] = rows.astype(BF).reshape(4, SLOTS, 2 * W)
        return carry

    def later_block(n, carry):
        block = jnp.where(n == 1, place.ga, jnp.where(n == 2, place.gb, place.gc))

        @pl.when(n == 1)
        def _():
            swaps["a"].wait_recv()

        @pl.when(n == 2)
        def _():
            swaps["b"].wait_recv()
            cap_store(0).wait()

        @pl.when(n == 3)
        def _():
            swaps["c"].wait_recv()
            cap_store(1).wait()

        def between():
            @pl.when(n == 1)
            def _():
                swap_block("b")

            @pl.when(n == 2)
            def _():
                swap_block("c")

        forward(n, block, between)

        @pl.when(n == 1)
        def _():
            cap_store(1).start()

        return carry

    lax.fori_loop(1, 4, later_block, 0)

    found_sends = []

    def unpack():
        line_item.wait_recv()
        for h in range(2):
            rows = lax.dot_general(
                slot_of[...],
                lines[:, :, h * HALF : (h + 1) * HALF].reshape(ALL_SLOTS, HALF),
                TN,
                preferred_element_type=F32,
            )
            d_part[h] = rows.astype(BF).reshape(4, 4, 16, HALF)
        return post.send(lambda: d_part.at[o], lambda: d_rc, place.core)

    def d_merge(item):
        item.wait_recv()
        d_rc[...] = d_part[c] + d_rc[...]
        parts = [
            (lambda n=n: d_rc.at[:, place.a_at[n]], lambda n=n: d_rx.at[n], peer)
            for n, peer in enumerate(place.a_peers)
        ]
        item = post.group(parts, lambda: d_rx, lambda: d_rx)
        agenda.add(9.0, lambda: d_along_b(item))

    def d_along_b(item):
        item.wait_recv()
        d_rc[:, a] = (d_rc[:, a] + d_rx[0]) + (d_rx[1] + d_rx[2])
        parts = [
            (lambda n=n: d_rc.at[place.b_at[n], a], lambda n=n: d_rz.at[n], peer)
            for n, peer in enumerate(place.b_peers)
        ]
        item = post.group(parts, lambda: d_rz, lambda: d_rz)
        agenda.add(12.0, lambda: d_end(item))

    def d_end(item):
        item.wait_recv()
        row = (d_rc[b, a] + d_rz[0]) + (d_rz[1] + d_rz[2])
        found[b, a, :, place.cols] = (row.astype(F32) * EMBED_SCALE).astype(BF)
        gather_rows(place, post, agenda, found, found_sends, embed_done)

    def embed_store():
        return pltpu.make_async_copy(found, embed_hbm, local_sems.at[0])

    def embed_done():
        embed_store().start()
        for item in found_sends:
            post.sent(item)

    def ring_start(base, peers, at):
        stat_in[base + at] = stats[...]

        def part():
            return stat_in.at[base + at]

        def like():
            return stat_in.at[pl.ds(0, len(peers))]

        return post.group([(part, part, peer) for peer in peers], like, like)

    def ring_end(item, base, count):
        item.wait_recv()
        total = stat_in[base]
        for i in range(1, count):
            total = total + stat_in[base + i]
        stats[...] = total

    item = ring_start(0, place.line, place.x * 2 + c)
    half_item = unpack()
    ring_end(item, 0, 8)
    item = ring_start(8, place.sheet, place.z * 4 + y)
    cot_load.wait()
    lax.fori_loop(0, NT_COLS, cot_pack, 0)
    ring_end(item, 8, 16)
    cot_item = exchange(cot_packed, normed.at[pl.ds(1024, ALL_SLOTS)].reshape(4, SLOTS, D))
    agenda.now = 40.0
    d_merge(half_item)

    def cap_load(n):
        return pltpu.make_async_copy(
            cap_hbm.at[n], stage.at[n, pl.ds(0, ROWS)], local_sems.at[1 + n]
        )

    def slopes(n):
        block, side = blocks[n], n % 2
        if n < 2:
            cap_load(n).wait()
        weight = metas[block, 2:3, :].astype(F32)
        factor = weight / stats[block, 0:1, :]
        target = metas[block, 1:2, :]
        lanes = pl.ds(pl.multiple_of(block * 256, 128), 256)

        def slab(i, carry):
            rows = pl.ds(pl.multiple_of(i * MT, 16), MT)
            ids = lax.broadcasted_iota(jnp.int32, (MT, 256), 0) + (first_row + i * MT)
            capped = stage[side, rows, :]
            hit = jnp.where(ids == target, weight, 0.0)
            ratio = capped * (1.0 / SOFTCAP)
            value = (jnp.exp(capped) * factor - hit) * (1.0 - ratio * ratio)
            marks[rows, lanes] = value.astype(BF)
            return carry

        lax.fori_loop(0, NV, slab, 0)
        if n >= 2:
            cap_load(n - 2).start()

    for n in (2, 3, 0, 1):
        agenda.compute(0.9, lambda: slopes(n))

    def bound(k):
        rest = jnp.maximum(1.0 - jnp.exp(stats[k, 1:2, :]) / stats[k, 0:1, :], 0.0)
        return TABLE_BOUND * (2.0 * rest + 1e-4)

    for k in range(4):
        turned = jnp.broadcast_to(UNITS / bound(k), (128, 256)).T
        scale_rows[k * 256 : (k + 1) * 256, :] = turned
    back_rows[...] = jnp.broadcast_to(bound(g) * (1.0 / UNITS), (128, 256)).T

    weights = [metas[k, 2:3, :].astype(F32) for k in range(4)]
    weight_sum = sum(jnp.sum(w) for w in weights)
    loss_sum = sum(
        jnp.sum(w * (jnp.log(stats[k, 0:1, :]) - stats[k, 1:2, :])) for k, w in enumerate(weights)
    )
    loss_out[0:8] = jnp.full((8, 128), loss_sum / jnp.maximum(weight_sum, 1.0), F32)
    loss_out[8:16] = jnp.full((8, 128), most, F32)
    shape = (4, 4, 4, 16, W)

    class Flow:
        def __init__(self, step, j):
            self.send_sem, self.recv_sem = flow_send.at[step, j], flow_recv.at[step, j]

        def start(self, parts):
            for src, dst, peer in parts:
                pltpu.make_async_remote_copy(
                    src_ref=src,
                    dst_ref=dst,
                    send_sem=self.send_sem,
                    recv_sem=self.recv_sem,
                    device_id=peer,
                    device_id_type=MESH,
                ).start()

        def sent(self, like):
            pltpu.make_async_copy(like, like, self.send_sem).wait()

        def here(self, like):
            pltpu.make_async_copy(like, like, self.recv_sem).wait()

    def pull(t):
        slot = t % 2

        @pl.when(t >= 2)
        def _():
            Flow(0, t - 2).sent(snd.at[slot])

        product = lax.dot_general(
            marks[:, 0:1024], columns(table, t, c), TN, preferred_element_type=F32
        )
        for half in range(2):
            lanes = slice(half * 128, half * 128 + 128)
            other = slice(W + half * 128, W + half * 128 + 128)
            stage[slot, 0:1024, lanes] = product[:, lanes] * scale_rows[...]
            code = encode(product[:, other] * scale_rows[...])
            snd[slot, :, :, :, :, lanes] = code.reshape(4, 4, 4, 16, 128)
        Flow(0, t).start([(snd.at[slot], rc.at[t % 4], place.core)])

    def held(slot, at):
        whole = stage.at[slot, pl.ds(0, 1024)].reshape(*shape)
        return whole[:, :, at]

    near_a = (a + 1 - 2 * (a % 2), 3 - a)

    def partners(j):
        first = near_a[0] + (j % 2) * (near_a[1] - near_a[0])
        second = near_a[1] + (j % 2) * (near_a[0] - near_a[1])
        return first, second

    def merge(j):
        slot = j % 2
        first, second = partners(j)
        Flow(0, j).here(rc.at[j % 4])

        @pl.when(j >= 2)
        def _():
            Flow(1, j - 2).sent(sx.at[slot])

        for n, at in enumerate((first, (a + 2) % 4)):
            sx[slot, n] = encode(held(slot, at) + decode(rc[j % 4, :, :, at]))
        Flow(1, j).start([(sx.at[slot], rx.at[j], place._at(first, b))])
        acc[j] = held(slot, a) + decode(rc[j % 4, :, :, a])
        acc_two[j % 3] = held(slot, second) + decode(rc[j % 4, :, :, second])

    def second_half(j):
        _, second = partners(j)
        Flow(1, j).here(rx.at[j])

        @pl.when(j >= 2)
        def _():
            Flow(2, j - 2).sent(s_two.at[j % 2])

        s_two[j % 2] = encode(acc_two[j % 3] + decode(rx[j, 1]))
        Flow(2, j).start([(s_two.at[j % 2], r_two.at[j], place._at(second, b))])
        acc[j] = acc[j] + decode(rx[j, 0])

    def along_b(j):
        Flow(2, j).here(r_two.at[j])
        parts = []
        for n in range(4):
            at = (b + n) % 4
            value = acc[j, :, at] + decode(r_two[j, :, at])
            if n == 0:
                acc_z[j] = value
            else:
                sz[j, n - 1] = encode(value)
                parts.append((sz.at[j, n - 1], rz.at[j, n - 1], place.b_peers[n - 1]))
        Flow(3, j).start(parts)

    def along_y(j):
        Flow(3, j).here(rz.at[j])
        acc_z[j] = acc_z[j] + decode(rz[j, 0]) + decode(rz[j, 1]) + decode(rz[j, 2])
        parts = []
        for n, peer in enumerate(place.y_peers):
            sy[j, n] = encode(acc_z[j, place.y_at[n]])
            parts.append((sy.at[j, n], ry.at[j, n], peer))
        Flow(4, j).start(parts)

    def give_b(j):
        Flow(4, j).here(ry.at[j])
        value = acc_z[j, g] + decode(ry[j, 0]) + decode(ry[j, 1]) + decode(ry[j, 2])
        cols = place.tile_cols(j)
        up[b, a, :, cols] = encode(value)
        part = up.at[b, a, :, cols]
        Flow(5, j).start([(part, part, peer) for peer in place.b_peers])

    def give_a(j):
        cols = place.tile_cols(j)
        Flow(5, j).here(up.at[0:3, 0, :, cols])
        part = up.at[:, a, :, cols]
        Flow(6, j).start([(part, part, peer) for peer in place.a_peers])

    def give_core(j):
        cols = place.tile_cols(j)
        Flow(6, j).here(up.at[:, 0:3, :, cols])
        part = up.at[:, :, :, cols]
        Flow(7, j).start([(part, part, place.core)])

    def last(j):
        cols = place.tile_cols(j)
        Flow(7, j).here(up.at[:, :, :, cols])
        down, inv = back_rows[...], inverses[...]
        for h in range(2):
            for q in range(W // 128):
                at = h * HALF + j * W + q * 128
                cols = pl.ds(pl.multiple_of(at, 128), 128)
                value = decode(up[:, :, :, cols].reshape(256, 128)) * down
                product = value * hidden[:, cols].astype(F32)
                dots[...] += product * gain[:, cols]
                gain_in[y, pl.ds(h * (HALF // 128) + j * 2 + q, 1), :] = jnp.sum(
                    product * inv, axis=0, keepdims=True
                )

    steps = (merge, second_half, along_b, along_y, give_b, give_a, give_core, last)

    def head_store(n):
        cols = pl.ds(pl.multiple_of(n * W, 128), W)
        return pltpu.make_async_copy(
            d_stage.at[n % 2, pl.ds(0, ROWS)], head_hbm.at[:, cols], local_sems.at[3 + n % 2]
        )

    def head_tile(n):
        @pl.when(n >= 2)
        def _():
            head_store(n - 2).wait()

        cols = pl.ds(pl.multiple_of(n * W, 128), W)
        product = lax.dot_general(marks[...], normed[:, cols], NN, preferred_element_type=F32)
        d_stage[n % 2, 0:ROWS] = product.astype(BF)
        head_store(n).start()

    def take_due(t, turns, pace):
        for k in range(turns):
            due = agenda.now + pace
            if agenda.due(due):
                @pl.when(t == k)
                def _():
                    agenda.run(due)
            agenda.now = max(agenda.now, due)

    def turn(t, carry):
        pull(t)
        for lag, step in zip(LAG, steps):
            @pl.when(t >= lag)
            def _():
                step(t - lag)

        take_due(t, NT_COLS, 2.8)
        return carry

    dots[...] = jnp.zeros_like(dots)
    lax.fori_loop(0, NT_COLS, turn, 0)
    cot_item.wait_recv()
    normed[1152:1280, :] = normed[1024:1152, :]

    def tail(t, carry):
        @pl.when(t < HEAD_TILES)
        def _():
            head_tile(t)

        for n, ((at, pace), step) in enumerate(zip(TAIL_AT, steps)):
            begun = NT_COLS - LAG[n] if n < len(LAG) else 0
            ahead = at - t
            j = NT_COLS - 1 - ahead // pace

            @pl.when((ahead >= 0) & (ahead % pace == 0) & (j >= begun))
            def _():
                step(j)

        take_due(t, TAIL, 1.9)
        return carry

    lax.fori_loop(0, TAIL, tail, 0)
    agenda.run()

    GR = 16

    def upstream(i):
        rows = pl.ds(pl.multiple_of(i * GR, 16), GR)
        down = back_rows[rows, :]
        value = decode(up[i // 4, i % 4]) * jnp.concatenate([down] * (D // 128), axis=1)
        return value, hidden[rows, :].astype(F32), inverses[rows, :]

    def gain_part():
        return gain_in.at[y]

    gain_item = post.group(
        [(gain_part, gain_part, peer) for peer in place.y_peers],
        lambda: gain_in.at[0:3],
        lambda: gain_in.at[0:3],
    )
    embed_store().wait()

    def grad_rows(i, carry):
        value, wide, inv = upstream(i)
        rows = pl.ds(pl.multiple_of(i * GR, 16), GR)
        mean_dot = jnp.sum(dots[rows, :], axis=1, keepdims=True) * (1.0 / D)
        pull_back = inv * inv * inv * mean_dot
        out = jnp.concatenate([inv] * (D // 128), axis=1) * (value * gain[...])
        out = out - wide * jnp.concatenate([pull_back] * (D // 128), axis=1)
        found[i // 4, i % 4] = out.astype(BF)
        grad_store(i).start()
        return carry

    def grad_store(i):
        at = (i // 4, i % 4)
        return pltpu.make_async_copy(found.at[at], grad_hbm.at[at], local_sems.at[6])

    lax.fori_loop(0, 16, grad_rows, 0)
    metas_out[...] = metas[...]
    for n in (HEAD_TILES - 2, HEAD_TILES - 1):
        head_store(n).wait()

    def drain(j, carry):
        cols = place.tile_cols(j)
        Flow(3, j).sent(sz.at[j])
        Flow(4, j).sent(sy.at[j])
        for _ in range(3):
            Flow(5, j).sent(up.at[0, 0, :, cols])
        Flow(6, j).sent(up.at[:, 0:3, :, cols])
        Flow(7, j).sent(up.at[:, :, :, cols])
        return carry

    lax.fori_loop(0, NT_COLS, drain, 0)
    for j in (NT_COLS - 2, NT_COLS - 1):
        Flow(0, j).sent(snd.at[j % 2])
        Flow(1, j).sent(sx.at[j % 2])
        Flow(2, j).sent(s_two.at[j % 2])
    post.close()
    gain_item.wait_recv()
    gain_out[...] = gain_in[0] + gain_in[1] + gain_in[2] + gain_in[3]
    pltpu.make_async_copy(found, grad_hbm, local_sems.at[6]).wait()


def deliver_kernel(*refs):
    ins, outs, (small, large, sems) = refs[:3], refs[3:6], refs[6:]
    moves = [(ins[n], outs[n], small.at[n], n) for n in range(2)]
    for i in range(NV):
        rows = pl.ds(i * MT, MT)
        moves.append((ins[2].at[rows], outs[2].at[rows], large.at[rows], 2 + i))
    for src, _, buf, n in moves:
        pltpu.make_async_copy(src, buf, sems.at[n]).start()
    for src, dst, buf, n in moves:
        pltpu.make_async_copy(src, buf, sems.at[n]).wait()
        pltpu.make_async_copy(buf, dst, sems.at[n]).start()
    for _, dst, buf, n in moves:
        pltpu.make_async_copy(buf, dst, sems.at[n]).wait()


def around(array, axis):
    count = lax.axis_size(axis)
    for _ in range(count - 1):
        array = lax.ppermute(array, axis, [(i, (i + 1) % count) for i in range(count)])
        yield array


def dense_embedding(ids, embed_cotangent, table, head):
    local = ids - lax.axis_index(DP_VOCAB) * ROWS
    inside = (local >= 0) & (local < ROWS)
    rows = jnp.take(table, jnp.clip(local, 0, ROWS - 1), axis=0)
    total = jnp.where(inside[:, None], rows, 0)
    for axis in DP_VOCAB:
        total = sum(around(total, axis), total)
    g = gray(lax.axis_index("dp"))
    own = lax.dynamic_slice_in_dim(total, g * 256, 256, axis=0)
    embedded = (own.astype(F32) * EMBED_SCALE).astype(BF)
    y = lax.axis_index("dp")
    cot = lax.dynamic_update_slice_in_dim(jnp.zeros((1024, D), BF), embed_cotangent, g * 256, axis=0)
    for off, block in enumerate(around(embed_cotangent, "dp")):
        cot = lax.dynamic_update_slice_in_dim(cot, block, gray((y - off - 1) % 4) * 256, axis=0)
    where = jnp.where(inside, local, ROWS)
    part = jax.ops.segment_sum(cot.astype(F32), where, num_segments=ROWS + 1)[:ROWS]
    return embedded, (head.astype(F32) + part * EMBED_SCALE).astype(BF)


def body(input_ids, target_ids, loss_mask, final_hidden, norm_gain, embed_cotangent, table):
    any_ = pl.BlockSpec(memory_space=pl.ANY)
    vmem = pl.BlockSpec(memory_space=pltpu.VMEM)
    dma = pltpu.SemaphoreType.DMA
    V = pltpu.VMEM
    S = jax.ShapeDtypeStruct
    gain = norm_gain.reshape(D // 128, 128)
    n = NT_COLS
    head, metas, embed, grad, gain_grad, loss, _ = pl.pallas_call(
        main_kernel,
        out_shape=(
            S((ROWS, D), BF),
            S((4, 8, 256), jnp.int32),
            S((4, 4, 16, D), BF),
            S((4, 4, 16, D), BF),
            S((D // 128, 128), F32),
            S((16, 128), F32),
            S((2, ROWS, 256), F32),
        ),
        in_specs=[vmem, vmem, vmem, vmem, vmem, any_, any_],
        out_specs=(any_, vmem, any_, any_, vmem, vmem, any_),
        scratch_shapes=[
            V((ROWS, D), BF),
            V((1024 + 2 * ALL_SLOTS, D), BF),
            V((4, 8, 256), jnp.int32),
            V((1, D), F32),
            V((ROWS, 1024 + 2 * ALL_SLOTS), BF),
            V((4, 2, 256), F32),
            V((24, 4, 2, 256), F32),
            V((1024, 128), F32),
            V((256, 128), F32),
            V((256, 128), F32),
            V((256, 128), F32),
            V((2, 2048, W), BF),
            V((2, 4, 4, 16, HALF), BF),
            V((4, 4, 16, HALF), BF),
            V((3, 4, 16, HALF), BF),
            V((3, 16, HALF), BF),
            V((4, 4, 16, D), BF),
            V((ROWS, ALL_SLOTS), BF),
            V((ALL_SLOTS, 256), BF),
            V((4, SLOTS, D), BF),
            V((4, SLOTS, D), BF),
            V((4, SLOTS, D), BF),
            V((2, 2048, W), F32),
            V((2, 4, 4, 4, 16, W), I16),
            V((4, 4, 4, 4, 16, W), I16),
            V((2, 2, 4, 4, 16, W), I16),
            V((n, 2, 4, 4, 16, W), I16),
            V((2, 4, 4, 16, W), I16),
            V((n, 4, 4, 16, W), I16),
            V((n, 4, 4, 16, W), F32),
            V((3, 4, 4, 16, W), F32),
            V((n, 3, 4, 16, W), I16),
            V((n, 3, 4, 16, W), I16),
            V((n, 4, 16, W), F32),
            V((n, 3, 16, W), I16),
            V((n, 3, 16, W), I16),
            V((4, 4, 16, D), I16),
            V((4, D // 128, 128), F32),
            dma((7,)),
            dma((96,)),
            dma((96,)),
            dma((STEPS, n)),
            dma((STEPS, n)),
        ],
        compiler_params=pltpu.CompilerParams(
            collective_id=0, has_side_effects=True, vmem_limit_bytes=VMEM_LIMIT
        ),
        name="main",
    )(
        input_ids.reshape(1, 256),
        target_ids.reshape(1, 256),
        loss_mask.reshape(1, 256),
        final_hidden,
        gain,
        table,
        embed_cotangent.reshape(4, 4, 16, D),
    )

    embedded, table_grad = lax.cond(
        loss[8, 0] > SLOTS,
        lambda: dense_embedding(metas[:, 0, :].reshape(1024), embed_cotangent, table, head),
        lambda: (embed.reshape(256, D), head),
    )
    embedded, grad_hidden, table_grad = pl.pallas_call(
        deliver_kernel,
        out_shape=(S((256, D), BF), S((256, D), BF), S((ROWS, D), BF)),
        in_specs=[any_] * 3,
        out_specs=(any_,) * 3,
        scratch_shapes=[V((2, 256, D), BF), V((ROWS, D), BF), dma((2 + NV,))],
        compiler_params=pltpu.CompilerParams(vmem_limit_bytes=VMEM_LIMIT),
        name="deliver",
    )(embedded, grad.reshape(256, D), table_grad)
    return (embedded, loss[0, 0], grad_hidden, gain_grad.reshape(D), table_grad)


def solution(mesh):
    finer = Mesh(
        mesh.devices.reshape(mesh.shape["dp"], 4, 4, 2), ("dp", "vocab_0", "vocab_1", "vocab_2")
    )
    placed = (P("dp"), P("dp"), P("dp"), P("dp", None), P(), P("dp", None), P(DP_VOCAB, None))
    return jax.shard_map(
        body,
        mesh=finer,
        in_specs=placed,
        out_specs=(P("dp", None), P(), P("dp", None), P(), P(DP_VOCAB, None)),
        check_vma=False,
    )
```

```python
import math

import jax
import jax.numpy as jnp
from jax import lax
from jax.experimental import pallas as pl
from jax.experimental.pallas import tpu as pltpu
from jax.sharding import Mesh
from jax.sharding import PartitionSpec as P

SOFTCAP = 30.0
EPSILON = 1e-06
D = 3584
ROWS = 2000
EMBED_SCALE = math.sqrt(D)
SCALE_HIGH = 59.75
SCALE_LOW = EMBED_SCALE - SCALE_HIGH
DP_VOCAB = ("dp", "vocab_0", "vocab_1", "vocab_2")
MESH = pl.DeviceIdType.MESH
BF = jnp.bfloat16
F32 = jnp.float32
I16 = jnp.int16
NT = (((1,), (1,)), ((), ()))
TN = (((0,), (0,)), ((), ()))
NN = (((1,), (0,)), ((), ()))
MT = 400
MF = 256
NV = ROWS // MT
HALF = D // 2
W = 256
NT_COLS = HALF // W
EARLY = 4
SLOTS = 32
ALL_SLOTS = 4 * SLOTS
VMEM_LIMIT = 66_900_000
TABLE_BOUND = 5.0 / math.sqrt(D) * 1.01
UNITS = 24000.0
KNEE = 256.0
FINE = 32.0


def encode(value):
    bent = jnp.clip(value, -KNEE, KNEE)
    return jnp.round(value + bent * (FINE - 1.0)).astype(jnp.int32).astype(I16)


def decode(code):
    wide = code.astype(jnp.int32).astype(F32)
    return wide - jnp.clip(wide, -KNEE * FINE, KNEE * FINE) * (1.0 - 1.0 / FINE)


def gray(i):
    return i + (i // 2) * (1 - 2 * (i % 2))


class Place:
    def __init__(self):
        self.y = y = lax.axis_index("dp")
        self.z = z = lax.axis_index("vocab_0")
        self.x = x = lax.axis_index("vocab_1")
        self.c = c = lax.axis_index("vocab_2")
        self.o = 1 - c
        self.first_row = (((y * 4 + z) * 4 + x) * 2 + c) * ROWS
        self.g = gray(y)
        self.ga = self.g + 1 - 2 * (self.g % 2)
        self.gb = (self.g + 2) % 4
        self.gc = (self.ga + 2) % 4
        self.y_a = {"dp": y + 1 - 2 * (y % 2)}
        self.y_b = {"dp": 3 - y}
        self.core = {"vocab_2": self.o}
        self.a = x + c * (z - x)
        self.b = z + c * (x - z)
        self.a_peers = [self._at((self.a + off) % 4, self.b) for off in (1, 2, 3)]
        self.b_peers = [self._at(self.a, (self.b + off) % 4) for off in (1, 2, 3)]
        cores = [(off, core) for off in range(4) for core in (self.c, self.o)][1:]
        self.line = [{"vocab_1": (x + off) % 4, "vocab_2": core} for off, core in cores]
        planes = [(up, over) for up in range(4) for over in range(4)][1:]
        self.sheet = [{"vocab_0": (z + up) % 4, "dp": (y + over) % 4} for up, over in planes]
        self.y_peers = [{"dp": (y + off) % 4} for off in (1, 2, 3)]
        self.cols = pl.ds(pl.multiple_of(c * HALF, 128), HALF)
        self.a_at = [(self.a + off) % 4 for off in (1, 2, 3)]
        self.b_at = [(self.b + off) % 4 for off in (1, 2, 3)]
        self.y_at = [gray((y + off) % 4) for off in (1, 2, 3)]
        a, b = self.a, self.b
        a0, a1, b0, b1 = (a + a // 2) % 2, a // 2, (b + b // 2) % 2, b // 2
        self.colours = [(a0 + third) % 2 + 2 * ((a1 + third) % 2) for third in (b0, b1)]
        flip_a, flip_b = a + 1 - 2 * (a % 2), b + 1 - 2 * (b % 2)
        first, second = self._at(flip_a, b), self._at(3 - a, b)
        self.near = [
            [first, second, self._at(a, flip_b)],
            [second, first, self._at(a, 3 - b)],
        ]
        self.parts = [
            pl.ds(pl.multiple_of(c * HALF + part * (HALF // 2), 128), HALF // 2) for part in range(2)
        ]

    def _at(self, a, b):
        return {"vocab_1": a + self.c * (b - a), "vocab_0": b + self.c * (a - b)}

    def tile_cols(self, j):
        return pl.ds(pl.multiple_of(self.c * HALF + j * W, 128), W)

    def first_row_of(self, k):
        return (((gray(k) * 4 + self.z) * 4 + self.x) * 2 + self.c) * ROWS

    def meet(self):
        peers = self.line + self.sheet
        barrier = pltpu.get_barrier_semaphore()
        for peer in peers:
            pl.semaphore_signal(barrier, inc=1, device_id=peer, device_id_type=MESH)
        return lambda: pl.semaphore_wait(barrier, len(peers))


class Sent:
    def __init__(self, sems, at, parts, out_like, in_like, times):
        self.sems, self.at, self.parts = sems, at, parts
        self.out_like, self.in_like, self.times = out_like, in_like, times

    def start(self):
        for src, dst, peer in self.parts:
            pltpu.make_async_remote_copy(
                src_ref=src(),
                dst_ref=dst(),
                send_sem=self.sems[0].at[self.at],
                recv_sem=self.sems[1].at[self.at],
                device_id=peer,
                device_id_type=MESH,
            ).start()

    def wait_send(self):
        times, self.times = self.times, 0
        for _ in range(times):
            like = self.out_like()
            pltpu.make_async_copy(like, like, self.sems[0].at[self.at]).wait()

    def wait_recv(self):
        like = self.in_like()
        pltpu.make_async_copy(like, like, self.sems[1].at[self.at]).wait()


class Post:
    def __init__(self, send_sems, recv_sems):
        self.sems = (send_sems, recv_sems)
        self.used = 0
        self.open = []

    def send(self, src, dst, peer):
        return self.group([(src, dst, peer)], src, dst)

    def group(self, parts, out_like, in_like, times=1):
        sent = self.plan(parts, out_like, in_like, times)
        sent.start()
        return sent

    def plan(self, parts, out_like, in_like, times=1):
        sent = Sent(self.sems, self.used, parts, out_like, in_like, times)
        self.used += 1
        self.open.append(sent)
        return sent

    def sent(self, item):
        item.wait_send()
        self.open = [c for c in self.open if c is not item]

    def close(self):
        for item in self.open:
            item.wait_send()
        self.open = []


class Seen:
    def wait_recv(self):
        pass


class Agenda:
    def __init__(self):
        self.now = 0.0
        self.todo = []
        self.count = 0

    def add(self, after, step):
        self.todo.append((self.now + after, self.count, step))
        self.count += 1

    def run(self, until=None):
        while self.todo:
            self.todo.sort(key=lambda item: item[:2])
            if until is not None and self.todo[0][0] > until:
                return
            when, _, step = self.todo.pop(0)
            self.now = max(self.now, when)
            step()

    def due(self, until):
        return any(item[0] <= until for item in self.todo)

    def compute(self, cost, work):
        self.run(self.now)
        work()
        self.now += cost
        self.run(self.now)


def columns(table, j, core):
    own = pl.ds(pl.multiple_of(core * HALF + j * W, 128), W)
    other = pl.ds(pl.multiple_of((1 - core) * HALF + j * W, 128), W)
    return jnp.concatenate([table[:, own], table[:, other]], axis=1)


def gather_rows(place, post, agenda, buf, sends, done):
    a, b, cols = place.a, place.b, place.cols

    def mine():
        return buf.at[b, a, :, cols]

    def row():
        return buf.at[:, a, :, cols]

    def rows():
        return buf.at[:, 0:3, :, cols]

    def half():
        return buf.at[:, :, :, cols]

    first = post.group(
        [(mine, mine, peer) for peer in place.b_peers], mine, lambda: buf.at[0:3, 0, :, cols], 3
    )
    sends.append(first)

    def along_a():
        first.wait_recv()
        second = post.group([(row, row, peer) for peer in place.a_peers], rows, rows)
        sends.append(second)
        agenda.add(9.0, lambda: across(second))

    def across(second):
        second.wait_recv()
        third = post.send(half, half, place.core)
        sends.append(third)
        agenda.add(4.0, lambda: finish(third))

    def finish(third):
        third.wait_recv()
        done()

    agenda.add(13.0, along_a)


STEPS = 8
LAG = (1, 3, 5)
TAIL_AT = ((1, 2), (4, 2), (6, 1), (8, 1), (10, 1), (12, 1), (14, 0), (15, 0))
HEAD_TILES = 2 * NT_COLS
TAIL = TAIL_AT[-1][0] + 1


def main_kernel(
    ids_hbm, targets_hbm, mask_hbm, hidden_hbm, gain_hbm, table_hbm, cot_hbm,
    head_hbm, metas_out, embed_hbm, grad_hbm, gain_out, loss_out, cap_hbm,
    table, normed, metas, own_lines, hidden, gain_rows, gain, marks, stats, stat_in, scale_rows, back_rows, inverses, dots,
    d_stage, d_part, d_rc, d_rx, d_rz, found, owner_of, slot_of, packed, lines, cot_packed,
    stage, snd, rc, sx, rx, s_two, r_two, acc, acc_two, sz, rz, acc_z, sy, ry, up,
    gain_in, local_sems, send_sems, recv_sems, flow_send, flow_recv,
):
    place = Place()
    post = Post(send_sems, recv_sems)
    agenda = Agenda()
    first_row = place.first_row
    a, b, c, o, g, y = place.a, place.b, place.c, place.o, place.g, place.y
    blocks = [g, place.ga, place.gb, place.gc]
    entered = place.meet()
    early = [
        pltpu.make_async_copy(hidden_hbm, hidden, local_sems.at[7]),
        pltpu.make_async_copy(gain_hbm, gain_rows, local_sems.at[8]),
    ]
    for n, ref in enumerate((ids_hbm, targets_hbm, mask_hbm)):
        early.append(pltpu.make_async_copy(ref, own_lines.at[n], local_sems.at[9 + n]))
    for copy in early:
        copy.start()
    def table_load(i):
        rows = pl.ds(i * 1024, 1024 - 48 * i)
        return pltpu.make_async_copy(table_hbm.at[rows], table.at[rows], local_sems.at[5 * i])

    table_load(0).start()
    table_load(1).start()
    for copy in early[1:]:
        copy.wait()
    for n in range(3):
        metas[g, n : n + 1, :] = own_lines[n]
    gain[...] = jnp.concatenate([gain_rows[i : i + 1, :] for i in range(D // 128)], axis=1)
    early[0].wait()
    cot_load = pltpu.make_async_copy(cot_hbm, found, local_sems.at[3])
    cot_load.start()

    def inverse(wide):
        return lax.rsqrt(jnp.mean(wide * wide, axis=1, keepdims=True) + EPSILON)

    def rows_of(block, first, count):
        return pl.ds(pl.multiple_of(block * 256 + first, 16), count)

    def normalise(i, carry):
        at = i * 64
        rows = pl.ds(pl.multiple_of(at, 16), 64)
        wide = hidden[rows, :].astype(F32)
        inv = inverse(wide)
        inverses[rows, :] = jnp.broadcast_to(inv, (64, 128))
        normed[rows_of(g, at, 64), :] = (wide * inv * gain[...]).astype(BF)
        return carry

    lax.fori_loop(0, 4, normalise, 0)
    stats[...] = jnp.zeros_like(stats)
    entered()

    def ship(block, part, half, peer):
        def rows():
            at = place.colours[part] * 64 + half * 32
            return normed.at[rows_of(block, at, 32), place.parts[part]]

        return post.send(rows, rows, peer)

    meta_in = [
        post.send(lambda: metas.at[g], lambda: metas.at[g], peer) for peer in (place.y_a, place.y_b)
    ]
    both = (0, 1)
    a_low = [ship(g, part, 0, place.y_a) for part in both]
    b_high = [ship(g, part, 1, place.y_b) for part in both]
    a_high = [ship(g, part, 1, place.y_a) for part in both]
    b_low = [ship(g, part, 0, place.y_b) for part in both]
    meta_c = post.plan(
        [(lambda: metas.at[place.ga], lambda: metas.at[place.ga], place.y_b)],
        lambda: metas.at[place.ga],
        lambda: metas.at[place.gc],
    )
    spread = {"a": [], "b": [], "c": []}
    c_low, c_high = [], []

    def swap(block):
        def part():
            return normed.at[rows_of(block, 0, 256), place.cols]

        return post.plan([(part, part, place.core)], part, part)

    swaps = {"a": swap(place.ga), "b": swap(place.gb), "c": swap(place.gc)}

    def spread_piece(name, block, half, items):
        for part, item in enumerate(items):
            item.wait_recv()
            spread[name] += [ship(block, part, half, peer) for peer in place.near[part]]

    def swap_block(name):
        for item in spread[name]:
            item.wait_recv()
        swaps[name].start()

    def cap_store(n):
        return pltpu.make_async_copy(
            stage.at[n, pl.ds(0, ROWS)], cap_hbm.at[n], local_sems.at[1 + n]
        )

    def forward(n, block, between, later=None):
        side = n % 2
        rows = normed[rows_of(block, 0, 256), :]
        total = jnp.zeros((1, 256), F32)
        picked = total
        for at in range(0, ROWS, MF):
            if at == 4 * MF:
                between()
            if at == 6 * MF and later is not None:
                later()
            size = min(MF, ROWS - at)
            logits = lax.dot_general(table[at : at + size, :], rows, NT, preferred_element_type=F32)
            capped = SOFTCAP * jnp.tanh(logits * (1.0 / SOFTCAP))
            stage[side, at : at + size] = capped
            ids = lax.broadcasted_iota(jnp.int32, capped.shape, 0) + (first_row + at)
            hit = ids == metas[block, 1:2, :]
            total += jnp.sum(jnp.exp(capped), axis=0, keepdims=True)
            picked += jnp.sum(jnp.where(hit, capped, 0.0), axis=0, keepdims=True)
        stats[block, 0:1, :] = total
        stats[block, 1:2, :] = picked

    seen = [Seen(), Seen()]

    def pass_on():
        table_load(1).wait()
        for item in meta_in:
            item.wait_recv()
        meta_c.start()
        for part in both:
            a_low[part].wait_recv()
            c_low.append(ship(place.ga, part, 0, place.y_b))
            spread["a"] += [ship(place.ga, part, 0, peer) for peer in place.near[part]]
        for part in both:
            b_high[part].wait_recv()
            c_high.append(ship(place.gb, part, 1, place.y_a))

    table_load(0).wait()
    forward(0, g, pass_on, lambda: spread_piece("a", place.ga, 1, a_high))
    cap_store(0).start()

    meta_c.wait_recv()
    ids = [metas[k, 0:1, :] for k in range(4)]
    locals_ = [row - first_row for row in ids]
    for k in range(4):
        locals_.append(own_lines[0] - place.first_row_of(k))
    owned = [jnp.where((row >= 0) & (row < ROWS), 1.0, 0.0) for row in locals_]
    later = lax.broadcasted_iota(jnp.int32, (256, 256), 0) < lax.broadcasted_iota(
        jnp.int32, (256, 256), 1
    )
    ranks = lax.dot_general(
        jnp.concatenate(owned + [jnp.zeros((8, 256), F32)], axis=0).astype(BF),
        jnp.where(later, 1.0, 0.0).astype(BF),
        NN,
        preferred_element_type=F32,
    )
    numbers = lax.broadcasted_iota(jnp.int32, (SLOTS, 256), 0).astype(F32)

    def chosen(k):
        same = (numbers == ranks[k : k + 1, :]) & (owned[k] > 0.5)
        return jnp.where(same, 1.0, 0.0)

    mine = jnp.concatenate([chosen(k) for k in range(4)], axis=0).astype(BF)
    slot_of[...] = jnp.concatenate([chosen(4 + k) for k in range(4)], axis=0).astype(BF)
    digits = [jnp.right_shift(row, 6) for row in locals_[:4]]
    digits += [jnp.bitwise_and(row, 63) for row in locals_[:4]]
    digits = [jnp.where(owned[n % 4] > 0.5, row.astype(F32), 0.0) for n, row in enumerate(digits)]
    read = lax.dot_general(
        jnp.concatenate(digits + [jnp.ones((8, 256), F32)], axis=0).astype(BF),
        mine,
        NT,
        preferred_element_type=F32,
    )
    lane = lax.broadcasted_iota(jnp.int32, (1, ALL_SLOTS), 1)
    wanted = jnp.zeros((1, ALL_SLOTS), F32)
    for k in range(4):
        here = (lane >= k * SLOTS) & (lane < (k + 1) * SLOTS)
        wanted = jnp.where(here, read[k : k + 1] * 64.0 + read[4 + k : 5 + k], wanted)
    wanted = jnp.where(read[8:9] > 0.5, wanted, -1.0)

    starts = lax.broadcasted_iota(jnp.int32, (128, 256), 0) * ROWS
    most = jnp.float32(0.0)
    for row in ids:
        held = jnp.where((row >= starts) & (row < starts + ROWS), 1.0, 0.0)
        most = jnp.maximum(most, jnp.max(jnp.sum(held, axis=1, keepdims=True)))
    keep = jnp.where(most <= SLOTS, 1.0, 0.0)

    def mark(i, carry):
        rows = pl.ds(pl.multiple_of(i * MT, 16), MT)
        at = lax.broadcasted_iota(jnp.int32, (MT, ALL_SLOTS), 0) + i * MT
        same = at.astype(F32) == wanted
        owner_of[rows, :] = jnp.where(same, 1.0, 0.0).astype(BF)
        marks[rows, 1024:1152] = jnp.where(same, keep * SCALE_HIGH, 0.0).astype(BF)
        marks[rows, 1152:1280] = jnp.where(same, keep * SCALE_LOW, 0.0).astype(BF)
        return carry


    lax.fori_loop(0, NV, mark, 0)

    def look_up(j, carry):
        cols = pl.ds(pl.multiple_of(j * 2 * W, 128), 2 * W)
        rows = lax.dot_general(owner_of[...], table[:, cols], TN, preferred_element_type=F32)
        packed[:, :, cols] = rows.astype(BF).reshape(4, SLOTS, 2 * W)
        return carry

    def exchange(src, dst):
        dst[g] = src[g]
        parts = [
            (lambda n=n: src.at[place.y_at[n]], lambda: dst.at[g], peer)
            for n, peer in enumerate(place.y_peers)
        ]
        return post.group(parts, lambda: src.at[0:3], lambda: dst.at[0:3])

    spread_piece("b", place.gb, 1, seen)
    spread_piece("b", place.gb, 0, b_low)
    lax.fori_loop(0, EARLY, look_up, 0)
    swap_block("a")
    spread_piece("c", place.gc, 0, c_low)
    spread_piece("c", place.gc, 1, c_high)
    lax.fori_loop(EARLY, NT_COLS, look_up, 0)
    line_item = exchange(packed, lines)

    def cot_pack(j, carry):
        cols = pl.ds(pl.multiple_of(j * 2 * W, 128), 2 * W)
        rows = lax.dot_general(
            slot_of[...], found[:, :, :, cols].reshape(256, 2 * W), NN, preferred_element_type=F32
        )
        cot_packed[:, :, cols] = rows.astype(BF).reshape(4, SLOTS, 2 * W)
        return carry

    def later_block(n, carry):
        block = jnp.where(n == 1, place.ga, jnp.where(n == 2, place.gb, place.gc))

        @pl.when(n == 1)
        def _():
            swaps["a"].wait_recv()

        @pl.when(n == 2)
        def _():
            swaps["b"].wait_recv()
            cap_store(0).wait()

        @pl.when(n == 3)
        def _():
            swaps["c"].wait_recv()
            cap_store(1).wait()

        def between():
            @pl.when(n == 1)
            def _():
                swap_block("b")

            @pl.when(n == 2)
            def _():
                swap_block("c")

        forward(n, block, between)

        @pl.when(n == 1)
        def _():
            cap_store(1).start()

        return carry

    lax.fori_loop(1, 4, later_block, 0)

    found_sends = []

    def unpack():
        line_item.wait_recv()
        for h in range(2):
            rows = lax.dot_general(
                slot_of[...],
                lines[:, :, h * HALF : (h + 1) * HALF].reshape(ALL_SLOTS, HALF),
                TN,
                preferred_element_type=F32,
            )
            d_part[h] = rows.astype(BF).reshape(4, 4, 16, HALF)
        return post.send(lambda: d_part.at[o], lambda: d_rc, place.core)

    def d_merge(item):
        item.wait_recv()
        d_rc[...] = d_part[c] + d_rc[...]
        parts = [
            (lambda n=n: d_rc.at[:, place.a_at[n]], lambda n=n: d_rx.at[n], peer)
            for n, peer in enumerate(place.a_peers)
        ]
        item = post.group(parts, lambda: d_rx, lambda: d_rx)
        agenda.add(9.0, lambda: d_along_b(item))

    def d_along_b(item):
        item.wait_recv()
        d_rc[:, a] = (d_rc[:, a] + d_rx[0]) + (d_rx[1] + d_rx[2])
        parts = [
            (lambda n=n: d_rc.at[place.b_at[n], a], lambda n=n: d_rz.at[n], peer)
            for n, peer in enumerate(place.b_peers)
        ]
        item = post.group(parts, lambda: d_rz, lambda: d_rz)
        agenda.add(12.0, lambda: d_end(item))

    def d_end(item):
        item.wait_recv()
        row = (d_rc[b, a] + d_rz[0]) + (d_rz[1] + d_rz[2])
        found[b, a, :, place.cols] = (row.astype(F32) * EMBED_SCALE).astype(BF)
        gather_rows(place, post, agenda, found, found_sends, embed_done)

    def embed_store():
        return pltpu.make_async_copy(found, embed_hbm, local_sems.at[0])

    def embed_done():
        embed_store().start()
        for item in found_sends:
            post.sent(item)

    def ring_start(base, peers, at):
        stat_in[base + at] = stats[...]

        def part():
            return stat_in.at[base + at]

        def like():
            return stat_in.at[pl.ds(0, len(peers))]

        return post.group([(part, part, peer) for peer in peers], like, like)

    def ring_end(item, base, count):
        item.wait_recv()
        total = stat_in[base]
        for i in range(1, count):
            total = total + stat_in[base + i]
        stats[...] = total

    item = ring_start(0, place.line, place.x * 2 + c)
    half_item = unpack()
    ring_end(item, 0, 8)
    item = ring_start(8, place.sheet, place.z * 4 + y)
    cot_load.wait()
    lax.fori_loop(0, NT_COLS, cot_pack, 0)
    ring_end(item, 8, 16)
    cot_item = exchange(cot_packed, normed.at[pl.ds(1024, ALL_SLOTS)].reshape(4, SLOTS, D))
    agenda.now = 40.0
    d_merge(half_item)

    def cap_load(n):
        return pltpu.make_async_copy(
            cap_hbm.at[n], stage.at[n, pl.ds(0, ROWS)], local_sems.at[1 + n]
        )

    def slopes(n):
        block, side = blocks[n], n % 2
        if n < 2:
            cap_load(n).wait()
        weight = metas[block, 2:3, :].astype(F32)
        factor = weight / stats[block, 0:1, :]
        target = metas[block, 1:2, :]
        lanes = pl.ds(pl.multiple_of(block * 256, 128), 256)

        def slab(i, carry):
            rows = pl.ds(pl.multiple_of(i * MT, 16), MT)
            ids = lax.broadcasted_iota(jnp.int32, (MT, 256), 0) + (first_row + i * MT)
            capped = stage[side, rows, :]
            hit = jnp.where(ids == target, weight, 0.0)
            ratio = capped * (1.0 / SOFTCAP)
            value = (jnp.exp(capped) * factor - hit) * (1.0 - ratio * ratio)
            marks[rows, lanes] = value.astype(BF)
            return carry

        lax.fori_loop(0, NV, slab, 0)
        if n >= 2:
            cap_load(n - 2).start()

    for n in (2, 3, 0, 1):
        agenda.compute(0.9, lambda: slopes(n))

    def bound(k):
        rest = jnp.maximum(1.0 - jnp.exp(stats[k, 1:2, :]) / stats[k, 0:1, :], 0.0)
        return TABLE_BOUND * (2.0 * rest + 1e-4)

    for k in range(4):
        turned = jnp.broadcast_to(UNITS / bound(k), (128, 256)).T
        scale_rows[k * 256 : (k + 1) * 256, :] = turned
    back_rows[...] = jnp.broadcast_to(bound(g) * (1.0 / UNITS), (128, 256)).T

    weights = [metas[k, 2:3, :].astype(F32) for k in range(4)]
    weight_sum = sum(jnp.sum(w) for w in weights)
    loss_sum = sum(
        jnp.sum(w * (jnp.log(stats[k, 0:1, :]) - stats[k, 1:2, :])) for k, w in enumerate(weights)
    )
    loss_out[0:8] = jnp.full((8, 128), loss_sum / jnp.maximum(weight_sum, 1.0), F32)
    loss_out[8:16] = jnp.full((8, 128), most, F32)
    shape = (4, 4, 4, 16, W)

    class Flow:
        def __init__(self, step, j):
            self.send_sem, self.recv_sem = flow_send.at[step, j], flow_recv.at[step, j]

        def start(self, parts):
            for src, dst, peer in parts:
                pltpu.make_async_remote_copy(
                    src_ref=src,
                    dst_ref=dst,
                    send_sem=self.send_sem,
                    recv_sem=self.recv_sem,
                    device_id=peer,
                    device_id_type=MESH,
                ).start()

        def sent(self, like):
            pltpu.make_async_copy(like, like, self.send_sem).wait()

        def here(self, like):
            pltpu.make_async_copy(like, like, self.recv_sem).wait()

    def pull(t):
        slot = t % 2

        @pl.when(t >= 2)
        def _():
            Flow(0, t - 2).sent(snd.at[slot])

        product = lax.dot_general(
            marks[:, 0:1024], columns(table, t, c), TN, preferred_element_type=F32
        )
        for half in range(2):
            lanes = slice(half * 128, half * 128 + 128)
            other = slice(W + half * 128, W + half * 128 + 128)
            stage[slot, 0:1024, lanes] = product[:, lanes] * scale_rows[...]
            code = encode(product[:, other] * scale_rows[...])
            snd[slot, :, :, :, :, lanes] = code.reshape(4, 4, 4, 16, 128)
        Flow(0, t).start([(snd.at[slot], rc.at[t % 4], place.core)])

    def held(slot, at):
        whole = stage.at[slot, pl.ds(0, 1024)].reshape(*shape)
        return whole[:, :, at]

    near_a = (a + 1 - 2 * (a % 2), 3 - a)

    def partners(j):
        first = near_a[0] + (j % 2) * (near_a[1] - near_a[0])
        second = near_a[1] + (j % 2) * (near_a[0] - near_a[1])
        return first, second

    def merge(j):
        slot = j % 2
        first, second = partners(j)
        Flow(0, j).here(rc.at[j % 4])

        @pl.when(j >= 2)
        def _():
            Flow(1, j - 2).sent(sx.at[slot])

        for n, at in enumerate((first, (a + 2) % 4)):
            sx[slot, n] = encode(held(slot, at) + decode(rc[j % 4, :, :, at]))
        Flow(1, j).start([(sx.at[slot], rx.at[j], place._at(first, b))])
        acc[j] = held(slot, a) + decode(rc[j % 4, :, :, a])
        acc_two[j % 3] = held(slot, second) + decode(rc[j % 4, :, :, second])

    def second_half(j):
        _, second = partners(j)
        Flow(1, j).here(rx.at[j])

        @pl.when(j >= 2)
        def _():
            Flow(2, j - 2).sent(s_two.at[j % 2])

        s_two[j % 2] = encode(acc_two[j % 3] + decode(rx[j, 1]))
        Flow(2, j).start([(s_two.at[j % 2], r_two.at[j], place._at(second, b))])
        acc[j] = acc[j] + decode(rx[j, 0])

    def along_y(j):
        Flow(2, j).here(r_two.at[j])
        acc_z[j] = acc[j, g] + decode(r_two[j, g])
        parts = []
        for n, peer in enumerate(place.y_peers):
            at = place.y_at[n]
            sz[j, n] = encode(acc[j, at] + decode(r_two[j, at]))
            parts.append((sz.at[j, n], rz.at[j, n], peer))
        Flow(3, j).start(parts)

    def along_b(j):
        Flow(3, j).here(rz.at[j])
        acc_z[j] = acc_z[j] + decode(rz[j, 0]) + decode(rz[j, 1]) + decode(rz[j, 2])
        parts = []
        for n, peer in enumerate(place.b_peers):
            sy[j, n] = encode(acc_z[j, place.b_at[n]])
            parts.append((sy.at[j, n], ry.at[j, n], peer))
        Flow(4, j).start(parts)

    def give_b(j):
        Flow(4, j).here(ry.at[j])
        value = acc_z[j, b] + decode(ry[j, 0]) + decode(ry[j, 1]) + decode(ry[j, 2])
        cols = place.tile_cols(j)
        up[b, a, :, cols] = encode(value)
        part = up.at[b, a, :, cols]
        Flow(5, j).start([(part, part, peer) for peer in place.b_peers])

    def give_a(j):
        cols = place.tile_cols(j)
        Flow(5, j).here(up.at[0:3, 0, :, cols])
        part = up.at[:, a, :, cols]
        Flow(6, j).start([(part, part, peer) for peer in place.a_peers])

    def give_core(j):
        cols = place.tile_cols(j)
        Flow(6, j).here(up.at[:, 0:3, :, cols])
        part = up.at[:, :, :, cols]
        Flow(7, j).start([(part, part, place.core)])

    def last(j):
        cols = place.tile_cols(j)
        Flow(7, j).here(up.at[:, :, :, cols])
        down, inv = back_rows[...], inverses[...]
        for h in range(2):
            for q in range(W // 128):
                at = h * HALF + j * W + q * 128
                cols = pl.ds(pl.multiple_of(at, 128), 128)
                value = decode(up[:, :, :, cols].reshape(256, 128)) * down
                product = value * hidden[:, cols].astype(F32)
                dots[...] += product * gain[:, cols]
                gain_in[y, pl.ds(h * (HALF // 128) + j * 2 + q, 1), :] = jnp.sum(
                    product * inv, axis=0, keepdims=True
                )

    steps = (merge, second_half, along_y, along_b, give_b, give_a, give_core, last)

    def head_store(n):
        cols = pl.ds(pl.multiple_of(n * W, 128), W)
        return pltpu.make_async_copy(
            d_stage.at[n % 2, pl.ds(0, ROWS)], head_hbm.at[:, cols], local_sems.at[3 + n % 2]
        )

    def head_tile(n):
        @pl.when(n >= 2)
        def _():
            head_store(n - 2).wait()

        cols = pl.ds(pl.multiple_of(n * W, 128), W)
        product = lax.dot_general(marks[...], normed[:, cols], NN, preferred_element_type=F32)
        d_stage[n % 2, 0:ROWS] = product.astype(BF)
        head_store(n).start()

    def take_due(t, turns, pace):
        for k in range(turns):
            due = agenda.now + pace
            if agenda.due(due):
                @pl.when(t == k)
                def _():
                    agenda.run(due)
            agenda.now = max(agenda.now, due)

    def turn(t, carry):
        pull(t)
        for lag, step in zip(LAG, steps):
            @pl.when(t >= lag)
            def _():
                step(t - lag)

        take_due(t, NT_COLS, 2.8)
        return carry

    dots[...] = jnp.zeros_like(dots)
    lax.fori_loop(0, NT_COLS, turn, 0)
    cot_item.wait_recv()
    normed[1152:1280, :] = normed[1024:1152, :]

    agenda.add(22.0, post.close)

    def tail(t, carry):
        @pl.when(t < HEAD_TILES)
        def _():
            head_tile(t)

        for n, ((at, pace), step) in enumerate(zip(TAIL_AT, steps)):
            if pace == 0:
                for q in range(2):
                    j = NT_COLS - 1 - 2 * (at - t) + q

                    @pl.when((j >= 0) & (j < NT_COLS))
                    def _():
                        step(j)

                continue
            begun = NT_COLS - LAG[n] if n < len(LAG) else 0
            ahead = at - t
            j = NT_COLS - 1 - ahead // pace

            @pl.when((ahead >= 0) & (ahead % pace == 0) & (j >= begun))
            def _():
                step(j)

        take_due(t, TAIL, 1.9)
        return carry

    lax.fori_loop(0, TAIL, tail, 0)
    agenda.run()

    GR = 16

    def upstream(i):
        rows = pl.ds(pl.multiple_of(i * GR, 16), GR)
        down = back_rows[rows, :]
        value = decode(up[i // 4, i % 4]) * jnp.concatenate([down] * (D // 128), axis=1)
        return value, hidden[rows, :].astype(F32), inverses[rows, :]

    def gain_part():
        return gain_in.at[y]

    gain_item = post.group(
        [(gain_part, gain_part, peer) for peer in place.y_peers],
        lambda: gain_in.at[0:3],
        lambda: gain_in.at[0:3],
    )

    def grad_rows(i, carry):
        value, wide, inv = upstream(i)
        rows = pl.ds(pl.multiple_of(i * GR, 16), GR)
        mean_dot = jnp.sum(dots[rows, :], axis=1, keepdims=True) * (1.0 / D)
        pull_back = inv * inv * inv * mean_dot
        out = jnp.concatenate([inv] * (D // 128), axis=1) * (value * gain[...])
        out = out - wide * jnp.concatenate([pull_back] * (D // 128), axis=1)
        normed[rows, :] = out.astype(BF)
        pltpu.make_async_copy(normed.at[rows], grad_hbm.at[rows], local_sems.at[6]).start()
        return carry

    lax.fori_loop(0, 16, grad_rows, 0)
    metas_out[...] = metas[...]
    for n in (HEAD_TILES - 2, HEAD_TILES - 1):
        head_store(n).wait()

    def drain(j, carry):
        cols = place.tile_cols(j)
        Flow(3, j).sent(sz.at[j])
        Flow(4, j).sent(sy.at[j])
        for _ in range(3):
            Flow(5, j).sent(up.at[0, 0, :, cols])
        Flow(6, j).sent(up.at[:, 0:3, :, cols])
        Flow(7, j).sent(up.at[:, :, :, cols])
        return carry

    lax.fori_loop(0, NT_COLS, drain, 0)
    for j in (NT_COLS - 2, NT_COLS - 1):
        Flow(0, j).sent(snd.at[j % 2])
        Flow(1, j).sent(sx.at[j % 2])
        Flow(2, j).sent(s_two.at[j % 2])
    post.close()
    gain_item.wait_recv()
    gain_out[...] = gain_in[0] + gain_in[1] + gain_in[2] + gain_in[3]
    embed_store().wait()
    pltpu.make_async_copy(normed.at[pl.ds(0, 256)], grad_hbm, local_sems.at[6]).wait()


def deliver_kernel(*refs):
    ins, outs, (small, large, sems) = refs[:3], refs[3:6], refs[6:]
    moves = [(ins[n], outs[n], small.at[n], n) for n in range(2)]
    for i in range(NV):
        rows = pl.ds(i * MT, MT)
        moves.append((ins[2].at[rows], outs[2].at[rows], large.at[rows], 2 + i))
    for src, _, buf, n in moves:
        pltpu.make_async_copy(src, buf, sems.at[n]).start()
    for src, dst, buf, n in moves:
        pltpu.make_async_copy(src, buf, sems.at[n]).wait()
        pltpu.make_async_copy(buf, dst, sems.at[n]).start()
    for _, dst, buf, n in moves:
        pltpu.make_async_copy(buf, dst, sems.at[n]).wait()


def around(array, axis):
    count = lax.axis_size(axis)
    for _ in range(count - 1):
        array = lax.ppermute(array, axis, [(i, (i + 1) % count) for i in range(count)])
        yield array


def dense_embedding(ids, embed_cotangent, table, head):
    local = ids - lax.axis_index(DP_VOCAB) * ROWS
    inside = (local >= 0) & (local < ROWS)
    rows = jnp.take(table, jnp.clip(local, 0, ROWS - 1), axis=0)
    total = jnp.where(inside[:, None], rows, 0)
    for axis in DP_VOCAB:
        total = sum(around(total, axis), total)
    g = gray(lax.axis_index("dp"))
    own = lax.dynamic_slice_in_dim(total, g * 256, 256, axis=0)
    embedded = (own.astype(F32) * EMBED_SCALE).astype(BF)
    y = lax.axis_index("dp")
    cot = lax.dynamic_update_slice_in_dim(jnp.zeros((1024, D), BF), embed_cotangent, g * 256, axis=0)
    for off, block in enumerate(around(embed_cotangent, "dp")):
        cot = lax.dynamic_update_slice_in_dim(cot, block, gray((y - off - 1) % 4) * 256, axis=0)
    where = jnp.where(inside, local, ROWS)
    part = jax.ops.segment_sum(cot.astype(F32), where, num_segments=ROWS + 1)[:ROWS]
    return embedded, (head.astype(F32) + part * EMBED_SCALE).astype(BF)


def body(input_ids, target_ids, loss_mask, final_hidden, norm_gain, embed_cotangent, table):
    any_ = pl.BlockSpec(memory_space=pl.ANY)
    vmem = pl.BlockSpec(memory_space=pltpu.VMEM)
    dma = pltpu.SemaphoreType.DMA
    V = pltpu.VMEM
    S = jax.ShapeDtypeStruct
    gain = norm_gain.reshape(D // 128, 128)
    n = NT_COLS
    head, metas, embed, grad, gain_grad, loss, _ = pl.pallas_call(
        main_kernel,
        out_shape=(
            S((ROWS, D), BF),
            S((4, 8, 256), jnp.int32),
            S((4, 4, 16, D), BF),
            S((256, D), BF),
            S((D // 128, 128), F32),
            S((16, 128), F32),
            S((2, ROWS, 256), F32),
        ),
        in_specs=[any_] * 7,
        out_specs=(any_, vmem, any_, any_, vmem, vmem, any_),
        scratch_shapes=[
            V((ROWS, D), BF),
            V((1024 + 2 * ALL_SLOTS, D), BF),
            V((4, 8, 256), jnp.int32),
            V((3, 1, 256), jnp.int32),
            V((256, D), BF),
            V((D // 128, 128), F32),
            V((1, D), F32),
            V((ROWS, 1024 + 2 * ALL_SLOTS), BF),
            V((4, 2, 256), F32),
            V((24, 4, 2, 256), F32),
            V((1024, 128), F32),
            V((256, 128), F32),
            V((256, 128), F32),
            V((256, 128), F32),
            V((2, 2048, W), BF),
            V((2, 4, 4, 16, HALF), BF),
            V((4, 4, 16, HALF), BF),
            V((3, 4, 16, HALF), BF),
            V((3, 16, HALF), BF),
            V((4, 4, 16, D), BF),
            V((ROWS, ALL_SLOTS), BF),
            V((ALL_SLOTS, 256), BF),
            V((4, SLOTS, D), BF),
            V((4, SLOTS, D), BF),
            V((4, SLOTS, D), BF),
            V((2, 2048, W), F32),
            V((2, 4, 4, 4, 16, W), I16),
            V((4, 4, 4, 4, 16, W), I16),
            V((2, 2, 4, 4, 16, W), I16),
            V((n, 2, 4, 4, 16, W), I16),
            V((2, 4, 4, 16, W), I16),
            V((n, 4, 4, 16, W), I16),
            V((n, 4, 4, 16, W), F32),
            V((3, 4, 4, 16, W), F32),
            V((n, 3, 4, 16, W), I16),
            V((n, 3, 4, 16, W), I16),
            V((n, 4, 16, W), F32),
            V((n, 3, 16, W), I16),
            V((n, 3, 16, W), I16),
            V((4, 4, 16, D), I16),
            V((4, D // 128, 128), F32),
            dma((12,)),
            dma((96,)),
            dma((96,)),
            dma((STEPS, n)),
            dma((STEPS, n)),
        ],
        compiler_params=pltpu.CompilerParams(
            collective_id=0, has_side_effects=True, vmem_limit_bytes=VMEM_LIMIT
        ),
        name="main",
    )(
        input_ids.reshape(1, 256),
        target_ids.reshape(1, 256),
        loss_mask.reshape(1, 256),
        final_hidden,
        gain,
        table,
        embed_cotangent.reshape(4, 4, 16, D),
    )

    embedded, table_grad = lax.cond(
        loss[8, 0] > SLOTS,
        lambda: dense_embedding(metas[:, 0, :].reshape(1024), embed_cotangent, table, head),
        lambda: (embed.reshape(256, D), head),
    )
    embedded, grad_hidden, table_grad = pl.pallas_call(
        deliver_kernel,
        out_shape=(S((256, D), BF), S((256, D), BF), S((ROWS, D), BF)),
        in_specs=[any_] * 3,
        out_specs=(any_,) * 3,
        scratch_shapes=[V((2, 256, D), BF), V((ROWS, D), BF), dma((2 + NV,))],
        compiler_params=pltpu.CompilerParams(vmem_limit_bytes=VMEM_LIMIT),
        name="deliver",
    )(embedded, grad, table_grad)
    return (embedded, loss[0, 0], grad_hidden, gain_grad.reshape(D), table_grad)


def solution(mesh):
    finer = Mesh(
        mesh.devices.reshape(mesh.shape["dp"], 4, 4, 2), ("dp", "vocab_0", "vocab_1", "vocab_2")
    )
    placed = (P("dp"), P("dp"), P("dp"), P("dp", None), P(), P("dp", None), P(DP_VOCAB, None))
    return jax.shard_map(
        body,
        mesh=finer,
        in_specs=placed,
        out_specs=(P("dp", None), P(), P("dp", None), P(), P(DP_VOCAB, None)),
        check_vma=False,
    )
```

```python
import math

import jax
import jax.numpy as jnp
from jax import lax
from jax.experimental import pallas as pl
from jax.experimental.pallas import tpu as pltpu
from jax.sharding import Mesh
from jax.sharding import PartitionSpec as P

SOFTCAP = 30.0
EPSILON = 1e-06
D = 3584
ROWS = 2000
EMBED_SCALE = math.sqrt(D)
SCALE_HIGH = 59.75
SCALE_LOW = EMBED_SCALE - SCALE_HIGH
DP_VOCAB = ("dp", "vocab_0", "vocab_1", "vocab_2")
MESH = pl.DeviceIdType.MESH
BF = jnp.bfloat16
F32 = jnp.float32
I16 = jnp.int16
NT = (((1,), (1,)), ((), ()))
TN = (((0,), (0,)), ((), ()))
NN = (((1,), (0,)), ((), ()))
MT = 400
MF = 256
NV = ROWS // MT
HALF = D // 2
W = 256
NT_COLS = HALF // W
EARLY = 4
SLOTS = 32
ALL_SLOTS = 4 * SLOTS
VMEM_LIMIT = 66_900_000
TABLE_BOUND = 5.0 / math.sqrt(D) * 1.01
UNITS = 24000.0
KNEE = 256.0
FINE = 32.0


def encode(value):
    bent = jnp.clip(value, -KNEE, KNEE)
    return jnp.round(value + bent * (FINE - 1.0)).astype(jnp.int32).astype(I16)


def decode(code):
    wide = code.astype(jnp.int32).astype(F32)
    return wide - jnp.clip(wide, -KNEE * FINE, KNEE * FINE) * (1.0 - 1.0 / FINE)


def bend(capped):
    ratio = capped * (1.0 / SOFTCAP)
    return 1.0 - ratio * ratio


def gray(i):
    return i + (i // 2) * (1 - 2 * (i % 2))


class Place:
    def __init__(self):
        self.y = y = lax.axis_index("dp")
        self.z = z = lax.axis_index("vocab_0")
        self.x = x = lax.axis_index("vocab_1")
        self.c = c = lax.axis_index("vocab_2")
        self.o = 1 - c
        self.first_row = (((y * 4 + z) * 4 + x) * 2 + c) * ROWS
        self.g = gray(y)
        self.ga = self.g + 1 - 2 * (self.g % 2)
        self.gb = (self.g + 2) % 4
        self.gc = (self.ga + 2) % 4
        self.y_a = {"dp": y + 1 - 2 * (y % 2)}
        self.y_b = {"dp": 3 - y}
        self.core = {"vocab_2": self.o}
        self.a = x + c * (z - x)
        self.b = z + c * (x - z)
        self.a_peers = [self._at((self.a + off) % 4, self.b) for off in (1, 2, 3)]
        self.b_peers = [self._at(self.a, (self.b + off) % 4) for off in (1, 2, 3)]
        cores = [(off, core) for off in range(4) for core in (self.c, self.o)][1:]
        self.line = [{"vocab_1": (x + off) % 4, "vocab_2": core} for off, core in cores]
        planes = [(up, over) for up in range(4) for over in range(4)][1:]
        self.sheet = [{"vocab_0": (z + up) % 4, "dp": (y + over) % 4} for up, over in planes]
        self.y_peers = [{"dp": (y + off) % 4} for off in (1, 2, 3)]
        self.cols = pl.ds(pl.multiple_of(c * HALF, 128), HALF)
        self.a_at = [(self.a + off) % 4 for off in (1, 2, 3)]
        self.b_at = [(self.b + off) % 4 for off in (1, 2, 3)]
        self.y_at = [gray((y + off) % 4) for off in (1, 2, 3)]
        a, b = self.a, self.b
        a0, a1, b0, b1 = (a + a // 2) % 2, a // 2, (b + b // 2) % 2, b // 2
        self.colours = [(a0 + third) % 2 + 2 * ((a1 + third) % 2) for third in (b0, b1)]
        flip_a, flip_b = a + 1 - 2 * (a % 2), b + 1 - 2 * (b % 2)
        first, second = self._at(flip_a, b), self._at(3 - a, b)
        self.near = [
            [first, second, self._at(a, flip_b)],
            [second, first, self._at(a, 3 - b)],
        ]
        self.parts = [
            pl.ds(pl.multiple_of(c * HALF + part * (HALF // 2), 128), HALF // 2) for part in range(2)
        ]

    def _at(self, a, b):
        return {"vocab_1": a + self.c * (b - a), "vocab_0": b + self.c * (a - b)}

    def tile_cols(self, j):
        return pl.ds(pl.multiple_of(self.c * HALF + j * W, 128), W)

    def first_row_of(self, k):
        return (((gray(k) * 4 + self.z) * 4 + self.x) * 2 + self.c) * ROWS

    def meet(self):
        peers = self.line + self.sheet
        barrier = pltpu.get_barrier_semaphore()
        for peer in peers:
            pl.semaphore_signal(barrier, inc=1, device_id=peer, device_id_type=MESH)
        return lambda: pl.semaphore_wait(barrier, len(peers))


class Sent:
    def __init__(self, sems, at, parts, out_like, in_like, times):
        self.sems, self.at, self.parts = sems, at, parts
        self.out_like, self.in_like, self.times = out_like, in_like, times

    def start(self, parts=None):
        for src, dst, peer in self.parts if parts is None else parts:
            pltpu.make_async_remote_copy(
                src_ref=src(),
                dst_ref=dst(),
                send_sem=self.sems[0].at[self.at],
                recv_sem=self.sems[1].at[self.at],
                device_id=peer,
                device_id_type=MESH,
            ).start()

    def wait_send(self):
        times, self.times = self.times, 0
        for _ in range(times):
            like = self.out_like()
            pltpu.make_async_copy(like, like, self.sems[0].at[self.at]).wait()

    def wait_recv(self):
        like = self.in_like()
        pltpu.make_async_copy(like, like, self.sems[1].at[self.at]).wait()


class Post:
    def __init__(self, send_sems, recv_sems):
        self.sems = (send_sems, recv_sems)
        self.used = 0
        self.open = []

    def send(self, src, dst, peer):
        return self.group([(src, dst, peer)], src, dst)

    def group(self, parts, out_like, in_like, times=1):
        sent = self.plan(parts, out_like, in_like, times)
        sent.start()
        return sent

    def plan(self, parts, out_like, in_like, times=1):
        sent = Sent(self.sems, self.used, parts, out_like, in_like, times)
        self.used += 1
        self.open.append(sent)
        return sent

    def sent(self, item):
        item.wait_send()
        self.open = [c for c in self.open if c is not item]

    def close(self):
        for item in self.open:
            item.wait_send()
        self.open = []


class Seen:
    def wait_recv(self):
        pass


class Agenda:
    def __init__(self):
        self.now = 0.0
        self.todo = []
        self.count = 0

    def add(self, after, step):
        self.todo.append((self.now + after, self.count, step))
        self.count += 1

    def run(self, until=None):
        while self.todo:
            self.todo.sort(key=lambda item: item[:2])
            if until is not None and self.todo[0][0] > until:
                return
            when, _, step = self.todo.pop(0)
            self.now = max(self.now, when)
            step()

    def due(self, until):
        return any(item[0] <= until for item in self.todo)

    def compute(self, cost, work):
        self.run(self.now)
        work()
        self.now += cost
        self.run(self.now)


def columns(table, j, core):
    own = pl.ds(pl.multiple_of(core * HALF + j * W, 128), W)
    other = pl.ds(pl.multiple_of((1 - core) * HALF + j * W, 128), W)
    return jnp.concatenate([table[:, own], table[:, other]], axis=1)


def gather_rows(place, post, agenda, buf, sends, done):
    a, b, cols = place.a, place.b, place.cols

    def mine():
        return buf.at[b, a, :, cols]

    def row():
        return buf.at[:, a, :, cols]

    def rows():
        return buf.at[:, 0:3, :, cols]

    def half():
        return buf.at[:, :, :, cols]

    first = post.group(
        [(mine, mine, peer) for peer in place.b_peers], mine, lambda: buf.at[0:3, 0, :, cols], 3
    )
    sends.append(first)

    def along_a():
        first.wait_recv()
        second = post.group([(row, row, peer) for peer in place.a_peers], rows, rows)
        sends.append(second)
        agenda.add(9.0, lambda: across(second))

    def across(second):
        second.wait_recv()
        third = post.send(half, half, place.core)
        sends.append(third)
        agenda.add(4.0, lambda: finish(third))

    def finish(third):
        third.wait_recv()
        done()

    agenda.add(13.0, along_a)


POSTS = 32
STEPS = 8
LAG = (1, 3, 5)
TAIL_AT = ((1, 2), (4, 2), (6, 1), (8, 1), (10, 1), (12, 1), (14, 0), (15, 0))
HEAD_TILES = 2 * NT_COLS
TAIL = TAIL_AT[-1][0] + 1


def main_kernel(
    ids_hbm, targets_hbm, mask_hbm, hidden_hbm, gain_hbm, table_hbm, cot_hbm,
    head_hbm, metas_hbm, embed_hbm, grad_hbm, gain_sum_hbm, loss_hbm, most_hbm, cap_hbm,
    table, normed, metas, own_lines, scalars, hidden, gain_rows, gain, marks, stats, stat_in, scale_rows, back_rows, inverses, dots,
    d_stage, d_part, d_rc, d_rx, d_rz, found, owner_of, slot_of, packed, lines, cot_packed,
    stage, snd, rc, sx, rx, s_two, r_two, acc, acc_two, sz, rz, acc_z, sy, ry, up,
    gain_in, local_sems, send_sems, recv_sems, flow_send, flow_recv,
):
    place = Place()
    post = Post(send_sems, recv_sems)
    agenda = Agenda()
    first_row = place.first_row
    a, b, c, o, g, y = place.a, place.b, place.c, place.o, place.g, place.y
    blocks = [g, place.ga, place.gb, place.gc]
    entered = place.meet()
    early = [
        pltpu.make_async_copy(hidden_hbm, hidden, local_sems.at[7]),
        pltpu.make_async_copy(gain_hbm, gain_rows, local_sems.at[8]),
    ]
    for n, ref in enumerate((ids_hbm, targets_hbm, mask_hbm)):
        early.append(pltpu.make_async_copy(ref, own_lines.at[n], local_sems.at[9 + n]))
    for copy in early:
        copy.start()
    def table_load(i):
        rows = pl.ds(i * 1024, 1024 - 48 * i)
        return pltpu.make_async_copy(table_hbm.at[rows], table.at[rows], local_sems.at[5 * i])

    table_load(0).start()
    table_load(1).start()
    for copy in early[1:]:
        copy.wait()
    for n in range(3):
        metas[g, n : n + 1, :] = own_lines[n]
    gain[...] = jnp.concatenate([gain_rows[i : i + 1, :] for i in range(D // 128)], axis=1)
    early[0].wait()
    cot_load = pltpu.make_async_copy(cot_hbm, found, local_sems.at[3])
    cot_load.start()

    def inverse(wide):
        return lax.rsqrt(jnp.mean(wide * wide, axis=1, keepdims=True) + EPSILON)

    def rows_of(block, first, count):
        return pl.ds(pl.multiple_of(block * 256 + first, 16), count)

    def normalise(i, carry):
        at = i * 64
        rows = pl.ds(pl.multiple_of(at, 16), 64)
        wide = hidden[rows, :].astype(F32)
        inv = inverse(wide)
        inverses[rows, :] = jnp.broadcast_to(inv, (64, 128))
        normed[rows_of(g, at, 64), :] = (wide * inv * gain[...]).astype(BF)
        return carry

    lax.fori_loop(0, 4, normalise, 0)
    stats[...] = jnp.zeros_like(stats)
    entered()

    def piece(block, part, half):
        def rows():
            at = place.colours[part] * 64 + half * 32
            return normed.at[rows_of(block, at, 32), place.parts[part]]

        return rows

    def ship(block, part, half, peer):
        rows = piece(block, part, half)
        return post.send(rows, rows, peer)

    meta_in = [
        post.send(lambda: metas.at[g], lambda: metas.at[g], peer) for peer in (place.y_a, place.y_b)
    ]
    both = (0, 1)
    a_low = [ship(g, part, 0, place.y_a) for part in both]
    b_high = [ship(g, part, 1, place.y_b) for part in both]
    a_high = [ship(g, part, 1, place.y_a) for part in both]
    b_low = [ship(g, part, 0, place.y_b) for part in both]
    meta_c = post.plan(
        [(lambda: metas.at[place.ga], lambda: metas.at[place.ga], place.y_b)],
        lambda: metas.at[place.ga],
        lambda: metas.at[place.gc],
    )
    def pieces():
        return normed.at[pl.ds(0, 12 * 32), place.parts[0]]

    spread = {name: post.plan([], pieces, pieces) for name in "abc"}
    c_low, c_high = [], []

    def swap(block):
        def part():
            return normed.at[rows_of(block, 0, 256), place.cols]

        return post.plan([(part, part, place.core)], part, part)

    swaps = {"a": swap(place.ga), "b": swap(place.gb), "c": swap(place.gc)}

    def pass_piece(name, block, part, half):
        rows = piece(block, part, half)
        spread[name].start([(rows, rows, peer) for peer in place.near[part]])

    def spread_piece(name, block, half, items):
        for part, item in enumerate(items):
            item.wait_recv()
            pass_piece(name, block, part, half)

    def swap_block(name):
        spread[name].wait_recv()
        swaps[name].start()

    def cap_store(n):
        return pltpu.make_async_copy(
            stage.at[n, pl.ds(0, ROWS)], cap_hbm.at[n], local_sems.at[1 + n]
        )

    def forward(n, block, between, later=None):
        side = n % 2
        rows = normed[rows_of(block, 0, 256), :]
        total = jnp.zeros((1, 256), F32)
        picked = total
        for at in range(0, ROWS, MF):
            if at == 4 * MF:
                between()
            if at == 6 * MF and later is not None:
                later()
            size = min(MF, ROWS - at)
            logits = lax.dot_general(table[at : at + size, :], rows, NT, preferred_element_type=F32)
            capped = SOFTCAP * jnp.tanh(logits * (1.0 / SOFTCAP))
            raised = jnp.exp(capped)
            stage[side, at : at + size] = raised * bend(capped)
            ids = lax.broadcasted_iota(jnp.int32, capped.shape, 0) + (first_row + at)
            hit = ids == metas[block, 1:2, :]
            total += jnp.sum(raised, axis=0, keepdims=True)
            picked += jnp.sum(jnp.where(hit, capped, 0.0), axis=0, keepdims=True)
        stats[block, 0:1, :] = total
        stats[block, 1:2, :] = picked

    seen = [Seen(), Seen()]

    def pass_on():
        table_load(1).wait()
        for item in meta_in:
            item.wait_recv()
        meta_c.start()
        for part in both:
            a_low[part].wait_recv()
            c_low.append(ship(place.ga, part, 0, place.y_b))
            pass_piece("a", place.ga, part, 0)
        for part in both:
            b_high[part].wait_recv()
            c_high.append(ship(place.gb, part, 1, place.y_a))

    table_load(0).wait()
    forward(0, g, pass_on, lambda: spread_piece("a", place.ga, 1, a_high))
    cap_store(0).start()

    meta_c.wait_recv()
    ids = [metas[k, 0:1, :] for k in range(4)]
    locals_ = [row - first_row for row in ids]
    for k in range(4):
        locals_.append(own_lines[0] - place.first_row_of(k))
    owned = [jnp.where((row >= 0) & (row < ROWS), 1.0, 0.0) for row in locals_]
    later = lax.broadcasted_iota(jnp.int32, (256, 256), 0) < lax.broadcasted_iota(
        jnp.int32, (256, 256), 1
    )
    ranks = lax.dot_general(
        jnp.concatenate(owned + [jnp.zeros((8, 256), F32)], axis=0).astype(BF),
        jnp.where(later, 1.0, 0.0).astype(BF),
        NN,
        preferred_element_type=F32,
    )
    numbers = lax.broadcasted_iota(jnp.int32, (SLOTS, 256), 0).astype(F32)

    def chosen(k):
        same = (numbers == ranks[k : k + 1, :]) & (owned[k] > 0.5)
        return jnp.where(same, 1.0, 0.0)

    mine = jnp.concatenate([chosen(k) for k in range(4)], axis=0).astype(BF)
    slot_of[...] = jnp.concatenate([chosen(4 + k) for k in range(4)], axis=0).astype(BF)
    digits = [jnp.right_shift(row, 6) for row in locals_[:4]]
    digits += [jnp.bitwise_and(row, 63) for row in locals_[:4]]
    digits = [jnp.where(owned[n % 4] > 0.5, row.astype(F32), 0.0) for n, row in enumerate(digits)]
    read = lax.dot_general(
        jnp.concatenate(digits + [jnp.ones((8, 256), F32)], axis=0).astype(BF),
        mine,
        NT,
        preferred_element_type=F32,
    )
    lane = lax.broadcasted_iota(jnp.int32, (1, ALL_SLOTS), 1)
    wanted = jnp.zeros((1, ALL_SLOTS), F32)
    for k in range(4):
        here = (lane >= k * SLOTS) & (lane < (k + 1) * SLOTS)
        wanted = jnp.where(here, read[k : k + 1] * 64.0 + read[4 + k : 5 + k], wanted)
    wanted = jnp.where(read[8:9] > 0.5, wanted, -1.0)

    starts = lax.broadcasted_iota(jnp.int32, (128, 256), 0) * ROWS
    most = jnp.float32(0.0)
    for row in ids:
        held = jnp.where((row >= starts) & (row < starts + ROWS), 1.0, 0.0)
        most = jnp.maximum(most, jnp.max(jnp.sum(held, axis=1, keepdims=True)))
    keep = jnp.where(most <= SLOTS, 1.0, 0.0)

    def mark(i, carry):
        rows = pl.ds(pl.multiple_of(i * MT, 16), MT)
        at = lax.broadcasted_iota(jnp.int32, (MT, ALL_SLOTS), 0) + i * MT
        same = at.astype(F32) == wanted
        owner_of[rows, :] = jnp.where(same, 1.0, 0.0).astype(BF)
        marks[rows, 1024:1152] = jnp.where(same, keep * SCALE_HIGH, 0.0).astype(BF)
        marks[rows, 1152:1280] = jnp.where(same, keep * SCALE_LOW, 0.0).astype(BF)
        return carry


    lax.fori_loop(0, NV, mark, 0)

    def look_up(j, carry):
        cols = pl.ds(pl.multiple_of(j * 2 * W, 128), 2 * W)
        rows = lax.dot_general(owner_of[...], table[:, cols], TN, preferred_element_type=F32)
        packed[:, :, cols] = rows.astype(BF).reshape(4, SLOTS, 2 * W)
        return carry

    def exchange(src, dst):
        dst[g] = src[g]
        parts = [
            (lambda n=n: src.at[place.y_at[n]], lambda: dst.at[g], peer)
            for n, peer in enumerate(place.y_peers)
        ]
        return post.group(parts, lambda: src.at[0:3], lambda: dst.at[0:3])

    spread_piece("b", place.gb, 1, seen)
    spread_piece("b", place.gb, 0, b_low)
    lax.fori_loop(0, EARLY, look_up, 0)
    swap_block("a")
    spread_piece("c", place.gc, 0, c_low)
    spread_piece("c", place.gc, 1, c_high)
    lax.fori_loop(EARLY, NT_COLS, look_up, 0)
    line_item = exchange(packed, lines)

    def cot_pack(j, carry):
        cols = pl.ds(pl.multiple_of(j * 2 * W, 128), 2 * W)
        rows = lax.dot_general(
            slot_of[...], found[:, :, :, cols].reshape(256, 2 * W), NN, preferred_element_type=F32
        )
        cot_packed[:, :, cols] = rows.astype(BF).reshape(4, SLOTS, 2 * W)
        return carry

    def later_block(n, carry):
        block = jnp.where(n == 1, place.ga, jnp.where(n == 2, place.gb, place.gc))

        @pl.when(n == 1)
        def _():
            swaps["a"].wait_recv()

        @pl.when(n == 2)
        def _():
            swaps["b"].wait_recv()
            cap_store(0).wait()

        @pl.when(n == 3)
        def _():
            swaps["c"].wait_recv()
            cap_store(1).wait()

        def between():
            @pl.when(n == 1)
            def _():
                swap_block("b")

            @pl.when(n == 2)
            def _():
                swap_block("c")

        forward(n, block, between)

        @pl.when(n == 1)
        def _():
            cap_store(1).start()

        return carry

    lax.fori_loop(1, 4, later_block, 0)

    found_sends = []

    def unpack():
        line_item.wait_recv()
        for h in range(2):
            rows = lax.dot_general(
                slot_of[...],
                lines[:, :, h * HALF : (h + 1) * HALF].reshape(ALL_SLOTS, HALF),
                TN,
                preferred_element_type=F32,
            )
            d_part[h] = rows.astype(BF).reshape(4, 4, 16, HALF)
        return post.send(lambda: d_part.at[o], lambda: d_rc, place.core)

    def d_merge(item):
        item.wait_recv()
        d_rc[...] = d_part[c] + d_rc[...]
        parts = [
            (lambda n=n: d_rc.at[:, place.a_at[n]], lambda n=n: d_rx.at[n], peer)
            for n, peer in enumerate(place.a_peers)
        ]
        item = post.group(parts, lambda: d_rx, lambda: d_rx)
        agenda.add(9.0, lambda: d_along_b(item))

    def d_along_b(item):
        item.wait_recv()
        d_rc[:, a] = (d_rc[:, a] + d_rx[0]) + (d_rx[1] + d_rx[2])
        parts = [
            (lambda n=n: d_rc.at[place.b_at[n], a], lambda n=n: d_rz.at[n], peer)
            for n, peer in enumerate(place.b_peers)
        ]
        item = post.group(parts, lambda: d_rz, lambda: d_rz)
        agenda.add(12.0, lambda: d_end(item))

    def d_end(item):
        item.wait_recv()
        row = (d_rc[b, a] + d_rz[0]) + (d_rz[1] + d_rz[2])
        found[b, a, :, place.cols] = (row.astype(F32) * EMBED_SCALE).astype(BF)
        gather_rows(place, post, agenda, found, found_sends, embed_done)

    def embed_store():
        return pltpu.make_async_copy(found, embed_hbm, local_sems.at[0])

    def embed_done():
        embed_store().start()
        for item in found_sends:
            post.sent(item)

    def ring_start(base, peers, at):
        stat_in[base + at] = stats[...]

        def part():
            return stat_in.at[base + at]

        def like():
            return stat_in.at[pl.ds(0, len(peers))]

        return post.group([(part, part, peer) for peer in peers], like, like)

    def ring_end(item, base, count):
        item.wait_recv()
        total = stat_in[base]
        for i in range(1, count):
            total = total + stat_in[base + i]
        stats[...] = total

    item = ring_start(0, place.line, place.x * 2 + c)
    half_item = unpack()
    ring_end(item, 0, 8)
    item = ring_start(8, place.sheet, place.z * 4 + y)
    cot_load.wait()
    lax.fori_loop(0, NT_COLS, cot_pack, 0)
    ring_end(item, 8, 16)
    cot_item = exchange(cot_packed, normed.at[pl.ds(1024, ALL_SLOTS)].reshape(4, SLOTS, D))
    agenda.now = 40.0
    d_merge(half_item)

    def cap_load(n):
        return pltpu.make_async_copy(
            cap_hbm.at[n], stage.at[n, pl.ds(0, ROWS)], local_sems.at[1 + n]
        )

    def slopes(n):
        block, side = blocks[n], n % 2
        if n < 2:
            cap_load(n).wait()
        weight = metas[block, 2:3, :].astype(F32)
        factor = weight / stats[block, 0:1, :]
        target = metas[block, 1:2, :]
        taken = weight * bend(stats[block, 1:2, :])
        lanes = pl.ds(pl.multiple_of(block * 256, 128), 256)

        def slab(i, carry):
            rows = pl.ds(pl.multiple_of(i * MT, 16), MT)
            ids = lax.broadcasted_iota(jnp.int32, (MT, 256), 0) + (first_row + i * MT)
            hit = jnp.where(ids == target, taken, 0.0)
            value = stage[side, rows, :] * factor - hit
            marks[rows, lanes] = value.astype(BF)
            return carry

        lax.fori_loop(0, NV, slab, 0)
        if n >= 2:
            cap_load(n - 2).start()

    for n in (2, 3, 0, 1):
        agenda.compute(0.9, lambda: slopes(n))

    def bound(k):
        rest = jnp.maximum(1.0 - jnp.exp(stats[k, 1:2, :]) / stats[k, 0:1, :], 0.0)
        return TABLE_BOUND * (2.0 * rest + 1e-4)

    for k in range(4):
        turned = jnp.broadcast_to(UNITS / bound(k), (128, 256)).T
        scale_rows[k * 256 : (k + 1) * 256, :] = turned
    back_rows[...] = jnp.broadcast_to(bound(g) * (1.0 / UNITS), (128, 256)).T

    weights = [metas[k, 2:3, :].astype(F32) for k in range(4)]
    weight_sum = sum(jnp.sum(w) for w in weights)
    loss_sum = sum(
        jnp.sum(w * (jnp.log(stats[k, 0:1, :]) - stats[k, 1:2, :])) for k, w in enumerate(weights)
    )
    scalars[0] = jnp.full((1, 1), loss_sum / jnp.maximum(weight_sum, 1.0), F32)
    scalars[1] = jnp.full((1, 1), most, F32)
    small_stores = [
        pltpu.make_async_copy(scalars.at[0], loss_hbm, local_sems.at[7]),
        pltpu.make_async_copy(scalars.at[1], most_hbm, local_sems.at[8]),
        pltpu.make_async_copy(metas, metas_hbm, local_sems.at[9]),
    ]
    for copy in small_stores:
        copy.start()
    shape = (4, 4, 4, 16, W)

    class Flow:
        def __init__(self, step, j):
            self.send_sem = flow_send.at[2 * step + j % 2 if step < 3 else step + 3]
            self.recv_sem = flow_recv.at[step, j]

        def start(self, parts):
            for src, dst, peer in parts:
                pltpu.make_async_remote_copy(
                    src_ref=src,
                    dst_ref=dst,
                    send_sem=self.send_sem,
                    recv_sem=self.recv_sem,
                    device_id=peer,
                    device_id_type=MESH,
                ).start()

        def sent(self, like):
            pltpu.make_async_copy(like, like, self.send_sem).wait()

        def here(self, like):
            pltpu.make_async_copy(like, like, self.recv_sem).wait()

    def pull(t):
        slot = t % 2

        @pl.when(t >= 2)
        def _():
            Flow(0, t - 2).sent(snd.at[slot])

        product = lax.dot_general(
            marks[:, 0:1024], columns(table, t, c), TN, preferred_element_type=F32
        )
        for half in range(2):
            lanes = slice(half * 128, half * 128 + 128)
            other = slice(W + half * 128, W + half * 128 + 128)
            stage[slot, 0:1024, lanes] = product[:, lanes] * scale_rows[...]
            code = encode(product[:, other] * scale_rows[...])
            snd[slot, :, :, :, :, lanes] = code.reshape(4, 4, 4, 16, 128)
        Flow(0, t).start([(snd.at[slot], rc.at[t % 4], place.core)])

    def held(slot, at):
        whole = stage.at[slot, pl.ds(0, 1024)].reshape(*shape)
        return whole[:, :, at]

    near_a = (a + 1 - 2 * (a % 2), 3 - a)

    def partners(j):
        first = near_a[0] + (j % 2) * (near_a[1] - near_a[0])
        second = near_a[1] + (j % 2) * (near_a[0] - near_a[1])
        return first, second

    def merge(j):
        slot = j % 2
        first, second = partners(j)
        Flow(0, j).here(rc.at[j % 4])

        @pl.when(j >= 2)
        def _():
            Flow(1, j - 2).sent(sx.at[slot])

        for n, at in enumerate((first, (a + 2) % 4)):
            sx[slot, n] = encode(held(slot, at) + decode(rc[j % 4, :, :, at]))
        Flow(1, j).start([(sx.at[slot], rx.at[j], place._at(first, b))])
        acc[j] = held(slot, a) + decode(rc[j % 4, :, :, a])
        acc_two[j % 3] = held(slot, second) + decode(rc[j % 4, :, :, second])

    def second_half(j):
        _, second = partners(j)
        Flow(1, j).here(rx.at[j])

        @pl.when(j >= 2)
        def _():
            Flow(2, j - 2).sent(s_two.at[j % 2])

        s_two[j % 2] = encode(acc_two[j % 3] + decode(rx[j, 1]))
        Flow(2, j).start([(s_two.at[j % 2], r_two.at[j], place._at(second, b))])
        acc[j] = acc[j] + decode(rx[j, 0])

    def along_y(j):
        Flow(2, j).here(r_two.at[j])
        acc_z[j] = acc[j, g] + decode(r_two[j, g])
        parts = []
        for n, peer in enumerate(place.y_peers):
            at = place.y_at[n]
            sz[j, n] = encode(acc[j, at] + decode(r_two[j, at]))
            parts.append((sz.at[j, n], rz.at[j, n], peer))
        Flow(3, j).start(parts)

    def along_b(j):
        Flow(3, j).here(rz.at[j])
        acc_z[j] = acc_z[j] + decode(rz[j, 0]) + decode(rz[j, 1]) + decode(rz[j, 2])
        parts = []
        for n, peer in enumerate(place.b_peers):
            sy[j, n] = encode(acc_z[j, place.b_at[n]])
            parts.append((sy.at[j, n], ry.at[j, n], peer))
        Flow(4, j).start(parts)

    def give_b(j):
        Flow(4, j).here(ry.at[j])
        value = acc_z[j, b] + decode(ry[j, 0]) + decode(ry[j, 1]) + decode(ry[j, 2])
        cols = place.tile_cols(j)
        up[b, a, :, cols] = encode(value)
        part = up.at[b, a, :, cols]
        Flow(5, j).start([(part, part, peer) for peer in place.b_peers])

    def give_a(j):
        cols = place.tile_cols(j)
        Flow(5, j).here(up.at[0:3, 0, :, cols])
        part = up.at[:, a, :, cols]
        Flow(6, j).start([(part, part, peer) for peer in place.a_peers])

    def give_core(j):
        cols = place.tile_cols(j)
        Flow(6, j).here(up.at[:, 0:3, :, cols])
        part = up.at[:, :, :, cols]
        Flow(7, j).start([(part, part, place.core)])

    def last(j):
        cols = place.tile_cols(j)
        Flow(7, j).here(up.at[:, :, :, cols])
        down, inv = back_rows[...], inverses[...]
        for h in range(2):
            for q in range(W // 128):
                at = h * HALF + j * W + q * 128
                cols = pl.ds(pl.multiple_of(at, 128), 128)
                value = decode(up[:, :, :, cols].reshape(256, 128)) * down
                product = value * hidden[:, cols].astype(F32)
                dots[...] += product * gain[:, cols]
                gain_in[y, pl.ds(h * (HALF // 128) + j * 2 + q, 1), :] = jnp.sum(
                    product * inv, axis=0, keepdims=True
                )

    steps = (merge, second_half, along_y, along_b, give_b, give_a, give_core, last)

    def head_store(n):
        cols = pl.ds(pl.multiple_of(n * W, 128), W)
        return pltpu.make_async_copy(
            d_stage.at[n % 2, pl.ds(0, ROWS)], head_hbm.at[:, cols], local_sems.at[3 + n % 2]
        )

    def head_tile(n):
        @pl.when(n >= 2)
        def _():
            head_store(n - 2).wait()

        cols = pl.ds(pl.multiple_of(n * W, 128), W)
        product = lax.dot_general(marks[...], normed[:, cols], NN, preferred_element_type=F32)
        d_stage[n % 2, 0:ROWS] = product.astype(BF)
        head_store(n).start()

    def take_due(t, turns, pace):
        for k in range(turns):
            due = agenda.now + pace
            if agenda.due(due):
                @pl.when(t == k)
                def _():
                    agenda.run(due)
            agenda.now = max(agenda.now, due)

    def turn(t, carry):
        pull(t)
        for lag, step in zip(LAG, steps):
            @pl.when(t >= lag)
            def _():
                step(t - lag)

        take_due(t, NT_COLS, 2.8)
        return carry

    dots[...] = jnp.zeros_like(dots)
    lax.fori_loop(0, NT_COLS, turn, 0)
    cot_item.wait_recv()
    normed[1152:1280, :] = normed[1024:1152, :]

    agenda.add(22.0, post.close)

    def tail(t, carry):
        @pl.when(t < HEAD_TILES)
        def _():
            head_tile(t)

        for n, ((at, pace), step) in enumerate(zip(TAIL_AT, steps)):
            if pace == 0:
                for q in range(2):
                    j = NT_COLS - 1 - 2 * (at - t) + q

                    @pl.when((j >= 0) & (j < NT_COLS))
                    def _():
                        step(j)

                continue
            begun = NT_COLS - LAG[n] if n < len(LAG) else 0
            ahead = at - t
            j = NT_COLS - 1 - ahead // pace

            @pl.when((ahead >= 0) & (ahead % pace == 0) & (j >= begun))
            def _():
                step(j)

        take_due(t, TAIL, 1.9)
        return carry

    lax.fori_loop(0, TAIL, tail, 0)

    def gain_part():
        return gain_in.at[y]

    gain_item = post.group(
        [(gain_part, gain_part, peer) for peer in place.y_peers],
        lambda: gain_in.at[0:3],
        lambda: gain_in.at[0:3],
    )

    agenda.run()

    GR = 16

    def upstream(i):
        rows = pl.ds(pl.multiple_of(i * GR, 16), GR)
        down = back_rows[rows, :]
        value = decode(up[i // 4, i % 4]) * jnp.concatenate([down] * (D // 128), axis=1)
        return value, hidden[rows, :].astype(F32), inverses[rows, :]

    def grad_rows(i, carry):
        value, wide, inv = upstream(i)
        rows = pl.ds(pl.multiple_of(i * GR, 16), GR)
        mean_dot = jnp.sum(dots[rows, :], axis=1, keepdims=True) * (1.0 / D)
        pull_back = inv * inv * inv * mean_dot
        out = jnp.concatenate([inv] * (D // 128), axis=1) * (value * gain[...])
        out = out - wide * jnp.concatenate([pull_back] * (D // 128), axis=1)
        normed[rows, :] = out.astype(BF)
        pltpu.make_async_copy(normed.at[rows], grad_hbm.at[rows], local_sems.at[6]).start()
        return carry

    lax.fori_loop(0, 16, grad_rows, 0)
    for copy in small_stores:
        copy.wait()
    for n in (HEAD_TILES - 2, HEAD_TILES - 1):
        head_store(n).wait()

    Flow(3, 0).sent(sz)
    Flow(4, 0).sent(sy)
    Flow(5, 0).sent(up.at[0:3, 0, :, place.cols])
    Flow(6, 0).sent(up.at[:, 0:3, :, place.cols])
    Flow(7, 0).sent(up.at[:, :, :, place.cols])
    for j in (NT_COLS - 2, NT_COLS - 1):
        Flow(0, j).sent(snd.at[j % 2])
        Flow(1, j).sent(sx.at[j % 2])
        Flow(2, j).sent(s_two.at[j % 2])
    post.close()
    gain_item.wait_recv()
    gain_rows[...] = gain_in[0] + gain_in[1] + gain_in[2] + gain_in[3]
    gain_store = pltpu.make_async_copy(gain_rows, gain_sum_hbm, local_sems.at[10])
    gain_store.start()
    gain_store.wait()
    embed_store().wait()
    pltpu.make_async_copy(normed.at[pl.ds(0, 256)], grad_hbm, local_sems.at[6]).wait()


def deliver_kernel(*refs):
    ins, outs, (small, large, line, sems) = refs[:4], refs[4:8], refs[8:]
    moves = [(ins[0], outs[0], line, 0)]
    moves += [(ins[n], outs[n], small.at[n - 1], n) for n in (1, 2)]
    for i in range(NV):
        rows = pl.ds(i * MT, MT)
        moves.append((ins[3].at[rows], outs[3].at[rows], large.at[rows], 3 + i))
    for src, _, buf, n in moves:
        pltpu.make_async_copy(src, buf, sems.at[n]).start()
    for src, dst, buf, n in moves:
        pltpu.make_async_copy(src, buf, sems.at[n]).wait()
        pltpu.make_async_copy(buf, dst, sems.at[n]).start()
    for _, dst, buf, n in moves:
        pltpu.make_async_copy(buf, dst, sems.at[n]).wait()


def around(array, axis):
    count = lax.axis_size(axis)
    for _ in range(count - 1):
        array = lax.ppermute(array, axis, [(i, (i + 1) % count) for i in range(count)])
        yield array


def dense_embedding(ids, embed_cotangent, table, head):
    local = ids - lax.axis_index(DP_VOCAB) * ROWS
    inside = (local >= 0) & (local < ROWS)
    rows = jnp.take(table, jnp.clip(local, 0, ROWS - 1), axis=0)
    total = jnp.where(inside[:, None], rows, 0)
    for axis in DP_VOCAB:
        total = sum(around(total, axis), total)
    g = gray(lax.axis_index("dp"))
    own = lax.dynamic_slice_in_dim(total, g * 256, 256, axis=0)
    embedded = (own.astype(F32) * EMBED_SCALE).astype(BF)
    y = lax.axis_index("dp")
    cot = lax.dynamic_update_slice_in_dim(jnp.zeros((1024, D), BF), embed_cotangent, g * 256, axis=0)
    for off, block in enumerate(around(embed_cotangent, "dp")):
        cot = lax.dynamic_update_slice_in_dim(cot, block, gray((y - off - 1) % 4) * 256, axis=0)
    where = jnp.where(inside, local, ROWS)
    part = jax.ops.segment_sum(cot.astype(F32), where, num_segments=ROWS + 1)[:ROWS]
    return embedded, (head.astype(F32) + part * EMBED_SCALE).astype(BF)


def body(input_ids, target_ids, loss_mask, final_hidden, norm_gain, embed_cotangent, table):
    any_ = pl.BlockSpec(memory_space=pl.ANY)
    vmem = pl.BlockSpec(memory_space=pltpu.VMEM)
    dma = pltpu.SemaphoreType.DMA
    V = pltpu.VMEM
    S = jax.ShapeDtypeStruct
    gain = norm_gain.reshape(D // 128, 128)
    n = NT_COLS
    head, metas, embed, grad, gain_grad, loss, most, _ = pl.pallas_call(
        main_kernel,
        out_shape=(
            S((ROWS, D), BF),
            S((4, 8, 256), jnp.int32),
            S((4, 4, 16, D), BF),
            S((256, D), BF),
            S((D // 128, 128), F32),
            S((1, 1), F32),
            S((1, 1), F32),
            S((2, ROWS, 256), F32),
        ),
        in_specs=[any_] * 7,
        out_specs=(any_,) * 8,
        scratch_shapes=[
            V((ROWS, D), BF),
            V((1024 + 2 * ALL_SLOTS, D), BF),
            V((4, 8, 256), jnp.int32),
            V((3, 1, 256), jnp.int32),
            V((2, 1, 1), F32),
            V((256, D), BF),
            V((D // 128, 128), F32),
            V((1, D), F32),
            V((ROWS, 1024 + 2 * ALL_SLOTS), BF),
            V((4, 2, 256), F32),
            V((24, 4, 2, 256), F32),
            V((1024, 128), F32),
            V((256, 128), F32),
            V((256, 128), F32),
            V((256, 128), F32),
            V((2, 2048, W), BF),
            V((2, 4, 4, 16, HALF), BF),
            V((4, 4, 16, HALF), BF),
            V((3, 4, 16, HALF), BF),
            V((3, 16, HALF), BF),
            V((4, 4, 16, D), BF),
            V((ROWS, ALL_SLOTS), BF),
            V((ALL_SLOTS, 256), BF),
            V((4, SLOTS, D), BF),
            V((4, SLOTS, D), BF),
            V((4, SLOTS, D), BF),
            V((2, 2048, W), F32),
            V((2, 4, 4, 4, 16, W), I16),
            V((4, 4, 4, 4, 16, W), I16),
            V((2, 2, 4, 4, 16, W), I16),
            V((n, 2, 4, 4, 16, W), I16),
            V((2, 4, 4, 16, W), I16),
            V((n, 4, 4, 16, W), I16),
            V((n, 4, 4, 16, W), F32),
            V((3, 4, 4, 16, W), F32),
            V((n, 3, 4, 16, W), I16),
            V((n, 3, 4, 16, W), I16),
            V((n, 4, 16, W), F32),
            V((n, 3, 16, W), I16),
            V((n, 3, 16, W), I16),
            V((4, 4, 16, D), I16),
            V((4, D // 128, 128), F32),
            dma((12,)),
            dma((POSTS,)),
            dma((POSTS,)),
            dma((STEPS + 3,)),
            dma((STEPS, n)),
        ],
        compiler_params=pltpu.CompilerParams(
            collective_id=0, has_side_effects=True, vmem_limit_bytes=VMEM_LIMIT
        ),
        name="main",
    )(
        input_ids.reshape(1, 256),
        target_ids.reshape(1, 256),
        loss_mask.reshape(1, 256),
        final_hidden,
        gain,
        table,
        embed_cotangent.reshape(4, 4, 16, D),
    )

    embedded, table_grad = lax.cond(
        most.reshape(()) > SLOTS,
        lambda: dense_embedding(metas[:, 0, :].reshape(1024), embed_cotangent, table, head),
        lambda: (embed.reshape(256, D), head),
    )
    gain_grad, embedded, grad_hidden, table_grad = pl.pallas_call(
        deliver_kernel,
        out_shape=(S((D // 128, 128), F32), S((256, D), BF), S((256, D), BF), S((ROWS, D), BF)),
        in_specs=[any_] * 4,
        out_specs=(any_,) * 4,
        scratch_shapes=[
            V((2, 256, D), BF),
            V((ROWS, D), BF),
            V((D // 128, 128), F32),
            dma((3 + NV,)),
        ],
        compiler_params=pltpu.CompilerParams(vmem_limit_bytes=VMEM_LIMIT),
        name="deliver",
    )(gain_grad, embedded, grad, table_grad)
    return (embedded, loss.reshape(()), grad_hidden, gain_grad.reshape(D), table_grad)


def solution(mesh):
    finer = Mesh(
        mesh.devices.reshape(mesh.shape["dp"], 4, 4, 2), ("dp", "vocab_0", "vocab_1", "vocab_2")
    )
    placed = (P("dp"), P("dp"), P("dp"), P("dp", None), P(), P("dp", None), P(DP_VOCAB, None))
    return jax.shard_map(
        body,
        mesh=finer,
        in_specs=placed,
        out_specs=(P("dp", None), P(), P("dp", None), P(), P(DP_VOCAB, None)),
        check_vma=False,
    )
```

```python
import math

import jax
import jax.numpy as jnp
from jax import lax
from jax.experimental import pallas as pl
from jax.experimental.pallas import tpu as pltpu
from jax.sharding import Mesh
from jax.sharding import PartitionSpec as P

SOFTCAP = 30.0
EPSILON = 1e-06
D = 3584
ROWS = 2000
EMBED_SCALE = math.sqrt(D)
SCALE_HIGH = 59.75
SCALE_LOW = EMBED_SCALE - SCALE_HIGH
DP_VOCAB = ("dp", "vocab_0", "vocab_1", "vocab_2")
MESH = pl.DeviceIdType.MESH
BF = jnp.bfloat16
F32 = jnp.float32
I16 = jnp.int16
NT = (((1,), (1,)), ((), ()))
TN = (((0,), (0,)), ((), ()))
NN = (((1,), (0,)), ((), ()))
MT = 400
MF = 256
NV = ROWS // MT
MOVED = 80
HALF = D // 2
W = 256
NT_COLS = HALF // W
EARLY = 4
SLOTS = 32
ALL_SLOTS = 4 * SLOTS
VMEM_LIMIT = 66_900_000
TABLE_BOUND = 5.0 / math.sqrt(D) * 1.01
UNITS = 24000.0
KNEE = 256.0
FINE = 32.0


def encode(value):
    bent = jnp.clip(value, -KNEE, KNEE)
    return jnp.round(value + bent * (FINE - 1.0)).astype(jnp.int32).astype(I16)


def decode(code):
    wide = code.astype(jnp.int32).astype(F32)
    return wide - jnp.clip(wide, -KNEE * FINE, KNEE * FINE) * (1.0 - 1.0 / FINE)


def bend(capped):
    ratio = capped * (1.0 / SOFTCAP)
    return 1.0 - ratio * ratio


def gray(i):
    return i + (i // 2) * (1 - 2 * (i % 2))


class Place:
    def __init__(self):
        self.y = y = lax.axis_index("dp")
        self.z = z = lax.axis_index("vocab_0")
        self.x = x = lax.axis_index("vocab_1")
        self.c = c = lax.axis_index("vocab_2")
        self.o = 1 - c
        self.first_row = (((y * 4 + z) * 4 + x) * 2 + c) * ROWS
        self.g = gray(y)
        self.ga = self.g + 1 - 2 * (self.g % 2)
        self.gb = (self.g + 2) % 4
        self.gc = (self.ga + 2) % 4
        self.y_a = {"dp": y + 1 - 2 * (y % 2)}
        self.y_b = {"dp": 3 - y}
        self.core = {"vocab_2": self.o}
        self.a = x + c * (z - x)
        self.b = z + c * (x - z)
        self.a_peers = [self._at((self.a + off) % 4, self.b) for off in (1, 2, 3)]
        self.b_peers = [self._at(self.a, (self.b + off) % 4) for off in (1, 2, 3)]
        cores = [(off, core) for off in range(4) for core in (self.c, self.o)][1:]
        self.line = [{"vocab_1": (x + off) % 4, "vocab_2": core} for off, core in cores]
        planes = [(up, over) for up in range(4) for over in range(4)][1:]
        self.sheet = [{"vocab_0": (z + up) % 4, "dp": (y + over) % 4} for up, over in planes]
        self.y_peers = [{"dp": (y + off) % 4} for off in (1, 2, 3)]
        self.cols = pl.ds(pl.multiple_of(c * HALF, 128), HALF)
        self.a_at = [(self.a + off) % 4 for off in (1, 2, 3)]
        self.b_at = [(self.b + off) % 4 for off in (1, 2, 3)]
        self.y_at = [gray((y + off) % 4) for off in (1, 2, 3)]
        a, b = self.a, self.b
        a0, a1, b0, b1 = (a + a // 2) % 2, a // 2, (b + b // 2) % 2, b // 2
        self.colours = [(a0 + third) % 2 + 2 * ((a1 + third) % 2) for third in (b0, b1)]
        flip_a, flip_b = a + 1 - 2 * (a % 2), b + 1 - 2 * (b % 2)
        first, second = self._at(flip_a, b), self._at(3 - a, b)
        self.near = [
            [first, second, self._at(a, flip_b)],
            [second, first, self._at(a, 3 - b)],
        ]
        self.parts = [
            pl.ds(pl.multiple_of(c * HALF + part * (HALF // 2), 128), HALF // 2) for part in range(2)
        ]

    def _at(self, a, b):
        return {"vocab_1": a + self.c * (b - a), "vocab_0": b + self.c * (a - b)}

    def tile_cols(self, j):
        return pl.ds(pl.multiple_of(self.c * HALF + j * W, 128), W)

    def first_row_of(self, k):
        return (((gray(k) * 4 + self.z) * 4 + self.x) * 2 + self.c) * ROWS

    def meet(self):
        peers = self.line + self.sheet
        barrier = pltpu.get_barrier_semaphore()
        for peer in peers:
            pl.semaphore_signal(barrier, inc=1, device_id=peer, device_id_type=MESH)
        return lambda: pl.semaphore_wait(barrier, len(peers))


class Sent:
    def __init__(self, sems, at, parts, out_like, in_like, times):
        self.sems, self.at, self.parts = sems, at, parts
        self.out_like, self.in_like, self.times = out_like, in_like, times

    def start(self, parts=None):
        for src, dst, peer in self.parts if parts is None else parts:
            pltpu.make_async_remote_copy(
                src_ref=src(),
                dst_ref=dst(),
                send_sem=self.sems[0].at[self.at],
                recv_sem=self.sems[1].at[self.at],
                device_id=peer,
                device_id_type=MESH,
            ).start()

    def wait_send(self):
        times, self.times = self.times, 0
        for _ in range(times):
            like = self.out_like()
            pltpu.make_async_copy(like, like, self.sems[0].at[self.at]).wait()

    def wait_recv(self):
        like = self.in_like()
        pltpu.make_async_copy(like, like, self.sems[1].at[self.at]).wait()


class Post:
    def __init__(self, send_sems, recv_sems):
        self.sems = (send_sems, recv_sems)
        self.used = 0
        self.open = []

    def send(self, src, dst, peer):
        return self.group([(src, dst, peer)], src, dst)

    def group(self, parts, out_like, in_like, times=1):
        sent = self.plan(parts, out_like, in_like, times)
        sent.start()
        return sent

    def plan(self, parts, out_like, in_like, times=1):
        sent = Sent(self.sems, self.used, parts, out_like, in_like, times)
        self.used += 1
        self.open.append(sent)
        return sent

    def sent(self, item):
        item.wait_send()
        self.open = [c for c in self.open if c is not item]

    def close(self):
        for item in self.open:
            item.wait_send()
        self.open = []


class Seen:
    def wait_recv(self):
        pass


class Agenda:
    def __init__(self):
        self.now = 0.0
        self.todo = []
        self.count = 0

    def add(self, after, step):
        self.todo.append((self.now + after, self.count, step))
        self.count += 1

    def run(self, until=None):
        while self.todo:
            self.todo.sort(key=lambda item: item[:2])
            if until is not None and self.todo[0][0] > until:
                return
            when, _, step = self.todo.pop(0)
            self.now = max(self.now, when)
            step()

    def due(self, until):
        return any(item[0] <= until for item in self.todo)

    def compute(self, cost, work):
        self.run(self.now)
        work()
        self.now += cost
        self.run(self.now)


def columns(table, j, core):
    own = pl.ds(pl.multiple_of(core * HALF + j * W, 128), W)
    other = pl.ds(pl.multiple_of((1 - core) * HALF + j * W, 128), W)
    return jnp.concatenate([table[:, own], table[:, other]], axis=1)


def gather_rows(place, post, agenda, buf, sends, done):
    a, b, cols = place.a, place.b, place.cols

    def mine():
        return buf.at[b, a, :, cols]

    def row():
        return buf.at[:, a, :, cols]

    def rows():
        return buf.at[:, 0:3, :, cols]

    def half():
        return buf.at[:, :, :, cols]

    first = post.group(
        [(mine, mine, peer) for peer in place.b_peers], mine, lambda: buf.at[0:3, 0, :, cols], 3
    )
    sends.append(first)

    def along_a():
        first.wait_recv()
        second = post.group([(row, row, peer) for peer in place.a_peers], rows, rows)
        sends.append(second)
        agenda.add(9.0, lambda: across(second))

    def across(second):
        second.wait_recv()
        third = post.send(half, half, place.core)
        sends.append(third)
        agenda.add(4.0, lambda: finish(third))

    def finish(third):
        third.wait_recv()
        done()

    agenda.add(13.0, along_a)


POSTS = 32
STEPS = 8
LAG = (1, 3, 5)
TAIL_AT = ((1, 2), (4, 2), (6, 1), (8, 1), (10, 1), (12, 1), (14, 0), (15, 0))
HEAD_TILES = 2 * NT_COLS
TAIL = TAIL_AT[-1][0] + 1


def main_kernel(
    ids_hbm, targets_hbm, mask_hbm, hidden_hbm, gain_hbm, table_hbm, cot_hbm,
    head_hbm, metas_hbm, embed_hbm, grad_hbm, gain_sum_hbm, loss_hbm, most_hbm, cap_hbm,
    table, normed, metas, own_lines, scalars, hidden, gain_rows, gain, marks, stats, stat_in, scale_rows, back_rows, inverses, dots,
    d_stage, d_part, d_rc, d_rx, d_rz, found, owner_of, slot_of, packed, lines, cot_packed,
    stage, snd, rc, sx, rx, s_two, r_two, acc, acc_two, sz, rz, acc_z, sy, ry, up,
    gain_in, local_sems, send_sems, recv_sems, flow_send, flow_recv,
):
    place = Place()
    post = Post(send_sems, recv_sems)
    agenda = Agenda()
    first_row = place.first_row
    a, b, c, o, g, y = place.a, place.b, place.c, place.o, place.g, place.y
    blocks = [g, place.ga, place.gb, place.gc]
    entered = place.meet()
    early = [
        pltpu.make_async_copy(hidden_hbm, hidden, local_sems.at[7]),
        pltpu.make_async_copy(gain_hbm, gain_rows, local_sems.at[8]),
    ]
    for n, ref in enumerate((ids_hbm, targets_hbm, mask_hbm)):
        early.append(pltpu.make_async_copy(ref, own_lines.at[n], local_sems.at[9 + n]))
    for copy in early:
        copy.start()
    def table_load(i):
        rows = pl.ds(i * 1024, 1024 - 48 * i)
        return pltpu.make_async_copy(table_hbm.at[rows], table.at[rows], local_sems.at[5 * i])

    table_load(0).start()
    table_load(1).start()
    for copy in early[1:]:
        copy.wait()
    for n in range(3):
        metas[g, n : n + 1, :] = own_lines[n]
    gain[...] = jnp.concatenate([gain_rows[i : i + 1, :] for i in range(D // 128)], axis=1)
    early[0].wait()
    cot_load = pltpu.make_async_copy(cot_hbm, found, local_sems.at[3])
    cot_load.start()

    def inverse(wide):
        return lax.rsqrt(jnp.mean(wide * wide, axis=1, keepdims=True) + EPSILON)

    def rows_of(block, first, count):
        return pl.ds(pl.multiple_of(block * 256 + first, 16), count)

    def normalise(i, carry):
        at = i * 64
        rows = pl.ds(pl.multiple_of(at, 16), 64)
        wide = hidden[rows, :].astype(F32)
        inv = inverse(wide)
        inverses[rows, :] = jnp.broadcast_to(inv, (64, 128))
        normed[rows_of(g, at, 64), :] = (wide * inv * gain[...]).astype(BF)
        return carry

    lax.fori_loop(0, 4, normalise, 0)
    stats[...] = jnp.zeros_like(stats)
    entered()

    def piece(block, part, half):
        def rows():
            at = place.colours[part] * 64 + half * 32
            return normed.at[rows_of(block, at, 32), place.parts[part]]

        return rows

    def ship(block, part, half, peer):
        rows = piece(block, part, half)
        return post.send(rows, rows, peer)

    meta_in = [
        post.send(lambda: metas.at[g], lambda: metas.at[g], peer) for peer in (place.y_a, place.y_b)
    ]
    both = (0, 1)
    a_low = [ship(g, part, 0, place.y_a) for part in both]
    b_high = [ship(g, part, 1, place.y_b) for part in both]
    a_high = [ship(g, part, 1, place.y_a) for part in both]
    b_low = [ship(g, part, 0, place.y_b) for part in both]
    meta_c = post.plan(
        [(lambda: metas.at[place.ga], lambda: metas.at[place.ga], place.y_b)],
        lambda: metas.at[place.ga],
        lambda: metas.at[place.gc],
    )
    def pieces():
        return normed.at[pl.ds(0, 12 * 32), place.parts[0]]

    spread = {name: post.plan([], pieces, pieces) for name in "abc"}
    c_low, c_high = [], []

    def swap(block):
        def part():
            return normed.at[rows_of(block, 0, 256), place.cols]

        return post.plan([(part, part, place.core)], part, part)

    swaps = {"a": swap(place.ga), "b": swap(place.gb), "c": swap(place.gc)}

    def pass_piece(name, block, part, half):
        rows = piece(block, part, half)
        spread[name].start([(rows, rows, peer) for peer in place.near[part]])

    def spread_piece(name, block, half, items):
        for part, item in enumerate(items):
            item.wait_recv()
            pass_piece(name, block, part, half)

    def swap_block(name):
        spread[name].wait_recv()
        swaps[name].start()

    def cap_store(n):
        return pltpu.make_async_copy(
            stage.at[n, pl.ds(0, ROWS)], cap_hbm.at[n], local_sems.at[1 + n]
        )

    def forward(n, block, between, later=None):
        side = n % 2
        rows = normed[rows_of(block, 0, 256), :]
        total = jnp.zeros((1, 256), F32)
        picked = total
        for at in range(0, ROWS, MF):
            if at == 4 * MF:
                between()
            if at == 6 * MF and later is not None:
                later()
            size = min(MF, ROWS - at)
            logits = lax.dot_general(table[at : at + size, :], rows, NT, preferred_element_type=F32)
            capped = SOFTCAP * jnp.tanh(logits * (1.0 / SOFTCAP))
            raised = jnp.exp(capped)
            stage[side, at : at + size] = raised * bend(capped)
            ids = lax.broadcasted_iota(jnp.int32, capped.shape, 0) + (first_row + at)
            hit = ids == metas[block, 1:2, :]
            total += jnp.sum(raised, axis=0, keepdims=True)
            picked += jnp.sum(jnp.where(hit, capped, 0.0), axis=0, keepdims=True)
        stats[block, 0:1, :] = total
        stats[block, 1:2, :] = picked

    seen = [Seen(), Seen()]

    def pass_on():
        table_load(1).wait()
        for item in meta_in:
            item.wait_recv()
        meta_c.start()
        for part in both:
            a_low[part].wait_recv()
            c_low.append(ship(place.ga, part, 0, place.y_b))
            pass_piece("a", place.ga, part, 0)
        for part in both:
            b_high[part].wait_recv()
            c_high.append(ship(place.gb, part, 1, place.y_a))

    table_load(0).wait()
    forward(0, g, pass_on, lambda: spread_piece("a", place.ga, 1, a_high))
    cap_store(0).start()

    meta_c.wait_recv()
    ids = [metas[k, 0:1, :] for k in range(4)]
    locals_ = [row - first_row for row in ids]
    for k in range(4):
        locals_.append(own_lines[0] - place.first_row_of(k))
    owned = [jnp.where((row >= 0) & (row < ROWS), 1.0, 0.0) for row in locals_]
    later = lax.broadcasted_iota(jnp.int32, (256, 256), 0) < lax.broadcasted_iota(
        jnp.int32, (256, 256), 1
    )
    ranks = lax.dot_general(
        jnp.concatenate(owned + [jnp.zeros((8, 256), F32)], axis=0).astype(BF),
        jnp.where(later, 1.0, 0.0).astype(BF),
        NN,
        preferred_element_type=F32,
    )
    numbers = lax.broadcasted_iota(jnp.int32, (SLOTS, 256), 0).astype(F32)

    def chosen(k):
        same = (numbers == ranks[k : k + 1, :]) & (owned[k] > 0.5)
        return jnp.where(same, 1.0, 0.0)

    mine = jnp.concatenate([chosen(k) for k in range(4)], axis=0).astype(BF)
    slot_of[...] = jnp.concatenate([chosen(4 + k) for k in range(4)], axis=0).astype(BF)
    digits = [jnp.right_shift(row, 6) for row in locals_[:4]]
    digits += [jnp.bitwise_and(row, 63) for row in locals_[:4]]
    digits = [jnp.where(owned[n % 4] > 0.5, row.astype(F32), 0.0) for n, row in enumerate(digits)]
    read = lax.dot_general(
        jnp.concatenate(digits + [jnp.ones((8, 256), F32)], axis=0).astype(BF),
        mine,
        NT,
        preferred_element_type=F32,
    )
    lane = lax.broadcasted_iota(jnp.int32, (1, ALL_SLOTS), 1)
    wanted = jnp.zeros((1, ALL_SLOTS), F32)
    for k in range(4):
        here = (lane >= k * SLOTS) & (lane < (k + 1) * SLOTS)
        wanted = jnp.where(here, read[k : k + 1] * 64.0 + read[4 + k : 5 + k], wanted)
    wanted = jnp.where(read[8:9] > 0.5, wanted, -1.0)

    starts = lax.broadcasted_iota(jnp.int32, (128, 256), 0) * ROWS
    most = jnp.float32(0.0)
    for row in ids:
        held = jnp.where((row >= starts) & (row < starts + ROWS), 1.0, 0.0)
        most = jnp.maximum(most, jnp.max(jnp.sum(held, axis=1, keepdims=True)))
    keep = jnp.where(most <= SLOTS, 1.0, 0.0)

    def mark(i, carry):
        rows = pl.ds(pl.multiple_of(i * MT, 16), MT)
        at = lax.broadcasted_iota(jnp.int32, (MT, ALL_SLOTS), 0) + i * MT
        same = at.astype(F32) == wanted
        owner_of[rows, :] = jnp.where(same, 1.0, 0.0).astype(BF)
        marks[rows, 1024:1152] = jnp.where(same, keep * SCALE_HIGH, 0.0).astype(BF)
        marks[rows, 1152:1280] = jnp.where(same, keep * SCALE_LOW, 0.0).astype(BF)
        return carry


    lax.fori_loop(0, NV, mark, 0)

    def look_up(j, carry):
        cols = pl.ds(pl.multiple_of(j * 2 * W, 128), 2 * W)
        rows = lax.dot_general(owner_of[...], table[:, cols], TN, preferred_element_type=F32)
        packed[:, :, cols] = rows.astype(BF).reshape(4, SLOTS, 2 * W)
        return carry

    def exchange(src, dst):
        dst[g] = src[g]
        parts = [
            (lambda n=n: src.at[place.y_at[n]], lambda: dst.at[g], peer)
            for n, peer in enumerate(place.y_peers)
        ]
        return post.group(parts, lambda: src.at[0:3], lambda: dst.at[0:3])

    spread_piece("b", place.gb, 1, seen)
    spread_piece("b", place.gb, 0, b_low)
    lax.fori_loop(0, EARLY, look_up, 0)
    swap_block("a")
    spread_piece("c", place.gc, 0, c_low)
    spread_piece("c", place.gc, 1, c_high)
    lax.fori_loop(EARLY, NT_COLS, look_up, 0)
    line_item = exchange(packed, lines)

    def cot_pack(j, carry):
        cols = pl.ds(pl.multiple_of(j * 2 * W, 128), 2 * W)
        rows = lax.dot_general(
            slot_of[...], found[:, :, :, cols].reshape(256, 2 * W), NN, preferred_element_type=F32
        )
        cot_packed[:, :, cols] = rows.astype(BF).reshape(4, SLOTS, 2 * W)
        return carry

    def later_block(n, carry):
        block = jnp.where(n == 1, place.ga, jnp.where(n == 2, place.gb, place.gc))

        @pl.when(n == 1)
        def _():
            swaps["a"].wait_recv()

        @pl.when(n == 2)
        def _():
            swaps["b"].wait_recv()
            cap_store(0).wait()

        @pl.when(n == 3)
        def _():
            swaps["c"].wait_recv()
            cap_store(1).wait()

        def between():
            @pl.when(n == 1)
            def _():
                swap_block("b")

            @pl.when(n == 2)
            def _():
                swap_block("c")

        forward(n, block, between)

        @pl.when(n == 1)
        def _():
            cap_store(1).start()

        return carry

    lax.fori_loop(1, 4, later_block, 0)

    found_sends = []

    def unpack():
        line_item.wait_recv()
        for h in range(2):
            rows = lax.dot_general(
                slot_of[...],
                lines[:, :, h * HALF : (h + 1) * HALF].reshape(ALL_SLOTS, HALF),
                TN,
                preferred_element_type=F32,
            )
            d_part[h] = rows.astype(BF).reshape(4, 4, 16, HALF)
        return post.send(lambda: d_part.at[o], lambda: d_rc, place.core)

    def d_merge(item):
        item.wait_recv()
        d_rc[...] = d_part[c] + d_rc[...]
        parts = [
            (lambda n=n: d_rc.at[:, place.a_at[n]], lambda n=n: d_rx.at[n], peer)
            for n, peer in enumerate(place.a_peers)
        ]
        item = post.group(parts, lambda: d_rx, lambda: d_rx)
        agenda.add(9.0, lambda: d_along_b(item))

    def d_along_b(item):
        item.wait_recv()
        d_rc[:, a] = (d_rc[:, a] + d_rx[0]) + (d_rx[1] + d_rx[2])
        parts = [
            (lambda n=n: d_rc.at[place.b_at[n], a], lambda n=n: d_rz.at[n], peer)
            for n, peer in enumerate(place.b_peers)
        ]
        item = post.group(parts, lambda: d_rz, lambda: d_rz)
        agenda.add(12.0, lambda: d_end(item))

    def d_end(item):
        item.wait_recv()
        row = (d_rc[b, a] + d_rz[0]) + (d_rz[1] + d_rz[2])
        found[b, a, :, place.cols] = (row.astype(F32) * EMBED_SCALE).astype(BF)
        gather_rows(place, post, agenda, found, found_sends, embed_done)

    def embed_store():
        return pltpu.make_async_copy(found, embed_hbm, local_sems.at[0])

    def embed_done():
        embed_store().start()
        for item in found_sends:
            post.sent(item)

    def ring_start(base, peers, at):
        stat_in[base + at] = stats[...]

        def part():
            return stat_in.at[base + at]

        def like():
            return stat_in.at[pl.ds(0, len(peers))]

        return post.group([(part, part, peer) for peer in peers], like, like)

    def ring_end(item, base, count):
        item.wait_recv()
        total = stat_in[base]
        for i in range(1, count):
            total = total + stat_in[base + i]
        stats[...] = total

    item = ring_start(0, place.line, place.x * 2 + c)
    half_item = unpack()
    ring_end(item, 0, 8)
    item = ring_start(8, place.sheet, place.z * 4 + y)
    cot_load.wait()
    lax.fori_loop(0, NT_COLS, cot_pack, 0)
    ring_end(item, 8, 16)
    cot_item = exchange(cot_packed, normed.at[pl.ds(1024, ALL_SLOTS)].reshape(4, SLOTS, D))
    agenda.now = 40.0
    d_merge(half_item)

    def cap_load(n):
        return pltpu.make_async_copy(
            cap_hbm.at[n], stage.at[n, pl.ds(0, ROWS)], local_sems.at[1 + n]
        )

    def slopes(n):
        block, side = blocks[n], n % 2
        if n < 2:
            cap_load(n).wait()
        weight = metas[block, 2:3, :].astype(F32)
        factor = weight / stats[block, 0:1, :]
        target = metas[block, 1:2, :]
        taken = weight * bend(stats[block, 1:2, :])
        lanes = pl.ds(pl.multiple_of(block * 256, 128), 256)

        def slab(i, carry):
            rows = pl.ds(pl.multiple_of(i * MT, 16), MT)
            ids = lax.broadcasted_iota(jnp.int32, (MT, 256), 0) + (first_row + i * MT)
            hit = jnp.where(ids == target, taken, 0.0)
            value = stage[side, rows, :] * factor - hit
            marks[rows, lanes] = value.astype(BF)
            return carry

        lax.fori_loop(0, NV, slab, 0)
        if n >= 2:
            cap_load(n - 2).start()

    for n in (2, 3, 0, 1):
        agenda.compute(0.9, lambda: slopes(n))

    def bound(k):
        rest = jnp.maximum(1.0 - jnp.exp(stats[k, 1:2, :]) / stats[k, 0:1, :], 0.0)
        return TABLE_BOUND * (2.0 * rest + 1e-4)

    for k in range(4):
        turned = jnp.broadcast_to(UNITS / bound(k), (128, 256)).T
        scale_rows[k * 256 : (k + 1) * 256, :] = turned
    back_rows[...] = jnp.broadcast_to(bound(g) * (1.0 / UNITS), (128, 256)).T

    weights = [metas[k, 2:3, :].astype(F32) for k in range(4)]
    weight_sum = sum(jnp.sum(w) for w in weights)
    loss_sum = sum(
        jnp.sum(w * (jnp.log(stats[k, 0:1, :]) - stats[k, 1:2, :])) for k, w in enumerate(weights)
    )
    scalars[0] = jnp.full((1, 1), loss_sum / jnp.maximum(weight_sum, 1.0), F32)
    scalars[1] = jnp.full((1, 1), most, F32)
    small_stores = [
        pltpu.make_async_copy(scalars.at[0], loss_hbm, local_sems.at[7]),
        pltpu.make_async_copy(scalars.at[1], most_hbm, local_sems.at[8]),
        pltpu.make_async_copy(metas, metas_hbm, local_sems.at[9]),
    ]
    for copy in small_stores:
        copy.start()
    shape = (4, 4, 4, 16, W)

    class Flow:
        def __init__(self, step, j):
            self.send_sem = flow_send.at[2 * step + j % 2 if step < 3 else step + 3]
            self.recv_sem = flow_recv.at[step, j]

        def start(self, parts):
            for src, dst, peer in parts:
                pltpu.make_async_remote_copy(
                    src_ref=src,
                    dst_ref=dst,
                    send_sem=self.send_sem,
                    recv_sem=self.recv_sem,
                    device_id=peer,
                    device_id_type=MESH,
                ).start()

        def sent(self, like):
            pltpu.make_async_copy(like, like, self.send_sem).wait()

        def here(self, like):
            pltpu.make_async_copy(like, like, self.recv_sem).wait()

    def pull(t):
        slot = t % 2

        @pl.when(t >= 2)
        def _():
            Flow(0, t - 2).sent(snd.at[slot])

        product = lax.dot_general(
            marks[:, 0:1024], columns(table, t, c), TN, preferred_element_type=F32
        )
        for half in range(2):
            lanes = slice(half * 128, half * 128 + 128)
            other = slice(W + half * 128, W + half * 128 + 128)
            stage[slot, 0:1024, lanes] = product[:, lanes] * scale_rows[...]
            code = encode(product[:, other] * scale_rows[...])
            snd[slot, :, :, :, :, lanes] = code.reshape(4, 4, 4, 16, 128)
        Flow(0, t).start([(snd.at[slot], rc.at[t % 4], place.core)])

    def held(slot, at):
        whole = stage.at[slot, pl.ds(0, 1024)].reshape(*shape)
        return whole[:, :, at]

    near_a = (a + 1 - 2 * (a % 2), 3 - a)

    def partners(j):
        first = near_a[0] + (j % 2) * (near_a[1] - near_a[0])
        second = near_a[1] + (j % 2) * (near_a[0] - near_a[1])
        return first, second

    def merge(j):
        slot = j % 2
        first, second = partners(j)
        Flow(0, j).here(rc.at[j % 4])

        @pl.when(j >= 2)
        def _():
            Flow(1, j - 2).sent(sx.at[slot])

        for n, at in enumerate((first, (a + 2) % 4)):
            sx[slot, n] = encode(held(slot, at) + decode(rc[j % 4, :, :, at]))
        Flow(1, j).start([(sx.at[slot], rx.at[j], place._at(first, b))])
        acc[j] = held(slot, a) + decode(rc[j % 4, :, :, a])
        acc_two[j % 3] = held(slot, second) + decode(rc[j % 4, :, :, second])

    def second_half(j):
        _, second = partners(j)
        Flow(1, j).here(rx.at[j])

        @pl.when(j >= 2)
        def _():
            Flow(2, j - 2).sent(s_two.at[j % 2])

        s_two[j % 2] = encode(acc_two[j % 3] + decode(rx[j, 1]))
        Flow(2, j).start([(s_two.at[j % 2], r_two.at[j], place._at(second, b))])
        acc[j] = acc[j] + decode(rx[j, 0])

    def along_y(j):
        Flow(2, j).here(r_two.at[j])
        acc_z[j] = acc[j, g] + decode(r_two[j, g])
        parts = []
        for n, peer in enumerate(place.y_peers):
            at = place.y_at[n]
            sz[j, n] = encode(acc[j, at] + decode(r_two[j, at]))
            parts.append((sz.at[j, n], rz.at[j, n], peer))
        Flow(3, j).start(parts)

    def along_b(j):
        Flow(3, j).here(rz.at[j])
        acc_z[j] = acc_z[j] + decode(rz[j, 0]) + decode(rz[j, 1]) + decode(rz[j, 2])
        parts = []
        for n, peer in enumerate(place.b_peers):
            sy[j, n] = encode(acc_z[j, place.b_at[n]])
            parts.append((sy.at[j, n], ry.at[j, n], peer))
        Flow(4, j).start(parts)

    def give_b(j):
        Flow(4, j).here(ry.at[j])
        value = acc_z[j, b] + decode(ry[j, 0]) + decode(ry[j, 1]) + decode(ry[j, 2])
        cols = place.tile_cols(j)
        up[b, a, :, cols] = encode(value)
        part = up.at[b, a, :, cols]
        Flow(5, j).start([(part, part, peer) for peer in place.b_peers])

    def give_a(j):
        cols = place.tile_cols(j)
        Flow(5, j).here(up.at[0:3, 0, :, cols])
        part = up.at[:, a, :, cols]
        Flow(6, j).start([(part, part, peer) for peer in place.a_peers])

    def give_core(j):
        cols = place.tile_cols(j)
        Flow(6, j).here(up.at[:, 0:3, :, cols])
        part = up.at[:, :, :, cols]
        Flow(7, j).start([(part, part, place.core)])

    def last(j):
        cols = place.tile_cols(j)
        Flow(7, j).here(up.at[:, :, :, cols])
        down, inv = back_rows[...], inverses[...]
        for h in range(2):
            for q in range(W // 128):
                at = h * HALF + j * W + q * 128
                cols = pl.ds(pl.multiple_of(at, 128), 128)
                value = decode(up[:, :, :, cols].reshape(256, 128)) * down
                product = value * hidden[:, cols].astype(F32)
                dots[...] += product * gain[:, cols]
                gain_in[y, pl.ds(h * (HALF // 128) + j * 2 + q, 1), :] = jnp.sum(
                    product * inv, axis=0, keepdims=True
                )

    steps = (merge, second_half, along_y, along_b, give_b, give_a, give_core, last)

    def head_store(n):
        cols = pl.ds(pl.multiple_of(n * W, 128), W)
        return pltpu.make_async_copy(
            d_stage.at[n % 2, pl.ds(0, ROWS)], head_hbm.at[:, cols], local_sems.at[3 + n % 2]
        )

    def head_tile(n):
        @pl.when(n >= 2)
        def _():
            head_store(n - 2).wait()

        cols = pl.ds(pl.multiple_of(n * W, 128), W)
        product = lax.dot_general(marks[...], normed[:, cols], NN, preferred_element_type=F32)
        d_stage[n % 2, 0:ROWS] = product.astype(BF)
        head_store(n).start()

    def take_due(t, turns, pace):
        for k in range(turns):
            due = agenda.now + pace
            if agenda.due(due):
                @pl.when(t == k)
                def _():
                    agenda.run(due)
            agenda.now = max(agenda.now, due)

    def turn(t, carry):
        pull(t)
        for lag, step in zip(LAG, steps):
            @pl.when(t >= lag)
            def _():
                step(t - lag)

        take_due(t, NT_COLS, 2.8)
        return carry

    dots[...] = jnp.zeros_like(dots)
    lax.fori_loop(0, NT_COLS, turn, 0)
    cot_item.wait_recv()
    normed[1152:1280, :] = normed[1024:1152, :]

    agenda.add(22.0, post.close)

    def tail(t, carry):
        @pl.when(t < HEAD_TILES)
        def _():
            head_tile(t)

        for n, ((at, pace), step) in enumerate(zip(TAIL_AT, steps)):
            if pace == 0:
                for q in range(2):
                    j = NT_COLS - 1 - 2 * (at - t) + q

                    @pl.when((j >= 0) & (j < NT_COLS))
                    def _():
                        step(j)

                continue
            begun = NT_COLS - LAG[n] if n < len(LAG) else 0
            ahead = at - t
            j = NT_COLS - 1 - ahead // pace

            @pl.when((ahead >= 0) & (ahead % pace == 0) & (j >= begun))
            def _():
                step(j)

        take_due(t, TAIL, 1.9)
        return carry

    lax.fori_loop(0, TAIL, tail, 0)

    def gain_part():
        return gain_in.at[y]

    gain_item = post.group(
        [(gain_part, gain_part, peer) for peer in place.y_peers],
        lambda: gain_in.at[0:3],
        lambda: gain_in.at[0:3],
    )

    agenda.run()

    GR = 16

    def upstream(i):
        rows = pl.ds(pl.multiple_of(i * GR, 16), GR)
        down = back_rows[rows, :]
        value = decode(up[i // 4, i % 4]) * jnp.concatenate([down] * (D // 128), axis=1)
        return value, hidden[rows, :].astype(F32), inverses[rows, :]

    def grad_rows(i, carry):
        value, wide, inv = upstream(i)
        rows = pl.ds(pl.multiple_of(i * GR, 16), GR)
        mean_dot = jnp.sum(dots[rows, :], axis=1, keepdims=True) * (1.0 / D)
        pull_back = inv * inv * inv * mean_dot
        out = jnp.concatenate([inv] * (D // 128), axis=1) * (value * gain[...])
        out = out - wide * jnp.concatenate([pull_back] * (D // 128), axis=1)
        normed[rows, :] = out.astype(BF)
        pltpu.make_async_copy(normed.at[rows], grad_hbm.at[rows], local_sems.at[6]).start()
        return carry

    lax.fori_loop(0, 16, grad_rows, 0)
    for copy in small_stores:
        copy.wait()
    for n in (HEAD_TILES - 2, HEAD_TILES - 1):
        head_store(n).wait()

    Flow(3, 0).sent(sz)
    Flow(4, 0).sent(sy)
    Flow(5, 0).sent(up.at[0:3, 0, :, place.cols])
    Flow(6, 0).sent(up.at[:, 0:3, :, place.cols])
    Flow(7, 0).sent(up.at[:, :, :, place.cols])
    for j in (NT_COLS - 2, NT_COLS - 1):
        Flow(0, j).sent(snd.at[j % 2])
        Flow(1, j).sent(sx.at[j % 2])
        Flow(2, j).sent(s_two.at[j % 2])
    post.close()
    gain_item.wait_recv()
    gain_rows[...] = gain_in[0] + gain_in[1] + gain_in[2] + gain_in[3]
    gain_store = pltpu.make_async_copy(gain_rows, gain_sum_hbm, local_sems.at[10])
    gain_store.start()
    gain_store.wait()
    embed_store().wait()
    pltpu.make_async_copy(normed.at[pl.ds(0, 256)], grad_hbm, local_sems.at[6]).wait()


def deliver_kernel(*refs):
    ins, outs, (small, large, line, sems) = refs[:4], refs[4:8], refs[8:]
    moves = [(ins[0], outs[0], line, 0)]
    moves += [(ins[n], outs[n], small.at[n - 1], n) for n in (1, 2)]
    for i in range(ROWS // MOVED):
        rows = pl.ds(i * MOVED, MOVED)
        moves.append((ins[3].at[rows], outs[3].at[rows], large.at[rows], 3 + i))
    for src, _, buf, n in moves:
        pltpu.make_async_copy(src, buf, sems.at[n]).start()
    for src, dst, buf, n in moves:
        pltpu.make_async_copy(src, buf, sems.at[n]).wait()
        pltpu.make_async_copy(buf, dst, sems.at[n]).start()
    for _, dst, buf, n in moves:
        pltpu.make_async_copy(buf, dst, sems.at[n]).wait()


def around(array, axis):
    count = lax.axis_size(axis)
    for _ in range(count - 1):
        array = lax.ppermute(array, axis, [(i, (i + 1) % count) for i in range(count)])
        yield array


def dense_embedding(ids, embed_cotangent, table, head):
    local = ids - lax.axis_index(DP_VOCAB) * ROWS
    inside = (local >= 0) & (local < ROWS)
    rows = jnp.take(table, jnp.clip(local, 0, ROWS - 1), axis=0)
    total = jnp.where(inside[:, None], rows, 0)
    for axis in DP_VOCAB:
        total = sum(around(total, axis), total)
    g = gray(lax.axis_index("dp"))
    own = lax.dynamic_slice_in_dim(total, g * 256, 256, axis=0)
    embedded = (own.astype(F32) * EMBED_SCALE).astype(BF)
    y = lax.axis_index("dp")
    cot = lax.dynamic_update_slice_in_dim(jnp.zeros((1024, D), BF), embed_cotangent, g * 256, axis=0)
    for off, block in enumerate(around(embed_cotangent, "dp")):
        cot = lax.dynamic_update_slice_in_dim(cot, block, gray((y - off - 1) % 4) * 256, axis=0)
    where = jnp.where(inside, local, ROWS)
    part = jax.ops.segment_sum(cot.astype(F32), where, num_segments=ROWS + 1)[:ROWS]
    return embedded, (head.astype(F32) + part * EMBED_SCALE).astype(BF)


def body(input_ids, target_ids, loss_mask, final_hidden, norm_gain, embed_cotangent, table):
    any_ = pl.BlockSpec(memory_space=pl.ANY)
    vmem = pl.BlockSpec(memory_space=pltpu.VMEM)
    dma = pltpu.SemaphoreType.DMA
    V = pltpu.VMEM
    S = jax.ShapeDtypeStruct
    gain = norm_gain.reshape(D // 128, 128)
    n = NT_COLS
    head, metas, embed, grad, gain_grad, loss, most, _ = pl.pallas_call(
        main_kernel,
        out_shape=(
            S((ROWS, D), BF),
            S((4, 8, 256), jnp.int32),
            S((4, 4, 16, D), BF),
            S((256, D), BF),
            S((D // 128, 128), F32),
            S((1, 1), F32),
            S((1, 1), F32),
            S((2, ROWS, 256), F32),
        ),
        in_specs=[any_] * 7,
        out_specs=(any_,) * 8,
        scratch_shapes=[
            V((ROWS, D), BF),
            V((1024 + 2 * ALL_SLOTS, D), BF),
            V((4, 8, 256), jnp.int32),
            V((3, 1, 256), jnp.int32),
            V((2, 1, 1), F32),
            V((256, D), BF),
            V((D // 128, 128), F32),
            V((1, D), F32),
            V((ROWS, 1024 + 2 * ALL_SLOTS), BF),
            V((4, 2, 256), F32),
            V((24, 4, 2, 256), F32),
            V((1024, 128), F32),
            V((256, 128), F32),
            V((256, 128), F32),
            V((256, 128), F32),
            V((2, 2048, W), BF),
            V((2, 4, 4, 16, HALF), BF),
            V((4, 4, 16, HALF), BF),
            V((3, 4, 16, HALF), BF),
            V((3, 16, HALF), BF),
            V((4, 4, 16, D), BF),
            V((ROWS, ALL_SLOTS), BF),
            V((ALL_SLOTS, 256), BF),
            V((4, SLOTS, D), BF),
            V((4, SLOTS, D), BF),
            V((4, SLOTS, D), BF),
            V((2, 2048, W), F32),
            V((2, 4, 4, 4, 16, W), I16),
            V((4, 4, 4, 4, 16, W), I16),
            V((2, 2, 4, 4, 16, W), I16),
            V((n, 2, 4, 4, 16, W), I16),
            V((2, 4, 4, 16, W), I16),
            V((n, 4, 4, 16, W), I16),
            V((n, 4, 4, 16, W), F32),
            V((3, 4, 4, 16, W), F32),
            V((n, 3, 4, 16, W), I16),
            V((n, 3, 4, 16, W), I16),
            V((n, 4, 16, W), F32),
            V((n, 3, 16, W), I16),
            V((n, 3, 16, W), I16),
            V((4, 4, 16, D), I16),
            V((4, D // 128, 128), F32),
            dma((12,)),
            dma((POSTS,)),
            dma((POSTS,)),
            dma((STEPS + 3,)),
            dma((STEPS, n)),
        ],
        compiler_params=pltpu.CompilerParams(
            collective_id=0, has_side_effects=True, vmem_limit_bytes=VMEM_LIMIT
        ),
        name="main",
    )(
        input_ids.reshape(1, 256),
        target_ids.reshape(1, 256),
        loss_mask.reshape(1, 256),
        final_hidden,
        gain,
        table,
        embed_cotangent.reshape(4, 4, 16, D),
    )

    embedded, table_grad = lax.cond(
        most.reshape(()) > SLOTS,
        lambda: dense_embedding(metas[:, 0, :].reshape(1024), embed_cotangent, table, head),
        lambda: (embed.reshape(256, D), head),
    )
    gain_grad, embedded, grad_hidden, table_grad = pl.pallas_call(
        deliver_kernel,
        out_shape=(S((D // 128, 128), F32), S((256, D), BF), S((256, D), BF), S((ROWS, D), BF)),
        in_specs=[any_] * 4,
        out_specs=(any_,) * 4,
        scratch_shapes=[
            V((2, 256, D), BF),
            V((ROWS, D), BF),
            V((D // 128, 128), F32),
            dma((3 + ROWS // MOVED,)),
        ],
        compiler_params=pltpu.CompilerParams(vmem_limit_bytes=VMEM_LIMIT),
        name="deliver",
    )(gain_grad, embedded, grad, table_grad)
    return (embedded, loss.reshape(()), grad_hidden, gain_grad.reshape(D), table_grad)


def solution(mesh):
    finer = Mesh(
        mesh.devices.reshape(mesh.shape["dp"], 4, 4, 2), ("dp", "vocab_0", "vocab_1", "vocab_2")
    )
    placed = (P("dp"), P("dp"), P("dp"), P("dp", None), P(), P("dp", None), P(DP_VOCAB, None))
    return jax.shard_map(
        body,
        mesh=finer,
        in_specs=placed,
        out_specs=(P("dp", None), P(), P("dp", None), P(), P(DP_VOCAB, None)),
        check_vma=False,
    )
```
